32 devices in a mesh: rows: 8 (over z, y), cols: 4 (over x, core).
Axes of the slice: x: 2, y: 2, z: 4, core: 2. Of those that a mesh axis runs over, the one named last changes fastest.
Arguments:
- latent: bfloat16 [4, 8, 1024], P(None, 'rows', 'cols'), may hold values from -18 to 18
- deep: bfloat16 [320, 8, 1024], P(None, 'rows', 'cols'), may hold values from -6 to 6
- timestep: int32 [1], replicated, may hold values from 0 to 999
- in_weight: bfloat16 [36, 320], replicated, may hold values from -1 to 1
- front_weight: bfloat16 [5760, 320], P('rows'), may hold values from -0.078125 to 0.078125
- middle_weight: bfloat16 [2880, 320], P('cols'), may hold values from -0.109375 to 0.109375
- skip_weight: bfloat16 [640, 320], P('cols'), may hold values from -0.25 to 0.25
- out_weight: bfloat16 [2880, 4], replicated, may hold values from -0.109375 to 0.109375
- time_weight: bfloat16 [320, 1280], replicated, may hold values from -0.3125 to 0.3125
- time_second: bfloat16 [1280, 1280], P('cols'), may hold values from -0.15625 to 0.15625
- time_proj: bfloat16 [1280, 320], replicated, may hold values from -0.15625 to 0.15625
- input_gain: float32 [640], replicated, may hold values from 0.1 to 1.9
- middle_gain: float32 [320], replicated, may hold values from 0.1 to 1.9
- output_gain: float32 [320], replicated, may hold values from 0.1 to 1.9
Outputs:
- noise: float32 [4, 8, 1024], P(None, 'rows', 'cols')
The draws below stay inside these ranges and needn't reach their ends.
All inputs are finite; a program needn't handle non-finite values.
Results may differ from the reference program's by a relative error of at most 0.0047.
Values may be sent and summed in bfloat16 or wider, within the bound.
A program may use at most 64 MiB of HBM per device.

```python
import math
import jax
import jax.numpy as jnp
from jax import lax

C = 320
CIN = 4
GROUPS = 32
FREQ = 320
TIME = 1280
H = 8
W = 1024


def draw_latent(key, part):
    key_base = jax.random.fold_in(key, 11)
    key_rough = jax.random.fold_in(key, 23)
    positions = jnp.arange(H, dtype=jnp.float32) / H
    rising = 3.0 ** positions
    rough = jax.random.uniform(key_rough, (CIN, H, W), jnp.float32, 0.5, 1.5)
    base = jnp.clip(jax.random.normal(key_base, (CIN, H, W), jnp.float32), -4.0, 4.0)
    return (base * rough * rising[None, :, None]).astype(jnp.bfloat16)


def draw_deep(key, part):
    map_count = 6
    wave_count = 3
    key_rowfreq = jax.random.fold_in(key, 101)
    key_colfreq = jax.random.fold_in(key, 103)
    key_phase = jax.random.fold_in(key, 107)
    key_amplitude = jax.random.fold_in(key, 109)
    key_loadings = jax.random.fold_in(key, 113)
    key_jitter = jax.random.fold_in(key, 127)
    key_offset = jax.random.fold_in(key, 131)
    freq_rows = jax.random.randint(key_rowfreq, (map_count, wave_count), 1, 5).astype(jnp.float32)
    freq_cols = jax.random.randint(key_colfreq, (map_count, wave_count), 1, 9).astype(jnp.float32)
    phases = jax.random.uniform(key_phase, (map_count, wave_count), jnp.float32, 0.0, 2.0 * math.pi)
    amplitude = jax.random.normal(key_amplitude, (map_count, wave_count), jnp.float32)
    row_pos = jnp.arange(H, dtype=jnp.float32) / H
    col_pos = jnp.arange(W, dtype=jnp.float32) / W
    smooth_maps = jnp.zeros((map_count, H, W), jnp.float32)
    for wave_index in range(wave_count):
        angle_grid = 2.0 * math.pi * (freq_rows[:, wave_index, None, None] * row_pos[None, :, None] + freq_cols[:, wave_index, None, None] * col_pos[None, None, :]) + phases[:, wave_index, None, None]
        smooth_maps = smooth_maps + amplitude[:, wave_index, None, None] * jnp.cos(angle_grid)
    map_norms = jnp.sqrt(0.5 * jnp.sum(amplitude * amplitude, axis=1) + 0.001)
    smooth_maps = smooth_maps / map_norms[:, None, None]
    loadings = jax.random.normal(key_loadings, (C, map_count), jnp.float32) * (1.1 / math.sqrt(map_count))
    common_part = jnp.einsum('ck,khw->chw', loadings, smooth_maps)
    offsets = 0.3 * jax.random.normal(key_offset, (C,), jnp.float32)
    jitter = 0.5 * jax.random.normal(key_jitter, (C, H, W), jnp.float32)
    result_value = common_part + jitter + offsets[:, None, None]
    return jnp.clip(result_value, -6.0, 6.0).astype(jnp.bfloat16)


def shard_levels(stream_key, shape, shards, smallest, largest):
    def one(dim, shards_of):
        steps = jax.random.uniform(jax.random.fold_in(jax.random.fold_in(stream_key, 6), dim), (shards_of,), jnp.float32, smallest / len(shards), largest / len(shards))
        return jnp.repeat(jnp.exp(steps), shape[dim] // shards_of).reshape((-1,) + (1,) * (len(shape) - dim - 1))

    level = one(*shards[0])
    for cut in shards[1:]:
        level = level * one(*cut)
    return level


def noise(key, shape, width, most, cuts=(), held_as=jnp.bfloat16):
    level = shard_levels(key, shape, cuts, -0.22, 0.18) if cuts else 1.0
    values = jax.random.normal(key, shape, jnp.float32) * width * level
    return jnp.minimum(jnp.maximum(values, -most), most).astype(held_as)


def setup_inputs(seed: int = 0) -> dict:
    seeds = jax.random.split(jax.random.key(seed), 15)
    latent = draw_latent(jax.random.fold_in(seeds[14], 71), 0)
    deep = draw_deep(jax.random.fold_in(seeds[14], 71), 0)
    timestep = jax.random.randint(seeds[2], (1,), 0, 1000).astype(jnp.int32)
    in_weight = noise(seeds[3], (9 * CIN, C), (9 * CIN) ** -0.5, 1.0)
    front_weight = noise(seeds[4], (18 * C, C), (18 * C) ** -0.5, 0.078125, ((0, 8),))
    middle_weight = noise(seeds[5], (9 * C, C), (9 * C) ** -0.5, 0.109375, ((0, 4),))
    skip_weight = noise(seeds[6], (2 * C, C), (2 * C) ** -0.5, 0.25, ((0, 4),))
    out_weight = noise(seeds[7], (9 * C, CIN), (9 * C) ** -0.5, 0.109375)
    time_weight = noise(seeds[8], (FREQ, TIME), FREQ ** -0.5, 0.3125)
    time_second = noise(seeds[9], (TIME, TIME), TIME ** -0.5, 0.15625, ((0, 4),))
    time_proj = noise(seeds[10], (TIME, C), TIME ** -0.5, 0.15625)
    input_gain = jnp.clip(1.0 + 0.18 * jax.random.normal(seeds[11], (2 * C,), jnp.float32), 0.1, 1.9)
    middle_gain = jnp.clip(1.0 + 0.18 * jax.random.normal(seeds[12], (C,), jnp.float32), 0.1, 1.9)
    output_gain = jnp.clip(1.0 + 0.18 * jax.random.normal(seeds[13], (C,), jnp.float32), 0.1, 1.9)
    return {"latent": latent, "deep": deep, "timestep": timestep, "in_weight": in_weight, "front_weight": front_weight, "middle_weight": middle_weight, "skip_weight": skip_weight, "out_weight": out_weight, "time_weight": time_weight, "time_second": time_second, "time_proj": time_proj, "input_gain": input_gain, "middle_gain": middle_gain, "output_gain": output_gain}


epsilon = 1e-05

def convolve(field, weight):
    channels = field.shape[0]
    kernel = weight.astype(jnp.float32).reshape(3, 3, channels, -1).transpose(3, 2, 0, 1)
    result = lax.conv_general_dilated(field.astype(jnp.float32)[None], kernel, (1, 1), ((1, 1), (1, 1)), dimension_numbers=('NCHW', 'OIHW', 'NCHW'), precision=lax.Precision.HIGHEST)
    return result[0]

def norm_silu(values, gain):
    grouped = values.reshape(GROUPS, -1)
    center = lax.optimization_barrier(jnp.mean(grouped, axis=1, keepdims=True))
    offsets = grouped - center
    spread = lax.optimization_barrier(jnp.mean(offsets * offsets, axis=1, keepdims=True))
    scaled = (offsets * lax.rsqrt(spread + epsilon)).reshape(values.shape) * gain[:, None, None]
    return jax.nn.silu(scaled).astype(jnp.bfloat16)

def time_shift_of(timestep, time_weight, time_second, time_proj):
    half_width = time_weight.shape[0] // 2
    ratios = jnp.exp(-math.log(10000.0) * jnp.arange(half_width, dtype=jnp.float32) / half_width)
    angles = timestep[0].astype(jnp.float32) * ratios
    features = jnp.concatenate([jnp.cos(angles), jnp.sin(angles)])
    hidden = jax.nn.silu(jnp.dot(features, time_weight.astype(jnp.float32), precision=lax.Precision.HIGHEST))
    embedded = jnp.dot(hidden, time_second.astype(jnp.float32), precision=lax.Precision.HIGHEST)
    return jnp.dot(jax.nn.silu(embedded), time_proj.astype(jnp.float32), precision=lax.Precision.HIGHEST)

def reference(latent, deep, timestep, in_weight, front_weight, middle_weight, skip_weight, out_weight, time_weight, time_second, time_proj, input_gain, middle_gain, output_gain):
    skip_feat = convolve(latent, in_weight).astype(jnp.bfloat16)
    joined = jnp.concatenate([deep, skip_feat], axis=0)
    act_one = norm_silu(joined.astype(jnp.float32), input_gain)
    time_shift = time_shift_of(timestep, time_weight, time_second, time_proj)
    hidden_one = convolve(act_one, front_weight) + time_shift[:, None, None]
    act_two = norm_silu(hidden_one, middle_gain)
    flat_joined = joined.reshape(joined.shape[0], -1)
    shortcut = jnp.dot(jnp.transpose(skip_weight), flat_joined, preferred_element_type=jnp.float32)
    shortcut = shortcut.reshape(-1, joined.shape[1], joined.shape[2])
    block_out = convolve(act_two, middle_weight) + shortcut
    act_three = norm_silu(block_out, output_gain)
    return convolve(act_three, out_weight)
```

```python
import functools
import math

import jax
import jax.numpy as jnp
from jax import lax
from jax.experimental import pallas as pl
from jax.experimental.pallas import tpu as pltpu
from jax.sharding import PartitionSpec as P

GROUPS = 32
EPS = 1e-05
TILE = 16
LANES = 128
MESH = pl.DeviceIdType.MESH
F32 = jnp.float32
BF16 = jnp.bfloat16
SIDES = tuple((i, j) for i in (-1, 0, 1) for j in (-1, 0, 1) if (i, j) != (0, 0))


def dot(a, b, precision=None):
    return lax.dot_general(
        a, b, (((1,), (0,)), ((), ())), preferred_element_type=F32, precision=precision
    )


def split_dot(row, weight):
    high = row.astype(BF16)
    rest = row - high.astype(F32)
    middle = rest.astype(BF16)
    low = (rest - middle.astype(F32)).astype(BF16)
    pieces = jnp.concatenate([high.astype(F32), middle.astype(F32), low.astype(F32)], axis=0)
    return jnp.sum(dot(pieces.astype(BF16), weight), axis=0, keepdims=True)


def silu(z):
    return z / (1.0 + jnp.exp(-z))


def kernel(
    R, Q, ring,
    latent, deep, rows_in, in_w, front, middle, skip, out_w, time_w, time_s, time_p,
    noise,
    lat, jext, hext, oext, shifted, patch, fw, mw, sw, part, emb, sums_a, sums_b,
    lat_s, lat_r, halo_s, halo_r, fz_s, fy_s, fc_s, fm_r, fo_r, mid_s, mid_r, emb_s, emb_r,
    ca_s, ca_r, cb_s, cb_r, loc_s,
):
    r = lax.axis_index("rows")
    c = lax.axis_index("cols")
    C, px = deep.shape
    cin = latent.shape[0]
    image = float(px * R * Q)
    FQ = time_w.shape[0]
    gain_one = rows_in[:, FQ : FQ + 2 * C]
    gain_two = rows_in[:, FQ + 2 * C : FQ + 3 * C]
    gain_three = rows_in[:, FQ + 3 * C : FQ + 4 * C]

    def remote(src, dst, ssem, rsem, rr, cc):
        return pltpu.make_async_remote_copy(
            src_ref=src, dst_ref=dst, send_sem=ssem, recv_sem=rsem,
            device_id={"rows": rr, "cols": cc}, device_id_type=MESH,
        )

    def each(count, body):
        if count <= 8:
            for i in range(1, count):
                body(i)
        else:
            lax.fori_loop(1, count, lambda i, u: (body(i), u)[1], 0)

    barrier = pltpu.get_barrier_semaphore()

    def greet(rr, cc):
        pl.semaphore_signal(barrier, inc=1, device_id={"rows": rr, "cols": cc}, device_id_type=MESH)

    each(R, lambda i: greet(lax.rem(r + i, R), c))
    each(Q, lambda i: greet(r, lax.rem(c + i, Q)))
    for i in (-1, 1):
        for j in (-1, 1):
            greet(lax.rem(r + i + R, R), lax.rem(c + j + Q, Q))
    pl.semaphore_wait(barrier, R - 1 + Q - 1 + 4)

    def inside(rr, cc):
        return (rr >= 0) & (rr < R) & (cc >= 0) & (cc < Q)

    def lat_copy(k, rr, cc):
        i, j = SIDES[k]
        return remote(latent, lat.at[k], lat_s.at[k], lat_r.at[k], rr, cc)

    for k, (i, j) in enumerate(SIDES):
        @pl.when(inside(r + i, c + j))
        def _():
            lat_copy(k, r + i, c + j).start()

        @pl.when(jnp.logical_not(inside(r - i, c - j)))
        def _():
            lat[k] = jnp.zeros(lat.shape[1:], lat.dtype)

    parity = lax.rem(c, 2)
    mate = c + 1 - 2 * parity
    over = lax.rem(c + 2, Q)
    half_c = lax.rem(r, 2)
    twin = r + 1 - 2 * half_c
    mk, sk = middle.shape[0], skip.shape[0]

    def mid_copies(owner, s, slot_from, target):
        rows_m = pl.ds(pl.multiple_of(owner * mk, TILE), mk)
        rows_s = pl.ds(pl.multiple_of(owner * sk, TILE), sk)
        src_m, src_s = (middle, skip) if slot_from else (mw.at[rows_m], sw.at[rows_s])
        return (
            remote(src_m, mw.at[rows_m], mid_s.at[0, s], mid_r.at[0, s], r, target),
            remote(src_s, sw.at[rows_s], mid_s.at[1, s], mid_r.at[1, s], r, target),
        )

    fk = fw.shape[0] // R if ring else 0
    cut = fk // 2 // TILE * TILE
    spans = ((0, cut), (cut, fk - cut))

    def f_rows(owner, par):
        return pl.ds(pl.multiple_of(owner * fk, TILE) + spans[par][0], spans[par][1])

    def by_parity(par_of, body):
        for par in (0, 1):
            @pl.when(par_of == par)
            def _():
                body(par)

    def f_own(par, target, ssem):
        src = front.at[pl.ds(spans[par][0], spans[par][1])]
        return remote(src, fw.at[f_rows(r, par)], ssem, fm_r.at[r], target, c)

    def f_pass(owner, par, target):
        return remote(fw.at[f_rows(owner, par)], fw.at[f_rows(owner, par)],
                      fy_s.at[owner], fm_r.at[owner], target, c)

    def f_mate(owner, par):
        return remote(fw.at[f_rows(owner, par)], fw.at[f_rows(owner, par)],
                      fc_s.at[owner], fo_r.at[owner], r, mate)

    def by_distance(distances, body):
        for d in distances:
            for t in (r + 2 * d, r - 2 * d):
                @pl.when((t >= 0) & (t < R))
                def _():
                    body(t)

    locals_ = []
    if ring:
        locals_.append(pltpu.make_async_copy(
            front, fw.at[pl.ds(pl.multiple_of(r * fk, TILE), fk)], loc_s.at[0]))
    locals_.append(pltpu.make_async_copy(
        middle, mw.at[pl.ds(pl.multiple_of(c * mk, TILE), mk)], loc_s.at[1]))
    locals_.append(pltpu.make_async_copy(
        skip, sw.at[pl.ds(pl.multiple_of(c * sk, TILE), sk)], loc_s.at[2]))
    for copy in locals_:
        copy.start()

    if ring:
        def first(par):
            f_own(par, twin, fy_s.at[r]).start()
            def one(t):
                f_own(par, t, fz_s.at[t]).start()
            by_distance(range(1, R // 2), one)
        by_parity(parity, first)
    for copy in mid_copies(c, 0, True, over) + mid_copies(c, 1, True, mate):
        copy.start()

    def pass_on(distances):
        def go(par):
            def one(owner):
                f_pass(owner, par, twin).wait_recv()
                f_pass(owner, par, twin).start()
                f_mate(owner, par).start()
            by_distance(distances, one)
        by_parity(parity, go)

    for k, (i, j) in enumerate(SIDES):
        @pl.when(inside(r - i, c - j))
        def _():
            lat_copy(k, r - i, c - j).wait_recv()
    where = {side: k for k, side in enumerate(SIDES)}
    for a in range(3):
        tiles = []
        for b in range(3):
            side = (1 - a, 1 - b)
            block = latent[...] if side == (0, 0) else lat[where[side]]
            tiles.append(block.astype(F32))
        wide = jnp.concatenate(tiles, axis=1)
        for b in range(3):
            start = px + b - 1
            patch[cin * (3 * a + b) : cin * (3 * a + b + 1), :] = wide[:, start : start + px]
    skip_feat = dot(patch[...].T.astype(BF16), in_w[...]).astype(BF16)
    deep_t = deep[...].astype(F32).T.astype(BF16)
    own = pl.ds(TILE, px)
    jext[1, own, :] = jnp.concatenate([deep_t.astype(F32), skip_feat.astype(F32)], axis=1).astype(BF16)

    def halo_copy(stage, ext, k, rr, cc):
        i, j = SIDES[k]
        src = ((TILE, TILE), (TILE, px), (px, TILE))[j + 1]
        dst = ((TILE + px, TILE), (TILE, px), (0, TILE))[j + 1]
        return remote(ext.at[1, pl.ds(*src), :], ext.at[1 - i, pl.ds(*dst), :],
                      halo_s.at[stage, k], halo_r.at[stage, k], rr, cc)

    def halo_send(stage, ext):
        for k, (i, j) in enumerate(SIDES):
            @pl.when(inside(r + i, c + j))
            def _():
                halo_copy(stage, ext, k, r + i, c + j).start()

            @pl.when(jnp.logical_not(inside(r - i, c - j)))
            def _():
                dst = ((TILE + px, TILE), (TILE, px), (0, TILE))[j + 1]
                ext[1 - i, pl.ds(*dst), :] = jnp.zeros((dst[1], ext.shape[2]), ext.dtype)

    def halo_wait(stage, ext):
        for k, (i, j) in enumerate(SIDES):
            @pl.when(inside(r - i, c - j))
            def _():
                halo_copy(stage, ext, k, r - i, c - j).wait_recv()

    def indicator(channels, flip):
        shape = (LANES, channels) if flip else (channels, LANES)
        size = channels // GROUPS
        ch = lax.broadcasted_iota(jnp.int32, shape, 1 if flip else 0)
        g = lax.broadcasted_iota(jnp.int32, shape, 0 if flip else 1)
        return ((ch >= g * size) & (ch < g * size + size)).astype(F32)

    def sum_copy(buf, ssem, rsem, stage, slot, i, rr, cc):
        return remote(buf.at[stage, slot], buf.at[stage, slot],
                      ssem.at[stage, i], rsem.at[stage, i], rr, cc)

    def reduce_start(stage, values):
        top = jnp.sum(values, axis=0, keepdims=True)
        low = jnp.sum(values * values, axis=0, keepdims=True)
        both = jnp.concatenate([top, low, jnp.zeros((6, values.shape[1]), F32)], axis=0)
        sums_a[stage, c] = dot(both, indicator(values.shape[1], False), lax.Precision.HIGHEST)
        for i in range(1, Q):
            sum_copy(sums_a, ca_s, ca_r, stage, c, i, r, lax.rem(c + i, Q)).start()

    def reduce_end(stage, channels):
        for i in range(1, Q):
            s = lax.rem(c + Q - i, Q)
            sum_copy(sums_a, ca_s, ca_r, stage, s, i, r, s).wait_recv()
        sums_b[stage, r] = jnp.sum(sums_a[stage], axis=0)
        each(R, lambda i: sum_copy(sums_b, cb_s, cb_r, stage, r, i, lax.rem(r + i, R), c).start())

        def got(i):
            s = lax.rem(r + R - i, R)
            sum_copy(sums_b, cb_s, cb_r, stage, s, i, s, c).wait_recv()

        each(R, got)
        total = jnp.sum(sums_b[stage], axis=0) / (channels // GROUPS * image)
        center = total[0:1]
        inverse = lax.rsqrt(total[1:2] - center * center + EPS)
        both = jnp.concatenate([center, inverse, jnp.zeros((6, LANES), F32)], axis=0)
        wide = dot(both, indicator(channels, True), lax.Precision.HIGHEST)
        return wide[0:1], wide[1:2]

    def conv(ext, stats, gain, weight, exact=None, shift=None):
        center, inverse = stats
        if shift is not None:
            center = center - shift
        channels = ext.shape[2]
        scale = inverse * gain
        place = lax.broadcasted_iota(jnp.int32, (px + 2 * TILE, 1), 0)
        inner = (place >= TILE) & (place < TILE + px)
        total = None
        for a in (1, 0, 2):
            z = (ext[a].astype(F32) - center) * scale
            here = r + a - 1
            keep = (here >= 0) & (here < R) & (
                inner | ((place < TILE) & (c > 0)) | ((place >= TILE + px) & (c < Q - 1)))
            shifted[:, 0:channels] = jnp.where(keep, silu(z), 0.0)
            if a == 1 and exact is not None:
                shifted[own, 0:channels] = silu((exact - center) * scale)
            for b in range(3):
                act = shifted[TILE + b - 1 : TILE + b - 1 + px, 0:channels].astype(BF16)
                k = (3 * a + b) * channels
                term = dot(act, weight[k : k + channels, :])
                total = term if total is None else total + term
        return total

    joined = jext[1, own, :]
    reduce_start(0, joined.astype(F32))
    halo_send(0, jext)

    hidden = silu(split_dot(rows_in[:, 0:FQ], time_w[...]))
    tk = time_s.shape[0]
    for q in range(Q):
        @pl.when(c == q)
        def _():
            part[...] = hidden[:, q * tk : (q + 1) * tk]
    emb_own = split_dot(part[...], time_s[...])
    emb[c] = emb_own

    def emb_copy(i, src_c, tgt):
        return remote(emb.at[src_c], emb.at[src_c], emb_s.at[i], emb_r.at[i], r, tgt)

    for i in range(1, Q):
        emb_copy(i, c, lax.rem(c + i, Q)).start()

    if ring:
        pass_on((1,))
    stats = reduce_end(0, 2 * C)
    if ring:
        pass_on(range(2, R // 2))

        def from_twin(par):
            def one(t):
                owner = t + twin - r
                f_pass(owner, par, twin).wait_recv()
                f_mate(owner, par).start()
            one(r)
            by_distance(range(1, R // 2), one)
        by_parity(parity, from_twin)

    for copy in mid_copies(over, 0, False, over):
        copy.wait_recv()
    for copy in mid_copies(over, 2, False, mate):
        copy.start()

    for i in range(1, Q):
        s = lax.rem(c + Q - i, Q)
        emb_copy(i, s, s).wait_recv()
    embedded = jnp.sum(emb[...], axis=0)
    time_shift = split_dot(silu(embedded), time_p[...])

    for copy in locals_:
        copy.wait()
    halo_wait(0, jext)
    if ring:
        def from_mate(i):
            owner = lax.rem(r + i, R)
            def go(par):
                f_mate(owner, 1 - par).wait_recv()
            by_parity(parity, go)
        for i in range(1, R):
            from_mate(i)
    front_out = conv(jext, stats, gain_one, fw if ring else front)

    hext[1, own, :] = front_out.astype(BF16)
    reduce_start(1, front_out + time_shift)
    halo_send(1, hext)
    for copy in mid_copies(mate, 1, False, mate):
        copy.wait_recv()
    far = lax.rem(mate + 2, Q)
    for copy in mid_copies(far, 2, False, mate):
        copy.wait_recv()
    shortcut = dot(joined, sw[...])
    stats = reduce_end(1, C)
    halo_wait(1, hext)
    block_out = conv(hext, stats, gain_two, mw, front_out, time_shift) + shortcut

    oext[1, own, :] = block_out.astype(BF16)
    reduce_start(2, block_out)
    halo_send(2, oext)
    stats = reduce_end(2, C)
    halo_wait(2, oext)
    result = conv(oext, stats, gain_three, out_w, block_out)
    noise[...] = result.T[0 : noise.shape[0], :]

    for k, (i, j) in enumerate(SIDES):
        @pl.when(inside(r + i, c + j))
        def _():
            lat_copy(k, r + i, c + j).wait_send()
            for stage, ext in enumerate((jext, hext, oext)):
                halo_copy(stage, ext, k, r + i, c + j).wait_send()
    for i in range(1, Q):
        emb_copy(i, c, lax.rem(c + i, Q)).wait_send()
        for stage in range(3):
            sum_copy(sums_a, ca_s, ca_r, stage, c, i, r, lax.rem(c + i, Q)).wait_send()

    def sent(i):
        for stage in range(3):
            sum_copy(sums_b, cb_s, cb_r, stage, r, i, lax.rem(r + i, R), c).wait_send()

    each(R, sent)
    for copy in (mid_copies(c, 0, True, over) + mid_copies(c, 1, True, mate)
                 + mid_copies(over, 2, False, mate)):
        copy.wait_send()
    if ring:
        def last(par):
            f_own(par, twin, fy_s.at[r]).wait_send()
            def one(t):
                f_own(par, t, fz_s.at[t]).wait_send()
                f_pass(t, par, twin).wait_send()
            by_distance(range(1, R // 2), one)
            for i in range(1, R):
                f_mate(lax.rem(r + i, R), par).wait_send()
        by_parity(parity, last)


def shards(
    R, Q,
    latent, deep, timestep, in_weight, front_weight, middle_weight, skip_weight, out_weight,
    time_weight, time_second, time_proj, input_gain, middle_gain, output_gain,
):
    C = deep.shape[0]
    cin = latent.shape[0]
    px = deep.shape[1] * deep.shape[2]
    assert deep.shape[1] == 1 and Q == 4 and R % 2 == 0 and R > 2
    ring = R <= 8 and front_weight.shape[0] % TILE == 0
    half = time_weight.shape[0] // 2
    ratios = jnp.exp(-math.log(10000.0) * jnp.arange(half, dtype=F32) / half)
    angles = timestep[0].astype(F32) * ratios
    rows_in = jnp.concatenate(
        [jnp.cos(angles), jnp.sin(angles), input_gain, middle_gain, output_gain])[None, :]
    front = front_weight if ring else lax.all_gather(front_weight, "rows", axis=0, tiled=True)
    couts = out_weight.shape[1]
    out_w = jnp.pad(out_weight, ((0, 0), (0, LANES - couts)))
    vmem = pl.BlockSpec(memory_space=pltpu.VMEM)
    dma = pltpu.SemaphoreType.DMA
    wide = time_second.shape[1]
    tall = px + 2 * TILE
    args = (
        latent.reshape(cin, px), deep.reshape(C, px), rows_in, in_weight, front,
        middle_weight, skip_weight, out_w, time_weight, time_second, time_proj,
    )
    out = pl.pallas_call(
        functools.partial(kernel, R, Q, ring),
        out_shape=jax.ShapeDtypeStruct((couts, px), F32),
        in_specs=[vmem] * len(args),
        out_specs=vmem,
        scratch_shapes=[
            pltpu.VMEM((8, cin, px), BF16),
            pltpu.VMEM((3, tall, 2 * C), BF16),
            pltpu.VMEM((3, tall, C), BF16),
            pltpu.VMEM((3, tall, C), BF16),
            pltpu.VMEM((tall, 2 * C), F32),
            pltpu.VMEM((9 * cin, px), F32),
            pltpu.VMEM((18 * C if ring else TILE, C), BF16),
            pltpu.VMEM((9 * C, C), BF16),
            pltpu.VMEM((2 * C, C), BF16),
            pltpu.VMEM((1, time_second.shape[0]), F32),
            pltpu.VMEM((Q, 1, wide), F32),
            pltpu.VMEM((3, Q, 8, LANES), F32),
            pltpu.VMEM((3, R, 8, LANES), F32),
            dma((8,)), dma((8,)), dma((3, 8)), dma((3, 8)),
            dma((R,)), dma((R,)), dma((R,)), dma((R,)), dma((R,)),
            dma((2, 3)), dma((2, 3)), dma((Q,)), dma((Q,)),
            dma((3, Q)), dma((3, Q)), dma((3, R)), dma((3, R)), dma((3,)),
        ],
        compiler_params=pltpu.CompilerParams(
            collective_id=0, has_side_effects=True, vmem_limit_bytes=56 * 1024 * 1024
        ),
    )(*args)
    return out.reshape(couts, 1, px)


UNIT = 16
PACK = 24
ALONE = 3


class Box:
    pass


def snake(pos, c, R):
    q = pos + lax.rem(c, 2) * (R - 1 - 2 * pos)
    late = q // (R // 2)
    return (1 - late) * (2 * q) + late * (2 * (R - 1 - q) + 1)


def place_of(r, c, R):
    odd, h = lax.rem(r, 2), r // 2
    q = (1 - odd) * h + odd * (R - 1 - h)
    return q + lax.rem(c, 2) * (R - 1 - 2 * q)


def dot_nt(a, b, precision=None):
    return lax.dot_general(
        a, b, (((1,), (1,)), ((), ())), preferred_element_type=F32, precision=precision
    )


def pieces_of(row):
    high = row.astype(BF16)
    rest = row - high.astype(F32)
    middle = rest.astype(BF16)
    low = (rest - middle.astype(F32)).astype(BF16)
    return jnp.concatenate(
        [high.astype(F32), middle.astype(F32), low.astype(F32)], axis=0).astype(BF16)


def fast_kernel(
    R, Q, names,
    latent, deep, timestep, in_w, front, middle, skip, out_w, time_w, time_s, time_p,
    input_gain, middle_gain, output_gain, noise, *scratch,
):
    v = Box()
    for name, ref in zip(names, scratch):
        setattr(v, name, ref)
    r = lax.axis_index("rows")
    c = lax.axis_index("cols")
    C, px = deep.shape
    cin = latent.shape[0]
    couts = out_w.shape[0]
    image = float(px * R * Q)
    FQ = time_w.shape[0]
    W = px // R
    N = W * 8
    s = place_of(r, c, R)
    me = c * R + r
    CP = (C + LANES - 1) // LANES * LANES
    GAP = CP - C

    def remote(src, dst, ssem, rsem, rr, cc):
        return pltpu.make_async_remote_copy(
            src_ref=src, dst_ref=dst, send_sem=ssem, recv_sem=rsem,
            device_id={"rows": rr, "cols": cc}, device_id_type=MESH,
        )

    others = [(i, j) for i in range(R) for j in range(Q) if (i, j) != (0, 0)]
    barrier = pltpu.get_barrier_semaphore()
    for i, j in others:
        pl.semaphore_signal(
            barrier, inc=1, device_id={"rows": lax.rem(r + i, R), "cols": lax.rem(c + j, Q)},
            device_id_type=MESH)

    mk, skr, fk = middle.shape[1], skip.shape[0], front.shape[1]
    loads = {}
    for k, (name, src, dst) in enumerate((
        ("deep", deep, v.deep_v), ("front", front, v.front_v), ("latent", latent, v.lat_v),
        ("in", in_w, v.inw), ("tw", time_w, v.tw), ("ts", time_s, v.ts),
        ("middle", middle, v.mid_v),
        ("skip", skip, v.sw.at[pl.ds(pl.multiple_of(c * skr, TILE), skr)]),
        ("tp", time_p, v.tp), ("out", out_w, v.outw_v),
        ("gain_one", input_gain, v.gain_one), ("gain_two", middle_gain, v.gain_two),
        ("gain_three", output_gain, v.gain_three),
    )):
        loads[name] = pltpu.make_async_copy(src, dst, v.ld_s.at[k])
        loads[name].start()

    loads["deep"].wait()
    deep_t = v.deep_v[...].astype(F32).T
    v.dr[:, C:CP] = jnp.zeros((px, GAP), BF16)
    v.dr[:, 0:C] = deep_t.astype(BF16)
    pad = jnp.zeros((1, GAP), F32)
    deep_top = jnp.concatenate([jnp.sum(deep_t, axis=0, keepdims=True), pad], axis=1)
    deep_low = jnp.concatenate([jnp.sum(deep_t * deep_t, axis=0, keepdims=True), pad], axis=1)
    tall = PACK * UNIT
    main = C // LANES * LANES
    tail = C - main

    def packed(ref, k):
        turned = ref[...].astype(F32).T
        first, second = turned[0:tall], turned[k - tall : k]
        mixed = jnp.concatenate([first[:, main:C], second[:, main:C]], axis=1)
        return jnp.concatenate([first[:, 0:main], mixed, second[:, 0:main]], axis=1).astype(BF16)

    def unpack(block, ref, start):
        mixed = block[:, main : main + LANES]
        ref[start : start + tall, 0:main] = block[:, 0:main]
        ref[start : start + tall, main : main + LANES] = mixed
        swapped = pltpu.roll(mixed.astype(F32), LANES - tail, 1).astype(BF16)
        start = start + fk - tall
        ref[start : start + tall, 0:main] = block[:, main + LANES : 2 * C]
        ref[start : start + tall, main : main + LANES] = swapped

    loads["latent"].wait()
    v.lat[0, r] = v.lat_v[...]
    loads["front"].wait()
    v.fp[r] = packed(v.front_v, fk)

    pl.semaphore_wait(barrier, len(others))

    def lat_row(i, rr):
        return remote(v.lat_v, v.lat.at[0, r], v.one_s.at[0], v.one_r.at[0], rr, c)

    for i in range(1, R):
        lat_row(i, lax.rem(r + i, R)).start()

    def lat_left():
        return remote(v.lat_v, v.lat.at[2, r], v.one_s.at[1], v.one_r.at[2],
                      snake(R - 1, c - 1, R), c - 1)

    def lat_right():
        return remote(v.lat_v, v.lat.at[1, r], v.one_s.at[2], v.one_r.at[1],
                      snake(0, c + 1, R), c + 1)

    @pl.when(c > 0)
    def _():
        lat_left().start()

    @pl.when(c < Q - 1)
    def _():
        lat_right().start()

    core, xx = lax.rem(c, 2), c // 2
    mate = c + 1 - 2 * core
    over = lax.rem(c + 2, Q)
    y = lax.rem(r, 2)
    twin = r + 1 - 2 * y
    share = PACK // 2
    both = (share - 2 * ALONE) // 2
    sizes = {0: ALONE + both, 1: both, "E": ALONE}

    def f_part(owner, part, x_of, core_of):
        first = {
            0: x_of * (ALONE + both), 1: ALONE + both - x_of * both, "E": x_of * (ALONE + 2 * both),
        }[part]
        return v.fp.at[owner, pl.ds(
            pl.multiple_of((core_of * share + first) * UNIT, UNIT), sizes[part] * UNIT)]

    def f_move(owner, part, ssem, rr, cc):
        ref = f_part(owner, part, xx, core)
        return remote(ref, ref, ssem, v.fm_r.at[part, owner], rr, cc)

    def f_up(owner, part):
        return f_move(owner, part, v.one_s.at[6], r + 2, c)

    def f_down(owner, part):
        return f_move(owner, part, v.one_s.at[7], r - 2, c)

    def f_twin(owner, part):
        return f_move(owner, part, v.one_s.at[8], twin, c)

    def f_over(owner, x_of):
        ref = f_part(owner, "E", x_of, core)
        return remote(ref, ref, v.one_s.at[9], v.fx_r.at[owner], r, over)

    def f_mate(owner, part):
        ref = f_part(owner, part, xx, core)
        return remote(ref, ref, v.one_s.at[10], v.one_r.at[10], r, mate)

    def f_mate_extra(owner):
        ref = f_part(owner, "E", 1 - xx, core)
        return remote(ref, ref, v.one_s.at[10], v.one_r.at[10], r, mate)

    def when_row(t, body):
        @pl.when((t >= 0) & (t < R))
        def _():
            body()

    for part in (0, 1):
        when_row(r + 2, lambda: f_up(r, part).start())
        when_row(r - 2, lambda: f_down(r, part).start())
        f_twin(r, part).start()

    def from_z(d, sign, part):
        t = r + sign * 2 * d

        def body():
            f_twin(t, part).wait_recv()
            if sign < 0:
                when_row(r + 2, lambda: f_up(t, part).start())
            else:
                when_row(r - 2, lambda: f_down(t, part).start())
            f_twin(t, part).start()
            if part == 0:
                f_over(t, xx).start()
            f_mate(t, part).start()
        when_row(t, body)

    def from_y(owner, part):
        f_twin(owner, part).wait_recv()
        if part == 0:
            f_over(owner, xx).start()
        f_mate(owner, part).start()

    def z_steps(d):
        for part in (0, 1):
            for sign in (-1, 1):
                from_z(d, sign, part)

    def y_steps(d):
        for part in (0, 1):
            for sign in (-1, 1):
                t = r + sign * 2 * d
                when_row(t, lambda: from_y(t + twin - r, part))

    def a2a_copy(q):
        return remote(v.dr.at[pl.ds(W * q, W)], v.a2a.at[r], v.one_s.at[3], v.one_r.at[3],
                      snake(q, c, R), c)

    for q in range(R):
        @pl.when(s != q)
        def _():
            a2a_copy(q).start()

        @pl.when(s == q)
        def _():
            v.a2a[r] = v.dr[pl.ds(W * q, W), :]

    loads["middle"].wait()
    v.mp[c] = packed(v.mid_v, mk)
    loads["skip"].wait()
    cut_rows = tall // 2

    def mid_half(owner, which):
        return v.mp.at[owner, pl.ds(pl.multiple_of(which * cut_rows, UNIT), cut_rows)]

    def skip_rows(owner):
        return v.sw.at[pl.ds(pl.multiple_of(owner * skr, TILE), skr)]

    def mid_copy(ref, n, rr, cc):
        return remote(ref, ref, v.mid_s.at[n], v.mid_r.at[n], rr, cc)

    mid_over = (mid_copy(mid_half(c, y), 0, r, over), mid_copy(skip_rows(c), 1, r, over))
    mid_over_in = (mid_copy(mid_half(over, y), 0, r, over), mid_copy(skip_rows(over), 1, r, over))
    mid_twin = mid_copy(mid_half(over, y), 2, twin, c)
    mid_twin_in = mid_copy(mid_half(over, 1 - y), 2, twin, c)
    mid_mate = (mid_copy(v.mp.at[c], 3, r, mate), mid_copy(skip_rows(c), 4, r, mate),
                mid_copy(v.mp.at[over], 5, r, mate), mid_copy(skip_rows(over), 6, r, mate))
    far = lax.rem(mate + 2, Q)
    mid_mate_in = (mid_copy(v.mp.at[mate], 3, r, mate), mid_copy(skip_rows(mate), 4, r, mate),
                   mid_copy(v.mp.at[far], 5, r, mate), mid_copy(skip_rows(far), 6, r, mate))
    for copy in mid_over + mid_mate[0:2]:
        copy.start()

    loads["in"].wait()
    inw = v.inw[...].astype(F32)
    v.wb[...] = jnp.zeros(v.wb.shape, F32)
    for b in range(3):
        rows = [inw[cin * (3 * a + b) : cin * (3 * a + b + 1), :] for a in range(3)]
        band = jnp.concatenate(rows, axis=0)
        band = jnp.concatenate([jnp.zeros((3 * cin, GAP), F32), band], axis=1)
        for yy in range(R):
            lo, hi = max(0, yy - 1), min(R, yy + 2)
            v.wb[b, lo * cin : hi * cin, yy * CP : (yy + 1) * CP] = (
                band[(lo - yy + 1) * cin : (hi - yy + 1) * cin, :])

    loads["tw"].wait()
    loads["ts"].wait()
    half = FQ // 2
    index = lax.broadcasted_iota(jnp.int32, (1, half), 1).astype(F32)
    angles = timestep[0].astype(F32) * jnp.exp(-math.log(10000.0) * index / half)
    v.part[:, 0:half] = jnp.cos(angles)
    v.part[:, half:FQ] = jnp.sin(angles)
    hidden = silu(jnp.sum(dot(pieces_of(v.part[...]), v.tw[...]), axis=0, keepdims=True))
    tk = time_s.shape[0]
    for q in range(Q):
        @pl.when(c == q)
        def _():
            v.part[...] = hidden[:, q * tk : (q + 1) * tk]
    v.emb[c] = jnp.sum(dot(pieces_of(v.part[...]), v.ts[...]), axis=0, keepdims=True)

    def emb_copy(i, src_c, target):
        return remote(v.emb.at[src_c], v.emb.at[src_c], v.one_s.at[5], v.one_r.at[5], r, target)

    for i in range(1, Q):
        emb_copy(i, c, lax.rem(c + i, Q)).start()

    @pl.when((s != 0) | (c == 0))
    def _():
        v.lat[1] = jnp.zeros(v.lat.shape[1:], BF16)

    @pl.when((s != R - 1) | (c == Q - 1))
    def _():
        v.lat[2] = jnp.zeros(v.lat.shape[1:], BF16)

    def all_of(ref, n):
        return remote(ref, ref, v.one_s.at[n], v.one_r.at[n], twin, c)

    all_of(v.lat.at[0, pl.ds(0, R - 1)], 0).wait_recv()

    @pl.when((s == 0) & (c > 0))
    def _():
        all_of(v.lat.at[1], 1).wait_recv()

    @pl.when((s == R - 1) & (c < Q - 1))
    def _():
        all_of(v.lat.at[2], 2).wait_recv()

    for k in range(3):
        for q in range(R):
            v.latrows[k, cin * q : cin * (q + 1), :] = v.lat[k, q].astype(F32)
    lane = lax.broadcasted_iota(jnp.int32, (R * cin, px), 1)
    base = jnp.where((lane == px - 1) & (s == 0), v.latrows[1], v.latrows[0])
    base = jnp.where((lane == 0) & (s == R - 1), v.latrows[2], base)
    rolled = pltpu.roll(base, lax.rem(px + 1 - W * s, px), 1)
    v.tap[0:LANES, 0 : R * cin] = rolled[:, 0:LANES].T
    total = None
    for b in range(3):
        term = dot(v.tap[b : b + W, 0 : R * cin].astype(BF16), v.wb[b].astype(BF16))
        total = term if total is None else total + term
    v.sk[...] = total.astype(BF16).astype(F32)
    top = low = None
    for q in range(R):
        slab = v.sk[:, q * CP : (q + 1) * CP]
        top = slab if top is None else top + slab
        low = slab * slab if low is None else low + slab * slab
    skip_top = jnp.sum(top, axis=0, keepdims=True)
    skip_low = jnp.sum(low, axis=0, keepdims=True)

    def join(d, k):
        cut = C // LANES * LANES
        return jnp.concatenate(
            [d[:, 0:cut], d[:, cut:CP] + k[:, 0 : CP - cut], k[:, CP - cut : CP]], axis=1)

    def indicator(channels, flip):
        shape = (LANES, channels) if flip else (channels, LANES)
        size = channels // GROUPS
        ch = lax.broadcasted_iota(jnp.int32, shape, 1 if flip else 0)
        g = lax.broadcasted_iota(jnp.int32, shape, 0 if flip else 1)
        return ((ch >= g * size) & (ch < g * size + size)).astype(F32)

    def sum_copy(stage, slot, i, rr, cc):
        return remote(v.sums.at[stage, slot], v.sums.at[stage, slot],
                      v.sum_s.at[stage], v.sum_r.at[stage], rr, cc)

    def reduce_start(stage, top, low):
        channels = top.shape[1]
        both = jnp.concatenate([top, low, jnp.zeros((6, channels), F32)], axis=0)
        res = dot(both, indicator(channels, False), lax.Precision.HIGHEST)
        v.sums[stage, me] = res[0:1] + pltpu.roll(res, GROUPS, 1)[1:2]
        for n, (i, j) in enumerate(others):
            sum_copy(stage, me, n, lax.rem(r + i, R), lax.rem(c + j, Q)).start()

    def sum_all(stage):
        ref = v.sums.at[stage, pl.ds(0, R * Q - 1)]
        return remote(ref, ref, v.sum_s.at[stage], v.sum_r.at[stage], twin, c)

    def reduce_end(stage, channels):
        sum_all(stage).wait_recv()
        total = jnp.sum(v.sums[stage], axis=0) / (channels // GROUPS * image)
        spread = pltpu.roll(total, LANES - GROUPS, 1) - total * total
        inverse = lax.rsqrt(jnp.maximum(spread, 0.0) + EPS)
        both = jnp.concatenate([total, inverse, jnp.zeros((6, LANES), F32)], axis=0)
        both = jnp.where(lax.broadcasted_iota(jnp.int32, (8, LANES), 1) < GROUPS, both, 0.0)
        wide = dot(both, indicator(channels, True), lax.Precision.HIGHEST)
        return wide[0:1], wide[1:2]

    reduce_start(0, join(deep_top, skip_top), join(deep_low, skip_low))

    inner = (s + R - 1) // R
    last = (s + 1) // R
    left = (inner * snake(s - 1, c, R) + (1 - inner) * r, c - (1 - inner))
    right = ((1 - last) * snake(s + 1, c, R) + last * r, c + last)
    has_left, has_right = left[1] >= 0, right[1] < Q

    def halo_left(stage, ext):
        return remote(ext.at[:, pl.ds(8, 8)], ext.at[:, pl.ds(N + 8, 8)],
                      v.halo_s.at[stage, 0], v.halo_r.at[stage, 1], left[0], left[1])

    def halo_right(stage, ext):
        return remote(ext.at[:, pl.ds(N, 8)], ext.at[:, pl.ds(0, 8)],
                      v.halo_s.at[stage, 1], v.halo_r.at[stage, 0], right[0], right[1])

    def halo_send(stage, ext):
        zeros = jnp.zeros((ext.shape[0], 8, LANES), F32)

        @pl.when(has_left)
        def _():
            halo_left(stage, ext).start()

        @pl.when(has_right)
        def _():
            halo_right(stage, ext).start()

        @pl.when(jnp.logical_not(has_left))
        def _():
            ext[:, 0:8, :] = zeros

        @pl.when(jnp.logical_not(has_right))
        def _():
            ext[:, N + 8 : N + 16, :] = zeros

    def halo_wait(stage, ext):
        @pl.when(has_left)
        def _():
            halo_right(stage, ext).wait_recv()

        @pl.when(has_right)
        def _():
            halo_left(stage, ext).wait_recv()

    z_steps(1)
    for part in (0, 1):
        from_y(twin, part)

    all_of(v.a2a.at[pl.ds(0, R - 1)], 3).wait_recv()
    for q in range(R):
        joined = join(v.a2a[q].astype(F32), v.sk[:, q * CP : (q + 1) * CP])
        for n in range(2 * C // LANES):
            v.jx[n, pl.ds(8 + q, W, 8), :] = joined[:, n * LANES : (n + 1) * LANES]
    halo_send(0, v.jx)
    z_steps(2)
    y_steps(1)
    for d in range(3, R // 2):
        z_steps(d)
        y_steps(d - 1)
    y_steps(R // 2 - 1)
    for copy in mid_over_in:
        copy.wait_recv()
    for copy in (mid_twin, mid_mate[3]):
        copy.start()

    loads["out"].wait()
    loads["tp"].wait()
    for name in ("gain_one", "gain_two", "gain_three"):
        loads[name].wait()
    v.wr32[...] = jnp.zeros(v.wr32.shape, F32)
    for t in range(9):
        v.wr32[couts * t : couts * (t + 1), :] = v.outw_v[:, C * t : C * (t + 1)].astype(F32)
    out_taps = v.wr32[...].T.astype(BF16)

    all_of(v.emb.at[pl.ds(0, Q - 1)], 5).wait_recv()
    embedded = jnp.sum(v.emb[...], axis=0)
    time_shift = jnp.sum(dot_nt(pieces_of(silu(embedded)), v.tp[...]), axis=0, keepdims=True)

    place = lax.broadcasted_iota(jnp.int32, (W + 2, 8, 1), 0)
    inside = (
        ((place > 0) | has_left) & ((place < W + 1) | has_right))
    row = lax.broadcasted_iota(jnp.int32, (W + 2, 8, 1), 1)

    def keep_own(ext, values):
        for n in range(ext.shape[0]):
            lo, hi = n * LANES, min((n + 1) * LANES, values.shape[1])
            ext[n, 8 : N + 8, 0 : hi - lo] = values[:, lo:hi]

    def rows_of(ext, channels, first, count):
        return jnp.concatenate(
            [ext[n, first : first + count, 0 : min(LANES, channels - n * LANES)]
             for n in range(ext.shape[0])], axis=1)

    def activate(ext, stats, gain):
        center, inverse = stats
        scale = inverse * gain
        channels = gain.shape[1]
        for lo in range(0, channels, LANES):
            hi = min(channels, lo + LANES)
            z = silu((ext[lo // LANES, :, 0 : hi - lo] - center[:, lo:hi]) * scale[:, lo:hi])
            z = jnp.where(inside, z.reshape(W + 2, 8, hi - lo), 0.0)
            for a in range(3):
                if a == 1:
                    moved = z
                elif a == 0:
                    moved = jnp.where(row > 0, pltpu.roll(z, 1, 1), 0.0)
                else:
                    moved = jnp.where(row < 7, pltpu.roll(z, 7, 1), 0.0)
                flat = moved.reshape(N + 16, hi - lo)
                v.act_a[a, :, lo:hi] = flat.astype(BF16)
                v.act_b[a, :, lo:hi] = flat[8 : N + 8].astype(BF16)

    def conv(channels, weight):
        total = None
        for a in range(3):
            for b in range(3):
                if b == 1:
                    act = v.act_b[a, :, 0:channels]
                else:
                    act = v.act_a[a, 8 * b : 8 * b + N, 0:channels]
                k = (3 * a + b) * channels
                term = dot(act, weight[k : k + channels, 0:C])
                total = term if total is None else total + term
        return total

    stats = reduce_end(0, 2 * C)
    halo_wait(0, v.jx)
    activate(v.jx, stats, v.gain_one[...].reshape(1, 2 * C))

    owners = [(lax.rem(r + i, R)) for i in range(1, R)]
    for owner in owners:
        f_over(owner, 1 - xx).wait_recv()
        f_mate_extra(owner).start()
    mate_rows = v.fp.at[pl.ds(0, R - 1), pl.ds(0, share * UNIT)]
    all_of(mate_rows, 10).wait_recv()
    for owner in range(R):
        unpack(v.fp[owner], v.fw, owner * fk)

    hidden_one = conv(2 * C, v.fw) + time_shift
    keep_own(v.hx, hidden_one)
    reduce_start(1, jnp.sum(hidden_one, axis=0, keepdims=True),
                 jnp.sum(hidden_one * hidden_one, axis=0, keepdims=True))
    halo_send(1, v.hx)

    mid_twin_in.wait_recv()
    mid_mate[2].start()
    for copy in mid_mate_in:
        copy.wait_recv()
    for owner in range(Q):
        unpack(v.mp[owner], v.mw, owner * mk)
    shortcut = dot(rows_of(v.jx, 2 * C, 8, N).astype(BF16), v.sw[...])
    stats = reduce_end(1, C)
    halo_wait(1, v.hx)
    activate(v.hx, stats, v.gain_two[...].reshape(1, C))
    block_out = conv(C, v.mw) + shortcut

    keep_own(v.ox, block_out)
    reduce_start(2, jnp.sum(block_out, axis=0, keepdims=True),
                 jnp.sum(block_out * block_out, axis=0, keepdims=True))
    halo_send(2, v.ox)
    stats = reduce_end(2, C)
    halo_wait(2, v.ox)

    center, inverse = stats
    z = silu((rows_of(v.ox, C, 0, N + 16) - center) * (inverse * v.gain_three[...].reshape(1, C)))
    z = jnp.where(inside, z.reshape(W + 2, 8, C), 0.0).reshape(N + 16, C)
    spread = dot(z.astype(BF16), out_taps)
    lane = lax.broadcasted_iota(jnp.int32, (N, LANES), 1)
    row = lax.broadcasted_iota(jnp.int32, (W, 8, 1), 1)
    total = None
    for a in range(3):
        got = None
        for b in range(3):
            t = couts * (3 * a + b)
            here = jnp.where(
                (lane >= t) & (lane < t + couts), spread[8 * b : 8 * b + N, :], 0.0)
            got = here if got is None else got + here
        got = got.reshape(W, 8, LANES)
        if a == 0:
            got = jnp.where(row > 0, pltpu.roll(got, 1, 1), 0.0)
        elif a == 2:
            got = jnp.where(row < 7, pltpu.roll(got, 7, 1), 0.0)
        total = got if total is None else total + got
    v.tap[...] = total.reshape(N, LANES)
    ordered = jnp.concatenate([v.tap[pl.ds(q, W, 8), :] for q in range(R)], axis=0)
    fold = (lax.rem(lax.broadcasted_iota(jnp.int32, (8, LANES), 1), couts)
            == lax.broadcasted_iota(jnp.int32, (8, LANES), 0)).astype(F32)
    rows = dot_nt(fold, ordered, lax.Precision.HIGHEST)[0:couts]
    for q in range(R):
        v.outs[q, :, 0:W] = rows[:, W * q : W * (q + 1)]

    def out_copy(q, rr):
        return remote(v.outs.at[q], v.outr.at[s], v.one_s.at[4], v.one_r.at[4], rr, c)

    for q in range(R):
        @pl.when(r != q)
        def _():
            out_copy(q, q).start()

        @pl.when(r == q)
        def _():
            v.outr[s] = v.outs[q]

    all_of(v.outr.at[pl.ds(0, R - 1)], 4).wait_recv()
    for q in range(R):
        noise[:, W * q : W * (q + 1)] = v.outr[q, :, 0:W]

    all_of(v.lat.at[0, pl.ds(0, R - 1)], 0).wait_send()

    @pl.when(c > 0)
    def _():
        lat_left().wait_send()

    @pl.when(c < Q - 1)
    def _():
        lat_right().wait_send()

    all_of(v.a2a.at[pl.ds(0, R - 1)], 3).wait_send()
    all_of(v.outr.at[pl.ds(0, R - 1)], 4).wait_send()
    all_of(v.emb.at[pl.ds(0, Q - 1)], 5).wait_send()
    for stage, ext in enumerate((v.jx, v.hx, v.ox)):
        sum_all(stage).wait_send()

        @pl.when(has_left)
        def _():
            halo_left(stage, ext).wait_send()

        @pl.when(has_right)
        def _():
            halo_right(stage, ext).wait_send()
    for copy in mid_over + (mid_twin,) + mid_mate:
        copy.wait_send()
    moved = (share - ALONE) * UNIT
    level = r // 2
    for count in range(1, R // 2):
        @pl.when(level == count - 1)
        def _():
            all_of(v.fp.at[pl.ds(0, count), pl.ds(0, moved)], 6).wait_send()

        @pl.when(level == R // 2 - count)
        def _():
            all_of(v.fp.at[pl.ds(0, count), pl.ds(0, moved)], 7).wait_send()

    all_of(v.fp.at[pl.ds(0, R // 2), pl.ds(0, moved)], 8).wait_send()
    all_of(v.fp.at[pl.ds(0, R - 1), pl.ds(0, ALONE * UNIT)], 9).wait_send()
    all_of(mate_rows, 10).wait_send()


def fast_shards(
    R, Q,
    latent, deep, timestep, in_weight, front_weight, middle_weight, skip_weight, out_weight,
    time_weight, time_second, time_proj, input_gain, middle_gain, output_gain,
):
    C = deep.shape[0]
    cin = latent.shape[0]
    px = deep.shape[1] * deep.shape[2]
    couts = out_weight.shape[1]
    W = px // R
    N = W * 8
    CP = (C + LANES - 1) // LANES * LANES
    fk, mk, skr = front_weight.shape[0], middle_weight.shape[0], skip_weight.shape[0]
    hbm = pl.BlockSpec(memory_space=pl.ANY)
    vmem = pl.BlockSpec(memory_space=pltpu.VMEM)
    smem = pl.BlockSpec(memory_space=pltpu.SMEM)
    dma = pltpu.SemaphoreType.DMA
    args = (
        latent.reshape(cin, px), deep.reshape(C, px), timestep, in_weight, front_weight.T,
        middle_weight.T, skip_weight, out_weight.T, time_weight, time_second, time_proj.T,
        input_gain, middle_gain, output_gain,
    )
    fq, wide = time_weight.shape
    shapes = dict(
        lat_v=pltpu.VMEM((cin, px), BF16), lat=pltpu.VMEM((3, R, cin, px), BF16),
        latrows=pltpu.VMEM((3, R * cin, px), F32), deep_v=pltpu.VMEM((C, px), BF16),
        dr=pltpu.VMEM((px, CP), BF16), a2a=pltpu.VMEM((R, W, CP), BF16),
        inw=pltpu.VMEM((9 * cin, C), BF16), wb=pltpu.VMEM((3, R * cin, R * CP), F32),
        sk=pltpu.VMEM((W, R * CP), F32), jx=pltpu.VMEM((2 * C // LANES, N + 16, LANES), F32),
        hx=pltpu.VMEM((CP // LANES, N + 16, LANES), F32),
        ox=pltpu.VMEM((CP // LANES, N + 16, LANES), F32),
        act_a=pltpu.VMEM((3, N + 16, 2 * C), BF16), act_b=pltpu.VMEM((3, N, 2 * C), BF16),
        front_v=pltpu.VMEM((C, fk), BF16), fw=pltpu.VMEM((18 * C, CP), BF16),
        fp=pltpu.VMEM((R, PACK * UNIT, 2 * C), BF16), mp=pltpu.VMEM((Q, PACK * UNIT, 2 * C), BF16),
        mid_v=pltpu.VMEM((C, mk), BF16), mw=pltpu.VMEM((9 * C, CP), BF16),
        sw=pltpu.VMEM((2 * C, C), BF16), outw_v=pltpu.VMEM((couts, 9 * C), BF16),
        wr32=pltpu.VMEM((LANES, C), F32), tw=pltpu.VMEM((fq, wide), BF16),
        ts=pltpu.VMEM(time_second.shape, BF16), tp=pltpu.VMEM((C, wide), BF16),
        part=pltpu.VMEM((1, fq), F32), emb=pltpu.VMEM((Q, 1, wide), F32),
        sums=pltpu.VMEM((3, R * Q, 1, LANES), F32), tap=pltpu.VMEM((N, LANES), F32),
        outs=pltpu.VMEM((R, couts, LANES), F32), outr=pltpu.VMEM((R, couts, LANES), F32),
        gain_one=pltpu.VMEM((2 * C,), F32), gain_two=pltpu.VMEM((C,), F32),
        gain_three=pltpu.VMEM((C,), F32),
        ld_s=dma((13,)), one_s=dma((11,)), one_r=dma((11,)), halo_s=dma((3, 2)), halo_r=dma((3, 2)),
        fm_r=dma((2, R)), fx_r=dma((R,)), mid_s=dma((7,)), mid_r=dma((7,)),
        sum_s=dma((3,)), sum_r=dma((3,)),
    )
    specs = [hbm] * len(args)
    specs[2] = smem
    out = pl.pallas_call(
        functools.partial(fast_kernel, R, Q, tuple(shapes)),
        out_shape=jax.ShapeDtypeStruct((couts, px), F32),
        in_specs=specs,
        out_specs=vmem,
        scratch_shapes=list(shapes.values()),
        compiler_params=pltpu.CompilerParams(
            collective_id=0, has_side_effects=True, vmem_limit_bytes=56 * 1024 * 1024
        ),
    )(*args)
    return out.reshape(couts, 1, px)


def solution(mesh):
    R, Q = mesh.shape["rows"], mesh.shape["cols"]

    def body(*args):
        deep, front = args[1], args[4]
        fits = (
            R == 8 and Q == 4 and deep.shape[1] == 1 and deep.shape[2] % (R * LANES // 4) == 0
            and front.shape[0] % UNIT == 0
            and PACK * UNIT < front.shape[0] <= 2 * PACK * UNIT
            and args[5].shape[0] == front.shape[0] and deep.shape[0] % LANES * 2 == LANES)
        return (fast_shards if fits else shards)(R, Q, *args)

    return jax.shard_map(
        body,
        mesh=mesh,
        in_specs=(
            P(None, "rows", "cols"), P(None, "rows", "cols"), P(), P(),
            P("rows", None), P("cols", None), P("cols", None), P(),
            P(), P("cols", None), P(), P(), P(), P(),
        ),
        out_specs=P(None, "rows", "cols"),
        check_vma=False,
    )
```

```python
import functools
import math

import jax
import jax.numpy as jnp
from jax import lax
from jax.experimental import pallas as pl
from jax.experimental.pallas import tpu as pltpu
from jax.sharding import PartitionSpec as P

GROUPS = 32
EPS = 1e-05
TILE = 16
LANES = 128
MESH = pl.DeviceIdType.MESH
F32 = jnp.float32
BF16 = jnp.bfloat16
SIDES = tuple((i, j) for i in (-1, 0, 1) for j in (-1, 0, 1) if (i, j) != (0, 0))


def dot(a, b, precision=None):
    return lax.dot_general(
        a, b, (((1,), (0,)), ((), ())), preferred_element_type=F32, precision=precision
    )


def split_dot(row, weight):
    high = row.astype(BF16)
    rest = row - high.astype(F32)
    middle = rest.astype(BF16)
    low = (rest - middle.astype(F32)).astype(BF16)
    pieces = jnp.concatenate([high.astype(F32), middle.astype(F32), low.astype(F32)], axis=0)
    return jnp.sum(dot(pieces.astype(BF16), weight), axis=0, keepdims=True)


def silu(z):
    return z / (1.0 + jnp.exp(-z))


def kernel(
    R, Q, ring,
    latent, deep, rows_in, in_w, front, middle, skip, out_w, time_w, time_s, time_p,
    noise,
    lat, jext, hext, oext, shifted, patch, fw, mw, sw, part, emb, sums_a, sums_b,
    lat_s, lat_r, halo_s, halo_r, fz_s, fy_s, fc_s, fm_r, fo_r, mid_s, mid_r, emb_s, emb_r,
    ca_s, ca_r, cb_s, cb_r, loc_s,
):
    r = lax.axis_index("rows")
    c = lax.axis_index("cols")
    C, px = deep.shape
    cin = latent.shape[0]
    image = float(px * R * Q)
    FQ = time_w.shape[0]
    gain_one = rows_in[:, FQ : FQ + 2 * C]
    gain_two = rows_in[:, FQ + 2 * C : FQ + 3 * C]
    gain_three = rows_in[:, FQ + 3 * C : FQ + 4 * C]

    def remote(src, dst, ssem, rsem, rr, cc):
        return pltpu.make_async_remote_copy(
            src_ref=src, dst_ref=dst, send_sem=ssem, recv_sem=rsem,
            device_id={"rows": rr, "cols": cc}, device_id_type=MESH,
        )

    def each(count, body):
        if count <= 8:
            for i in range(1, count):
                body(i)
        else:
            lax.fori_loop(1, count, lambda i, u: (body(i), u)[1], 0)

    barrier = pltpu.get_barrier_semaphore()

    def greet(rr, cc):
        pl.semaphore_signal(barrier, inc=1, device_id={"rows": rr, "cols": cc}, device_id_type=MESH)

    each(R, lambda i: greet(lax.rem(r + i, R), c))
    each(Q, lambda i: greet(r, lax.rem(c + i, Q)))
    for i in (-1, 1):
        for j in (-1, 1):
            greet(lax.rem(r + i + R, R), lax.rem(c + j + Q, Q))
    pl.semaphore_wait(barrier, R - 1 + Q - 1 + 4)

    def inside(rr, cc):
        return (rr >= 0) & (rr < R) & (cc >= 0) & (cc < Q)

    def lat_copy(k, rr, cc):
        i, j = SIDES[k]
        return remote(latent, lat.at[k], lat_s.at[k], lat_r.at[k], rr, cc)

    for k, (i, j) in enumerate(SIDES):
        @pl.when(inside(r + i, c + j))
        def _():
            lat_copy(k, r + i, c + j).start()

        @pl.when(jnp.logical_not(inside(r - i, c - j)))
        def _():
            lat[k] = jnp.zeros(lat.shape[1:], lat.dtype)

    parity = lax.rem(c, 2)
    mate = c + 1 - 2 * parity
    over = lax.rem(c + 2, Q)
    half_c = lax.rem(r, 2)
    twin = r + 1 - 2 * half_c
    mk, sk = middle.shape[0], skip.shape[0]

    def mid_copies(owner, s, slot_from, target):
        rows_m = pl.ds(pl.multiple_of(owner * mk, TILE), mk)
        rows_s = pl.ds(pl.multiple_of(owner * sk, TILE), sk)
        src_m, src_s = (middle, skip) if slot_from else (mw.at[rows_m], sw.at[rows_s])
        return (
            remote(src_m, mw.at[rows_m], mid_s.at[0, s], mid_r.at[0, s], r, target),
            remote(src_s, sw.at[rows_s], mid_s.at[1, s], mid_r.at[1, s], r, target),
        )

    fk = fw.shape[0] // R if ring else 0
    cut = fk // 2 // TILE * TILE
    spans = ((0, cut), (cut, fk - cut))

    def f_rows(owner, par):
        return pl.ds(pl.multiple_of(owner * fk, TILE) + spans[par][0], spans[par][1])

    def by_parity(par_of, body):
        for par in (0, 1):
            @pl.when(par_of == par)
            def _():
                body(par)

    def f_own(par, target, ssem):
        src = front.at[pl.ds(spans[par][0], spans[par][1])]
        return remote(src, fw.at[f_rows(r, par)], ssem, fm_r.at[r], target, c)

    def f_pass(owner, par, target):
        return remote(fw.at[f_rows(owner, par)], fw.at[f_rows(owner, par)],
                      fy_s.at[owner], fm_r.at[owner], target, c)

    def f_mate(owner, par):
        return remote(fw.at[f_rows(owner, par)], fw.at[f_rows(owner, par)],
                      fc_s.at[owner], fo_r.at[owner], r, mate)

    def by_distance(distances, body):
        for d in distances:
            for t in (r + 2 * d, r - 2 * d):
                @pl.when((t >= 0) & (t < R))
                def _():
                    body(t)

    locals_ = []
    if ring:
        locals_.append(pltpu.make_async_copy(
            front, fw.at[pl.ds(pl.multiple_of(r * fk, TILE), fk)], loc_s.at[0]))
    locals_.append(pltpu.make_async_copy(
        middle, mw.at[pl.ds(pl.multiple_of(c * mk, TILE), mk)], loc_s.at[1]))
    locals_.append(pltpu.make_async_copy(
        skip, sw.at[pl.ds(pl.multiple_of(c * sk, TILE), sk)], loc_s.at[2]))
    for copy in locals_:
        copy.start()

    if ring:
        def first(par):
            f_own(par, twin, fy_s.at[r]).start()
            def one(t):
                f_own(par, t, fz_s.at[t]).start()
            by_distance(range(1, R // 2), one)
        by_parity(parity, first)
    for copy in mid_copies(c, 0, True, over) + mid_copies(c, 1, True, mate):
        copy.start()

    def pass_on(distances):
        def go(par):
            def one(owner):
                f_pass(owner, par, twin).wait_recv()
                f_pass(owner, par, twin).start()
                f_mate(owner, par).start()
            by_distance(distances, one)
        by_parity(parity, go)

    for k, (i, j) in enumerate(SIDES):
        @pl.when(inside(r - i, c - j))
        def _():
            lat_copy(k, r - i, c - j).wait_recv()
    where = {side: k for k, side in enumerate(SIDES)}
    for a in range(3):
        tiles = []
        for b in range(3):
            side = (1 - a, 1 - b)
            block = latent[...] if side == (0, 0) else lat[where[side]]
            tiles.append(block.astype(F32))
        wide = jnp.concatenate(tiles, axis=1)
        for b in range(3):
            start = px + b - 1
            patch[cin * (3 * a + b) : cin * (3 * a + b + 1), :] = wide[:, start : start + px]
    skip_feat = dot(patch[...].T.astype(BF16), in_w[...]).astype(BF16)
    deep_t = deep[...].astype(F32).T.astype(BF16)
    own = pl.ds(TILE, px)
    jext[1, own, :] = jnp.concatenate([deep_t.astype(F32), skip_feat.astype(F32)], axis=1).astype(BF16)

    def halo_copy(stage, ext, k, rr, cc):
        i, j = SIDES[k]
        src = ((TILE, TILE), (TILE, px), (px, TILE))[j + 1]
        dst = ((TILE + px, TILE), (TILE, px), (0, TILE))[j + 1]
        return remote(ext.at[1, pl.ds(*src), :], ext.at[1 - i, pl.ds(*dst), :],
                      halo_s.at[stage, k], halo_r.at[stage, k], rr, cc)

    def halo_send(stage, ext):
        for k, (i, j) in enumerate(SIDES):
            @pl.when(inside(r + i, c + j))
            def _():
                halo_copy(stage, ext, k, r + i, c + j).start()

            @pl.when(jnp.logical_not(inside(r - i, c - j)))
            def _():
                dst = ((TILE + px, TILE), (TILE, px), (0, TILE))[j + 1]
                ext[1 - i, pl.ds(*dst), :] = jnp.zeros((dst[1], ext.shape[2]), ext.dtype)

    def halo_wait(stage, ext):
        for k, (i, j) in enumerate(SIDES):
            @pl.when(inside(r - i, c - j))
            def _():
                halo_copy(stage, ext, k, r - i, c - j).wait_recv()

    def indicator(channels, flip):
        shape = (LANES, channels) if flip else (channels, LANES)
        size = channels // GROUPS
        ch = lax.broadcasted_iota(jnp.int32, shape, 1 if flip else 0)
        g = lax.broadcasted_iota(jnp.int32, shape, 0 if flip else 1)
        return ((ch >= g * size) & (ch < g * size + size)).astype(F32)

    def sum_copy(buf, ssem, rsem, stage, slot, i, rr, cc):
        return remote(buf.at[stage, slot], buf.at[stage, slot],
                      ssem.at[stage, i], rsem.at[stage, i], rr, cc)

    def reduce_start(stage, values):
        top = jnp.sum(values, axis=0, keepdims=True)
        low = jnp.sum(values * values, axis=0, keepdims=True)
        both = jnp.concatenate([top, low, jnp.zeros((6, values.shape[1]), F32)], axis=0)
        sums_a[stage, c] = dot(both, indicator(values.shape[1], False), lax.Precision.HIGHEST)
        for i in range(1, Q):
            sum_copy(sums_a, ca_s, ca_r, stage, c, i, r, lax.rem(c + i, Q)).start()

    def reduce_end(stage, channels):
        for i in range(1, Q):
            s = lax.rem(c + Q - i, Q)
            sum_copy(sums_a, ca_s, ca_r, stage, s, i, r, s).wait_recv()
        sums_b[stage, r] = jnp.sum(sums_a[stage], axis=0)
        each(R, lambda i: sum_copy(sums_b, cb_s, cb_r, stage, r, i, lax.rem(r + i, R), c).start())

        def got(i):
            s = lax.rem(r + R - i, R)
            sum_copy(sums_b, cb_s, cb_r, stage, s, i, s, c).wait_recv()

        each(R, got)
        total = jnp.sum(sums_b[stage], axis=0) / (channels // GROUPS * image)
        center = total[0:1]
        inverse = lax.rsqrt(total[1:2] - center * center + EPS)
        both = jnp.concatenate([center, inverse, jnp.zeros((6, LANES), F32)], axis=0)
        wide = dot(both, indicator(channels, True), lax.Precision.HIGHEST)
        return wide[0:1], wide[1:2]

    def conv(ext, stats, gain, weight, exact=None, shift=None):
        center, inverse = stats
        if shift is not None:
            center = center - shift
        channels = ext.shape[2]
        scale = inverse * gain
        place = lax.broadcasted_iota(jnp.int32, (px + 2 * TILE, 1), 0)
        inner = (place >= TILE) & (place < TILE + px)
        total = None
        for a in (1, 0, 2):
            z = (ext[a].astype(F32) - center) * scale
            here = r + a - 1
            keep = (here >= 0) & (here < R) & (
                inner | ((place < TILE) & (c > 0)) | ((place >= TILE + px) & (c < Q - 1)))
            shifted[:, 0:channels] = jnp.where(keep, silu(z), 0.0)
            if a == 1 and exact is not None:
                shifted[own, 0:channels] = silu((exact - center) * scale)
            for b in range(3):
                act = shifted[TILE + b - 1 : TILE + b - 1 + px, 0:channels].astype(BF16)
                k = (3 * a + b) * channels
                term = dot(act, weight[k : k + channels, :])
                total = term if total is None else total + term
        return total

    joined = jext[1, own, :]
    reduce_start(0, joined.astype(F32))
    halo_send(0, jext)

    hidden = silu(split_dot(rows_in[:, 0:FQ], time_w[...]))
    tk = time_s.shape[0]
    for q in range(Q):
        @pl.when(c == q)
        def _():
            part[...] = hidden[:, q * tk : (q + 1) * tk]
    emb_own = split_dot(part[...], time_s[...])
    emb[c] = emb_own

    def emb_copy(i, src_c, tgt):
        return remote(emb.at[src_c], emb.at[src_c], emb_s.at[i], emb_r.at[i], r, tgt)

    for i in range(1, Q):
        emb_copy(i, c, lax.rem(c + i, Q)).start()

    if ring:
        pass_on((1,))
    stats = reduce_end(0, 2 * C)
    if ring:
        pass_on(range(2, R // 2))

        def from_twin(par):
            def one(t):
                owner = t + twin - r
                f_pass(owner, par, twin).wait_recv()
                f_mate(owner, par).start()
            one(r)
            by_distance(range(1, R // 2), one)
        by_parity(parity, from_twin)

    for copy in mid_copies(over, 0, False, over):
        copy.wait_recv()
    for copy in mid_copies(over, 2, False, mate):
        copy.start()

    for i in range(1, Q):
        s = lax.rem(c + Q - i, Q)
        emb_copy(i, s, s).wait_recv()
    embedded = jnp.sum(emb[...], axis=0)
    time_shift = split_dot(silu(embedded), time_p[...])

    for copy in locals_:
        copy.wait()
    halo_wait(0, jext)
    if ring:
        def from_mate(i):
            owner = lax.rem(r + i, R)
            def go(par):
                f_mate(owner, 1 - par).wait_recv()
            by_parity(parity, go)
        for i in range(1, R):
            from_mate(i)
    front_out = conv(jext, stats, gain_one, fw if ring else front)

    hext[1, own, :] = front_out.astype(BF16)
    reduce_start(1, front_out + time_shift)
    halo_send(1, hext)
    for copy in mid_copies(mate, 1, False, mate):
        copy.wait_recv()
    far = lax.rem(mate + 2, Q)
    for copy in mid_copies(far, 2, False, mate):
        copy.wait_recv()
    shortcut = dot(joined, sw[...])
    stats = reduce_end(1, C)
    halo_wait(1, hext)
    block_out = conv(hext, stats, gain_two, mw, front_out, time_shift) + shortcut

    oext[1, own, :] = block_out.astype(BF16)
    reduce_start(2, block_out)
    halo_send(2, oext)
    stats = reduce_end(2, C)
    halo_wait(2, oext)
    result = conv(oext, stats, gain_three, out_w, block_out)
    noise[...] = result.T[0 : noise.shape[0], :]

    for k, (i, j) in enumerate(SIDES):
        @pl.when(inside(r + i, c + j))
        def _():
            lat_copy(k, r + i, c + j).wait_send()
            for stage, ext in enumerate((jext, hext, oext)):
                halo_copy(stage, ext, k, r + i, c + j).wait_send()
    for i in range(1, Q):
        emb_copy(i, c, lax.rem(c + i, Q)).wait_send()
        for stage in range(3):
            sum_copy(sums_a, ca_s, ca_r, stage, c, i, r, lax.rem(c + i, Q)).wait_send()

    def sent(i):
        for stage in range(3):
            sum_copy(sums_b, cb_s, cb_r, stage, r, i, lax.rem(r + i, R), c).wait_send()

    each(R, sent)
    for copy in (mid_copies(c, 0, True, over) + mid_copies(c, 1, True, mate)
                 + mid_copies(over, 2, False, mate)):
        copy.wait_send()
    if ring:
        def last(par):
            f_own(par, twin, fy_s.at[r]).wait_send()
            def one(t):
                f_own(par, t, fz_s.at[t]).wait_send()
                f_pass(t, par, twin).wait_send()
            by_distance(range(1, R // 2), one)
            for i in range(1, R):
                f_mate(lax.rem(r + i, R), par).wait_send()
        by_parity(parity, last)


def shards(
    R, Q,
    latent, deep, timestep, in_weight, front_weight, middle_weight, skip_weight, out_weight,
    time_weight, time_second, time_proj, input_gain, middle_gain, output_gain,
):
    C = deep.shape[0]
    cin = latent.shape[0]
    px = deep.shape[1] * deep.shape[2]
    assert deep.shape[1] == 1 and Q == 4 and R % 2 == 0 and R > 2
    ring = R <= 8 and front_weight.shape[0] % TILE == 0
    half = time_weight.shape[0] // 2
    ratios = jnp.exp(-math.log(10000.0) * jnp.arange(half, dtype=F32) / half)
    angles = timestep[0].astype(F32) * ratios
    rows_in = jnp.concatenate(
        [jnp.cos(angles), jnp.sin(angles), input_gain, middle_gain, output_gain])[None, :]
    front = front_weight if ring else lax.all_gather(front_weight, "rows", axis=0, tiled=True)
    couts = out_weight.shape[1]
    out_w = jnp.pad(out_weight, ((0, 0), (0, LANES - couts)))
    vmem = pl.BlockSpec(memory_space=pltpu.VMEM)
    dma = pltpu.SemaphoreType.DMA
    wide = time_second.shape[1]
    tall = px + 2 * TILE
    args = (
        latent.reshape(cin, px), deep.reshape(C, px), rows_in, in_weight, front,
        middle_weight, skip_weight, out_w, time_weight, time_second, time_proj,
    )
    out = pl.pallas_call(
        functools.partial(kernel, R, Q, ring),
        out_shape=jax.ShapeDtypeStruct((couts, px), F32),
        in_specs=[vmem] * len(args),
        out_specs=vmem,
        scratch_shapes=[
            pltpu.VMEM((8, cin, px), BF16),
            pltpu.VMEM((3, tall, 2 * C), BF16),
            pltpu.VMEM((3, tall, C), BF16),
            pltpu.VMEM((3, tall, C), BF16),
            pltpu.VMEM((tall, 2 * C), F32),
            pltpu.VMEM((9 * cin, px), F32),
            pltpu.VMEM((18 * C if ring else TILE, C), BF16),
            pltpu.VMEM((9 * C, C), BF16),
            pltpu.VMEM((2 * C, C), BF16),
            pltpu.VMEM((1, time_second.shape[0]), F32),
            pltpu.VMEM((Q, 1, wide), F32),
            pltpu.VMEM((3, Q, 8, LANES), F32),
            pltpu.VMEM((3, R, 8, LANES), F32),
            dma((8,)), dma((8,)), dma((3, 8)), dma((3, 8)),
            dma((R,)), dma((R,)), dma((R,)), dma((R,)), dma((R,)),
            dma((2, 3)), dma((2, 3)), dma((Q,)), dma((Q,)),
            dma((3, Q)), dma((3, Q)), dma((3, R)), dma((3, R)), dma((3,)),
        ],
        compiler_params=pltpu.CompilerParams(
            collective_id=0, has_side_effects=True, vmem_limit_bytes=56 * 1024 * 1024
        ),
    )(*args)
    return out.reshape(couts, 1, px)


UNIT = 16
PACK = 24
ALONE = 3


class Box:
    pass


def snake(pos, c, R):
    q = pos + lax.rem(c, 2) * (R - 1 - 2 * pos)
    late = q // (R // 2)
    return (1 - late) * (2 * q) + late * (2 * (R - 1 - q) + 1)


def place_of(r, c, R):
    odd, h = lax.rem(r, 2), r // 2
    q = (1 - odd) * h + odd * (R - 1 - h)
    return q + lax.rem(c, 2) * (R - 1 - 2 * q)


def dot_nt(a, b, precision=None):
    return lax.dot_general(
        a, b, (((1,), (1,)), ((), ())), preferred_element_type=F32, precision=precision
    )


def pieces_of(row):
    high = row.astype(BF16)
    rest = row - high.astype(F32)
    middle = rest.astype(BF16)
    low = (rest - middle.astype(F32)).astype(BF16)
    return jnp.concatenate(
        [high.astype(F32), middle.astype(F32), low.astype(F32)], axis=0).astype(BF16)


def fast_kernel(
    R, Q, names,
    latent, deep, timestep, in_w, front, middle, skip, out_w, time_w, time_s, time_p,
    input_gain, middle_gain, output_gain, noise, *scratch,
):
    v = Box()
    for name, ref in zip(names, scratch):
        setattr(v, name, ref)
    r = lax.axis_index("rows")
    c = lax.axis_index("cols")
    C, px = deep.shape
    cin = latent.shape[0]
    couts = out_w.shape[0]
    image = float(px * R * Q)
    FQ = time_w.shape[0]
    W = px // R
    N = W * 8
    s = place_of(r, c, R)
    me = c * R + r
    CP = (C + LANES - 1) // LANES * LANES
    GAP = CP - C

    def remote(src, dst, ssem, rsem, rr, cc):
        return pltpu.make_async_remote_copy(
            src_ref=src, dst_ref=dst, send_sem=ssem, recv_sem=rsem,
            device_id={"rows": rr, "cols": cc}, device_id_type=MESH,
        )

    others = [(i, j) for i in range(R) for j in range(Q) if (i, j) != (0, 0)]
    barrier = pltpu.get_barrier_semaphore()
    for i, j in others:
        pl.semaphore_signal(
            barrier, inc=1, device_id={"rows": lax.rem(r + i, R), "cols": lax.rem(c + j, Q)},
            device_id_type=MESH)

    mk, skr, fk = middle.shape[1], skip.shape[0], front.shape[1]
    loads = {}
    for k, (name, src, dst) in enumerate((
        ("front", front, v.front_v), ("latent", latent, v.lat_v), ("deep", deep, v.deep_v),
        ("in", in_w, v.inw), ("tw", time_w, v.tw), ("ts", time_s, v.ts),
        ("middle", middle, v.mid_v),
        ("skip", skip, v.sw.at[pl.ds(pl.multiple_of(c * skr, TILE), skr)]),
        ("tp", time_p, v.tp), ("out", out_w, v.outw_v),
        ("gain_one", input_gain, v.gain_one), ("gain_two", middle_gain, v.gain_two),
        ("gain_three", output_gain, v.gain_three),
    )):
        loads[name] = pltpu.make_async_copy(src, dst, v.ld_s.at[k])
        loads[name].start()

    tall = PACK * UNIT
    main = C // LANES * LANES
    tail = C - main

    def packed(ref, k):
        turned = ref[...].astype(F32).T
        first, second = turned[0:tall], turned[k - tall : k]
        mixed = jnp.concatenate([first[:, main:C], second[:, main:C]], axis=1)
        return jnp.concatenate([first[:, 0:main], mixed, second[:, 0:main]], axis=1).astype(BF16)

    def unpack(block, ref, start):
        mixed = block[:, main : main + LANES]
        ref[start : start + tall, 0:main] = block[:, 0:main]
        ref[start : start + tall, main : main + LANES] = mixed
        swapped = pltpu.roll(mixed.astype(F32), LANES - tail, 1).astype(BF16)
        start = start + fk - tall
        ref[start : start + tall, 0:main] = block[:, main + LANES : 2 * C]
        ref[start : start + tall, main : main + LANES] = swapped

    loads["latent"].wait()
    v.lat[0, r] = v.lat_v[...]
    loads["front"].wait()
    v.fp[r] = packed(v.front_v, fk)

    pl.semaphore_wait(barrier, len(others))

    def lat_row(i, rr):
        return remote(v.lat_v, v.lat.at[0, r], v.one_s.at[0], v.one_r.at[0], rr, c)

    for i in range(1, R):
        lat_row(i, lax.rem(r + i, R)).start()

    def lat_left():
        return remote(v.lat_v, v.lat.at[2, r], v.one_s.at[1], v.one_r.at[2],
                      snake(R - 1, c - 1, R), c - 1)

    def lat_right():
        return remote(v.lat_v, v.lat.at[1, r], v.one_s.at[2], v.one_r.at[1],
                      snake(0, c + 1, R), c + 1)

    @pl.when(c > 0)
    def _():
        lat_left().start()

    @pl.when(c < Q - 1)
    def _():
        lat_right().start()

    core, xx = lax.rem(c, 2), c // 2
    mate = c + 1 - 2 * core
    over = lax.rem(c + 2, Q)
    y = lax.rem(r, 2)
    twin = r + 1 - 2 * y
    share = PACK // 2
    sizes = (ALONE, share - 2 * ALONE)

    def f_part(owner, part, x_of, core_of):
        first = (x_of * (share - ALONE), ALONE)[part]
        return v.fp.at[owner, pl.ds(
            pl.multiple_of((core_of * share + first) * UNIT, UNIT), sizes[part] * UNIT)]

    def f_move(owner, part, ssem, rr, cc):
        ref = f_part(owner, part, xx, core)
        return remote(ref, ref, ssem, v.fm_r.at[part, owner], rr, cc)

    def f_up(owner, part):
        return f_move(owner, part, v.one_s.at[6], r + 2, c)

    def f_down(owner, part):
        return f_move(owner, part, v.one_s.at[7], r - 2, c)

    def f_twin(owner, part):
        return f_move(owner, part, v.one_s.at[8], twin, c)

    def f_over(owner, x_of):
        ref = f_part(owner, 0, x_of, core)
        return remote(ref, ref, v.one_s.at[9], v.fx_r.at[owner], r, over)

    def f_mate(owner, part):
        ref = f_part(owner, part, xx, core)
        return remote(ref, ref, v.one_s.at[10], v.one_r.at[10], r, mate)

    def f_mate_extra(owner):
        ref = f_part(owner, 0, 1 - xx, core)
        return remote(ref, ref, v.one_s.at[10], v.one_r.at[10], r, mate)

    def when_row(t, body):
        @pl.when((t >= 0) & (t < R))
        def _():
            body()

    for part in (0, 1):
        when_row(r + 2, lambda: f_up(r, part).start())
        when_row(r - 2, lambda: f_down(r, part).start())
        f_twin(r, part).start()

    def from_z(d, sign, part):
        t = r + sign * 2 * d

        def body():
            f_twin(t, part).wait_recv()
            if sign < 0:
                when_row(r + 2, lambda: f_up(t, part).start())
            else:
                when_row(r - 2, lambda: f_down(t, part).start())
            f_twin(t, part).start()
            if part == 0:
                f_over(t, xx).start()
            f_mate(t, part).start()
        when_row(t, body)

    def from_y(owner, part):
        f_twin(owner, part).wait_recv()
        if part == 0:
            f_over(owner, xx).start()
        f_mate(owner, part).start()

    def from_x(owner):
        f_over(owner, 1 - xx).wait_recv()
        f_mate_extra(owner).start()

    def x_steps(d, twins):
        for sign in (-1, 1):
            t = r + sign * 2 * d
            when_row(t, lambda: from_x(t + twins * (twin - r)))

    def z_steps(d):
        for part in (0, 1):
            for sign in (-1, 1):
                from_z(d, sign, part)

    def y_steps(d):
        for part in (0, 1):
            for sign in (-1, 1):
                t = r + sign * 2 * d
                when_row(t, lambda: from_y(t + twin - r, part))

    loads["middle"].wait()
    v.mp[c] = packed(v.mid_v, mk)
    loads["skip"].wait()
    quarter = tall // 4

    def mid_copy(ref, n, rr, cc):
        return remote(ref, ref, v.mid_s.at[n], v.mid_r.at[n], rr, cc)

    def mid_rows(owner, n, of):
        return v.mp.at[owner, pl.ds(pl.multiple_of((2 * of + n) * quarter, UNIT), quarter)]

    def skip_rows(owner):
        return v.sw.at[pl.ds(pl.multiple_of(owner * skr, TILE), skr)]

    far = lax.rem(mate + 2, Q)

    def mid_over(n, owner):
        ref = skip_rows(owner) if n == 2 else mid_rows(owner, n, y)
        return mid_copy(ref, n, r, over)

    def mid_twin(n, of):
        return mid_copy(mid_rows(over, n, of), 3 + n, twin, c)

    def mid_on(n, owner, of):
        ref = skip_rows(owner) if n == 4 else mid_rows(owner, n % 2, of)
        return mid_copy(ref, 5 + n, r, mate)

    def mid_mate(owner):
        return (mid_copy(v.mp.at[owner], 10, r, mate), mid_copy(skip_rows(owner), 11, r, mate))

    mid_over(0, c).start()
    for copy in mid_mate(c):
        copy.start()

    loads["deep"].wait()
    deep_t = v.deep_v[...].astype(F32).T
    v.dr[:, C:CP] = jnp.zeros((px, GAP), BF16)
    v.dr[:, 0:C] = deep_t.astype(BF16)
    pad = jnp.zeros((1, GAP), F32)
    deep_top = jnp.concatenate([jnp.sum(deep_t, axis=0, keepdims=True), pad], axis=1)
    deep_low = jnp.concatenate([jnp.sum(deep_t * deep_t, axis=0, keepdims=True), pad], axis=1)
    def a2a_copy(q):
        return remote(v.dr.at[pl.ds(W * q, W)], v.a2a.at[r], v.one_s.at[3], v.one_r.at[3],
                      snake(q, c, R), c)

    def a2a_send():
        for q in range(R):
            @pl.when(s != q)
            def _():
                a2a_copy(q).start()

            @pl.when(s == q)
            def _():
                v.a2a[r] = v.dr[pl.ds(W * q, W), :]

    loads["in"].wait()
    inw = v.inw[...].astype(F32)
    v.wb[...] = jnp.zeros(v.wb.shape, F32)
    for b in range(3):
        rows = [inw[cin * (3 * a + b) : cin * (3 * a + b + 1), :] for a in range(3)]
        band = jnp.concatenate(rows, axis=0)
        band = jnp.concatenate([jnp.zeros((3 * cin, GAP), F32), band], axis=1)
        for yy in range(R):
            lo, hi = max(0, yy - 1), min(R, yy + 2)
            v.wb[b, lo * cin : hi * cin, yy * CP : (yy + 1) * CP] = (
                band[(lo - yy + 1) * cin : (hi - yy + 1) * cin, :])

    loads["tw"].wait()
    loads["ts"].wait()
    half = FQ // 2
    index = lax.broadcasted_iota(jnp.int32, (1, half), 1).astype(F32)
    angles = timestep[0].astype(F32) * jnp.exp(-math.log(10000.0) * index / half)
    v.part[:, 0:half] = jnp.cos(angles)
    v.part[:, half:FQ] = jnp.sin(angles)
    hidden = silu(jnp.sum(dot(pieces_of(v.part[...]), v.tw[...]), axis=0, keepdims=True))
    tk = time_s.shape[0]
    for q in range(Q):
        @pl.when(c == q)
        def _():
            v.part[...] = hidden[:, q * tk : (q + 1) * tk]
    v.emb[c] = jnp.sum(dot(pieces_of(v.part[...]), v.ts[...]), axis=0, keepdims=True)

    def emb_copy(i, src_c, target):
        return remote(v.emb.at[src_c], v.emb.at[src_c], v.one_s.at[5], v.one_r.at[5], r, target)

    for i in range(1, Q):
        emb_copy(i, c, lax.rem(c + i, Q)).start()

    @pl.when((s != 0) | (c == 0))
    def _():
        v.lat[1] = jnp.zeros(v.lat.shape[1:], BF16)

    @pl.when((s != R - 1) | (c == Q - 1))
    def _():
        v.lat[2] = jnp.zeros(v.lat.shape[1:], BF16)

    def all_of(ref, n):
        return remote(ref, ref, v.one_s.at[n], v.one_r.at[n], twin, c)

    all_of(v.lat.at[0, pl.ds(0, R - 1)], 0).wait_recv()

    @pl.when((s == 0) & (c > 0))
    def _():
        all_of(v.lat.at[1], 1).wait_recv()

    @pl.when((s == R - 1) & (c < Q - 1))
    def _():
        all_of(v.lat.at[2], 2).wait_recv()

    for k in range(3):
        for q in range(R):
            v.latrows[k, cin * q : cin * (q + 1), :] = v.lat[k, q].astype(F32)
    lane = lax.broadcasted_iota(jnp.int32, (R * cin, px), 1)
    base = jnp.where((lane == px - 1) & (s == 0), v.latrows[1], v.latrows[0])
    base = jnp.where((lane == 0) & (s == R - 1), v.latrows[2], base)
    rolled = pltpu.roll(base, lax.rem(px + 1 - W * s, px), 1)
    v.tap[0:LANES, 0 : R * cin] = rolled[:, 0:LANES].T
    total = None
    for b in range(3):
        term = dot(v.tap[b : b + W, 0 : R * cin].astype(BF16), v.wb[b].astype(BF16))
        total = term if total is None else total + term
    v.sk[...] = total.astype(BF16).astype(F32)
    top = low = None
    for q in range(R):
        slab = v.sk[:, q * CP : (q + 1) * CP]
        top = slab if top is None else top + slab
        low = slab * slab if low is None else low + slab * slab
    skip_top = jnp.sum(top, axis=0, keepdims=True)
    skip_low = jnp.sum(low, axis=0, keepdims=True)

    def join(d, k):
        cut = C // LANES * LANES
        return jnp.concatenate(
            [d[:, 0:cut], d[:, cut:CP] + k[:, 0 : CP - cut], k[:, CP - cut : CP]], axis=1)

    def indicator(channels, flip):
        shape = (LANES, channels) if flip else (channels, LANES)
        size = channels // GROUPS
        ch = lax.broadcasted_iota(jnp.int32, shape, 1 if flip else 0)
        g = lax.broadcasted_iota(jnp.int32, shape, 0 if flip else 1)
        return ((ch >= g * size) & (ch < g * size + size)).astype(F32).astype(BF16)

    def sum_copy(stage, slot, i, rr, cc):
        return remote(v.sums.at[stage, slot], v.sums.at[stage, slot],
                      v.sum_s.at[stage], v.sum_r.at[stage], rr, cc)

    def reduce_start(stage, top, low):
        channels = top.shape[1]
        res = dot(jnp.concatenate([pieces_of(top), pieces_of(low)], axis=0),
                  indicator(channels, False))
        v.sums[stage, me] = jnp.sum(res[0:3], axis=0, keepdims=True) + pltpu.roll(
            jnp.sum(res[3:6], axis=0, keepdims=True), GROUPS, 1)
        for n, (i, j) in enumerate(others):
            sum_copy(stage, me, n, lax.rem(r + i, R), lax.rem(c + j, Q)).start()

    def sum_all(stage):
        ref = v.sums.at[stage, pl.ds(0, R * Q - 1)]
        return remote(ref, ref, v.sum_s.at[stage], v.sum_r.at[stage], twin, c)

    def reduce_end(stage, channels):
        sum_all(stage).wait_recv()
        total = jnp.sum(v.sums[stage], axis=0) / (channels // GROUPS * image)
        spread = pltpu.roll(total, LANES - GROUPS, 1) - total * total
        inverse = lax.rsqrt(jnp.maximum(spread, 0.0) + EPS)
        group = lax.broadcasted_iota(jnp.int32, (1, LANES), 1) < GROUPS
        wide = dot(jnp.concatenate([pieces_of(jnp.where(group, row, 0.0))
                                    for row in (total, inverse)], axis=0),
                   indicator(channels, True))
        return (jnp.sum(wide[0:3], axis=0, keepdims=True),
                jnp.sum(wide[3:6], axis=0, keepdims=True))

    reduce_start(0, join(deep_top, skip_top), join(deep_low, skip_low))

    inner = (s + R - 1) // R
    last = (s + 1) // R
    left = (inner * snake(s - 1, c, R) + (1 - inner) * r, c - (1 - inner))
    right = ((1 - last) * snake(s + 1, c, R) + last * r, c + last)
    has_left, has_right = left[1] >= 0, right[1] < Q

    def halo_left(stage, ext):
        return remote(ext.at[:, pl.ds(8, 8)], ext.at[:, pl.ds(N + 8, 8)],
                      v.halo_s.at[stage, 0], v.halo_r.at[stage, 1], left[0], left[1])

    def halo_right(stage, ext):
        return remote(ext.at[:, pl.ds(N, 8)], ext.at[:, pl.ds(0, 8)],
                      v.halo_s.at[stage, 1], v.halo_r.at[stage, 0], right[0], right[1])

    def halo_send(stage, ext):
        zeros = jnp.zeros((ext.shape[0], 8, LANES), F32)

        @pl.when(has_left)
        def _():
            halo_left(stage, ext).start()

        @pl.when(has_right)
        def _():
            halo_right(stage, ext).start()

        @pl.when(jnp.logical_not(has_left))
        def _():
            ext[:, 0:8, :] = zeros

        @pl.when(jnp.logical_not(has_right))
        def _():
            ext[:, N + 8 : N + 16, :] = zeros

    def halo_wait(stage, ext):
        @pl.when(has_left)
        def _():
            halo_right(stage, ext).wait_recv()

        @pl.when(has_right)
        def _():
            halo_left(stage, ext).wait_recv()

    z_steps(1)
    for part in (0, 1):
        from_y(twin, part)
    z_steps(2)
    a2a_send()
    mid_over(1, c).start()
    y_steps(1)
    for d in range(3, R // 2):
        z_steps(d)
        y_steps(d - 1)
    all_of(v.a2a.at[pl.ds(0, R - 1)], 3).wait_recv()
    for q in range(R):
        joined = join(v.a2a[q].astype(F32), v.sk[:, q * CP : (q + 1) * CP])
        for n in range(2 * C // LANES):
            v.jx[n, pl.ds(8 + q, W, 8), :] = joined[:, n * LANES : (n + 1) * LANES]
    halo_send(0, v.jx)
    from_x(twin)
    x_steps(1, 0)
    x_steps(2, 0)
    x_steps(1, 1)
    y_steps(R // 2 - 1)
    mid_over(2, c).start()
    for n in (0, 1):
        mid_over(n, over).wait_recv()
        mid_twin(n, y).start()
        mid_on(n, over, y).start()

    loads["out"].wait()
    loads["tp"].wait()
    for name in ("gain_one", "gain_two", "gain_three"):
        loads[name].wait()
    v.wr32[...] = jnp.zeros(v.wr32.shape, F32)
    for t in range(9):
        v.wr32[couts * t : couts * (t + 1), :] = v.outw_v[:, C * t : C * (t + 1)].astype(F32)
    out_taps = v.wr32[...].T.astype(BF16)

    all_of(v.emb.at[pl.ds(0, Q - 1)], 5).wait_recv()
    embedded = jnp.sum(v.emb[...], axis=0)
    time_shift = jnp.sum(dot_nt(pieces_of(silu(embedded)), v.tp[...]), axis=0, keepdims=True)

    place = lax.broadcasted_iota(jnp.int32, (W + 2, 8, 1), 0)
    inside = (
        ((place > 0) | has_left) & ((place < W + 1) | has_right))
    row = lax.broadcasted_iota(jnp.int32, (W + 2, 8, 1), 1)

    def keep_own(ext, values):
        for n in range(ext.shape[0]):
            lo, hi = n * LANES, min((n + 1) * LANES, values.shape[1])
            ext[n, 8 : N + 8, 0 : hi - lo] = values[:, lo:hi]

    def rows_of(ext, channels, first, count):
        return jnp.concatenate(
            [ext[n, first : first + count, 0 : min(LANES, channels - n * LANES)]
             for n in range(ext.shape[0])], axis=1)

    def activate(ext, stats, gain):
        center, inverse = stats
        scale = inverse * gain
        channels = gain.shape[1]
        for lo in range(0, channels, LANES):
            hi = min(channels, lo + LANES)
            z = silu((ext[lo // LANES, :, 0 : hi - lo] - center[:, lo:hi]) * scale[:, lo:hi])
            z = jnp.where(inside, z.reshape(W + 2, 8, hi - lo), 0.0)
            for a in range(3):
                if a == 1:
                    moved = z
                elif a == 0:
                    moved = jnp.where(row > 0, pltpu.roll(z, 1, 1), 0.0)
                else:
                    moved = jnp.where(row < 7, pltpu.roll(z, 7, 1), 0.0)
                flat = moved.reshape(N + 16, hi - lo)
                v.act_a[a, :, lo:hi] = flat.astype(BF16)
                v.act_b[a, :, lo:hi] = flat[8 : N + 8].astype(BF16)

    def conv(channels, weight):
        total = None
        for a in range(3):
            for b in range(3):
                if b == 1:
                    act = v.act_b[a, :, 0:channels]
                else:
                    act = v.act_a[a, 8 * b : 8 * b + N, 0:channels]
                k = (3 * a + b) * channels
                term = dot(act, weight[k : k + channels, 0:C])
                total = term if total is None else total + term
        return total

    for d in range(3, R // 2):
        x_steps(d, 0)
        x_steps(d - 1, 1)
    x_steps(R // 2 - 1, 1)
    stats = reduce_end(0, 2 * C)
    halo_wait(0, v.jx)
    activate(v.jx, stats, v.gain_one[...].reshape(1, 2 * C))

    mate_rows = v.fp.at[pl.ds(0, R - 1), pl.ds(0, share * UNIT)]
    all_of(mate_rows, 10).wait_recv()
    for owner in range(R):
        unpack(v.fp[owner], v.fw, owner * fk)

    hidden_one = conv(2 * C, v.fw) + time_shift
    keep_own(v.hx, hidden_one)
    reduce_start(1, jnp.sum(hidden_one, axis=0, keepdims=True),
                 jnp.sum(hidden_one * hidden_one, axis=0, keepdims=True))
    halo_send(1, v.hx)

    mid_over(2, over).wait_recv()
    mid_on(4, over, y).start()
    for n in (0, 1):
        mid_twin(n, 1 - y).wait_recv()
        mid_on(2 + n, over, 1 - y).start()
    for copy in mid_mate(mate):
        copy.wait_recv()
    for n in range(5):
        mid_on(n, far, y if n < 2 else 1 - y).wait_recv()
    for owner in range(Q):
        unpack(v.mp[owner], v.mw, owner * mk)
    shortcut = dot(rows_of(v.jx, 2 * C, 8, N).astype(BF16), v.sw[...])
    stats = reduce_end(1, C)
    halo_wait(1, v.hx)
    activate(v.hx, stats, v.gain_two[...].reshape(1, C))
    block_out = conv(C, v.mw) + shortcut

    keep_own(v.ox, block_out)
    reduce_start(2, jnp.sum(block_out, axis=0, keepdims=True),
                 jnp.sum(block_out * block_out, axis=0, keepdims=True))
    halo_send(2, v.ox)
    stats = reduce_end(2, C)
    halo_wait(2, v.ox)

    center, inverse = stats
    z = silu((rows_of(v.ox, C, 0, N + 16) - center) * (inverse * v.gain_three[...].reshape(1, C)))
    z = jnp.where(inside, z.reshape(W + 2, 8, C), 0.0).reshape(N + 16, C)
    spread = dot(z.astype(BF16), out_taps)
    lane = lax.broadcasted_iota(jnp.int32, (N, LANES), 1)
    row = lax.broadcasted_iota(jnp.int32, (W, 8, 1), 1)
    total = None
    for a in range(3):
        got = None
        for b in range(3):
            t = couts * (3 * a + b)
            here = jnp.where(
                (lane >= t) & (lane < t + couts), spread[8 * b : 8 * b + N, :], 0.0)
            got = here if got is None else got + here
        got = got.reshape(W, 8, LANES)
        if a == 0:
            got = jnp.where(row > 0, pltpu.roll(got, 1, 1), 0.0)
        elif a == 2:
            got = jnp.where(row < 7, pltpu.roll(got, 7, 1), 0.0)
        total = got if total is None else total + got
    v.tap[...] = total.reshape(N, LANES)
    ordered = jnp.concatenate([v.tap[pl.ds(q, W, 8), :] for q in range(R)], axis=0)
    fold = (lax.rem(lax.broadcasted_iota(jnp.int32, (8, LANES), 1), couts)
            == lax.broadcasted_iota(jnp.int32, (8, LANES), 0)).astype(F32)
    rows = dot_nt(fold, ordered, lax.Precision.HIGHEST)[0:couts]
    for q in range(R):
        v.outs[q, :, 0:W] = rows[:, W * q : W * (q + 1)]

    def out_copy(q, rr):
        return remote(v.outs.at[q], v.outr.at[s], v.one_s.at[4], v.one_r.at[4], rr, c)

    for q in range(R):
        @pl.when(r != q)
        def _():
            out_copy(q, q).start()

        @pl.when(r == q)
        def _():
            v.outr[s] = v.outs[q]

    all_of(v.outr.at[pl.ds(0, R - 1)], 4).wait_recv()
    for q in range(R):
        noise[:, W * q : W * (q + 1)] = v.outr[q, :, 0:W]

    all_of(v.lat.at[0, pl.ds(0, R - 1)], 0).wait_send()

    @pl.when(c > 0)
    def _():
        lat_left().wait_send()

    @pl.when(c < Q - 1)
    def _():
        lat_right().wait_send()

    all_of(v.a2a.at[pl.ds(0, R - 1)], 3).wait_send()
    all_of(v.outr.at[pl.ds(0, R - 1)], 4).wait_send()
    all_of(v.emb.at[pl.ds(0, Q - 1)], 5).wait_send()
    for stage, ext in enumerate((v.jx, v.hx, v.ox)):
        sum_all(stage).wait_send()

        @pl.when(has_left)
        def _():
            halo_left(stage, ext).wait_send()

        @pl.when(has_right)
        def _():
            halo_right(stage, ext).wait_send()
    for n in range(3):
        mid_over(n, c).wait_send()
    for n in range(2):
        mid_twin(n, y).wait_send()
    for n in range(5):
        mid_on(n, over, y if n < 2 else 1 - y).wait_send()
    for copy in mid_mate(c):
        copy.wait_send()
    moved = (share - ALONE) * UNIT
    level = r // 2
    for count in range(1, R // 2):
        @pl.when(level == count - 1)
        def _():
            all_of(v.fp.at[pl.ds(0, count), pl.ds(0, moved)], 6).wait_send()

        @pl.when(level == R // 2 - count)
        def _():
            all_of(v.fp.at[pl.ds(0, count), pl.ds(0, moved)], 7).wait_send()

    all_of(v.fp.at[pl.ds(0, R // 2), pl.ds(0, moved)], 8).wait_send()
    all_of(v.fp.at[pl.ds(0, R - 1), pl.ds(0, ALONE * UNIT)], 9).wait_send()
    all_of(mate_rows, 10).wait_send()


def fast_shards(
    R, Q,
    latent, deep, timestep, in_weight, front_weight, middle_weight, skip_weight, out_weight,
    time_weight, time_second, time_proj, input_gain, middle_gain, output_gain,
):
    C = deep.shape[0]
    cin = latent.shape[0]
    px = deep.shape[1] * deep.shape[2]
    couts = out_weight.shape[1]
    W = px // R
    N = W * 8
    CP = (C + LANES - 1) // LANES * LANES
    fk, mk, skr = front_weight.shape[0], middle_weight.shape[0], skip_weight.shape[0]
    hbm = pl.BlockSpec(memory_space=pl.ANY)
    vmem = pl.BlockSpec(memory_space=pltpu.VMEM)
    smem = pl.BlockSpec(memory_space=pltpu.SMEM)
    dma = pltpu.SemaphoreType.DMA
    args = (
        latent.reshape(cin, px), deep.reshape(C, px), timestep, in_weight, front_weight.T,
        middle_weight.T, skip_weight, out_weight.T, time_weight, time_second, time_proj.T,
        input_gain, middle_gain, output_gain,
    )
    fq, wide = time_weight.shape
    shapes = dict(
        lat_v=pltpu.VMEM((cin, px), BF16), lat=pltpu.VMEM((3, R, cin, px), BF16),
        latrows=pltpu.VMEM((3, R * cin, px), F32), deep_v=pltpu.VMEM((C, px), BF16),
        dr=pltpu.VMEM((px, CP), BF16), a2a=pltpu.VMEM((R, W, CP), BF16),
        inw=pltpu.VMEM((9 * cin, C), BF16), wb=pltpu.VMEM((3, R * cin, R * CP), F32),
        sk=pltpu.VMEM((W, R * CP), F32), jx=pltpu.VMEM((2 * C // LANES, N + 16, LANES), F32),
        hx=pltpu.VMEM((CP // LANES, N + 16, LANES), F32),
        ox=pltpu.VMEM((CP // LANES, N + 16, LANES), F32),
        act_a=pltpu.VMEM((3, N + 16, 2 * C), BF16), act_b=pltpu.VMEM((3, N, 2 * C), BF16),
        front_v=pltpu.VMEM((C, fk), BF16), fw=pltpu.VMEM((18 * C, CP), BF16),
        fp=pltpu.VMEM((R, PACK * UNIT, 2 * C), BF16), mp=pltpu.VMEM((Q, PACK * UNIT, 2 * C), BF16),
        mid_v=pltpu.VMEM((C, mk), BF16), mw=pltpu.VMEM((9 * C, CP), BF16),
        sw=pltpu.VMEM((2 * C, C), BF16), outw_v=pltpu.VMEM((couts, 9 * C), BF16),
        wr32=pltpu.VMEM((LANES, C), F32), tw=pltpu.VMEM((fq, wide), BF16),
        ts=pltpu.VMEM(time_second.shape, BF16), tp=pltpu.VMEM((C, wide), BF16),
        part=pltpu.VMEM((1, fq), F32), emb=pltpu.VMEM((Q, 1, wide), F32),
        sums=pltpu.VMEM((3, R * Q, 1, LANES), F32), tap=pltpu.VMEM((N, LANES), F32),
        outs=pltpu.VMEM((R, couts, LANES), F32), outr=pltpu.VMEM((R, couts, LANES), F32),
        gain_one=pltpu.VMEM((2 * C,), F32), gain_two=pltpu.VMEM((C,), F32),
        gain_three=pltpu.VMEM((C,), F32),
        ld_s=dma((13,)), one_s=dma((11,)), one_r=dma((11,)), halo_s=dma((3, 2)), halo_r=dma((3, 2)),
        fm_r=dma((2, R)), fx_r=dma((R,)), mid_s=dma((12,)), mid_r=dma((12,)),
        sum_s=dma((3,)), sum_r=dma((3,)),
    )
    specs = [hbm] * len(args)
    specs[2] = smem
    out = pl.pallas_call(
        functools.partial(fast_kernel, R, Q, tuple(shapes)),
        out_shape=jax.ShapeDtypeStruct((couts, px), F32),
        in_specs=specs,
        out_specs=vmem,
        scratch_shapes=list(shapes.values()),
        compiler_params=pltpu.CompilerParams(
            collective_id=0, has_side_effects=True, vmem_limit_bytes=56 * 1024 * 1024
        ),
    )(*args)
    return out.reshape(couts, 1, px)


def solution(mesh):
    R, Q = mesh.shape["rows"], mesh.shape["cols"]

    def body(*args):
        deep, front = args[1], args[4]
        fits = (
            R == 8 and Q == 4 and deep.shape[1] == 1 and deep.shape[2] % (R * LANES // 4) == 0
            and front.shape[0] % UNIT == 0
            and PACK * UNIT < front.shape[0] <= 2 * PACK * UNIT
            and args[5].shape[0] == front.shape[0] and deep.shape[0] % LANES * 2 == LANES)
        return (fast_shards if fits else shards)(R, Q, *args)

    return jax.shard_map(
        body,
        mesh=mesh,
        in_specs=(
            P(None, "rows", "cols"), P(None, "rows", "cols"), P(), P(),
            P("rows", None), P("cols", None), P("cols", None), P(),
            P(), P("cols", None), P(), P(), P(), P(),
        ),
        out_specs=P(None, "rows", "cols"),
        check_vma=False,
    )
```

```python
import functools
import math

import jax
import jax.numpy as jnp
from jax import lax
from jax.experimental import pallas as pl
from jax.experimental.pallas import tpu as pltpu
from jax.sharding import PartitionSpec as P

GROUPS = 32
EPS = 1e-05
TILE = 16
LANES = 128
MESH = pl.DeviceIdType.MESH
F32 = jnp.float32
BF16 = jnp.bfloat16
SIDES = tuple((i, j) for i in (-1, 0, 1) for j in (-1, 0, 1) if (i, j) != (0, 0))


def dot(a, b, precision=None):
    return lax.dot_general(
        a, b, (((1,), (0,)), ((), ())), preferred_element_type=F32, precision=precision
    )


def split_dot(row, weight):
    high = row.astype(BF16)
    rest = row - high.astype(F32)
    middle = rest.astype(BF16)
    low = (rest - middle.astype(F32)).astype(BF16)
    pieces = jnp.concatenate([high.astype(F32), middle.astype(F32), low.astype(F32)], axis=0)
    return jnp.sum(dot(pieces.astype(BF16), weight), axis=0, keepdims=True)


def silu(z):
    return z / (1.0 + jnp.exp(-z))


def kernel(
    R, Q, ring,
    latent, deep, rows_in, in_w, front, middle, skip, out_w, time_w, time_s, time_p,
    noise,
    lat, jext, hext, oext, shifted, patch, fw, mw, sw, part, emb, sums_a, sums_b,
    lat_s, lat_r, halo_s, halo_r, fz_s, fy_s, fc_s, fm_r, fo_r, mid_s, mid_r, emb_s, emb_r,
    ca_s, ca_r, cb_s, cb_r, loc_s,
):
    r = lax.axis_index("rows")
    c = lax.axis_index("cols")
    C, px = deep.shape
    cin = latent.shape[0]
    image = float(px * R * Q)
    FQ = time_w.shape[0]
    gain_one = rows_in[:, FQ : FQ + 2 * C]
    gain_two = rows_in[:, FQ + 2 * C : FQ + 3 * C]
    gain_three = rows_in[:, FQ + 3 * C : FQ + 4 * C]

    def remote(src, dst, ssem, rsem, rr, cc):
        return pltpu.make_async_remote_copy(
            src_ref=src, dst_ref=dst, send_sem=ssem, recv_sem=rsem,
            device_id={"rows": rr, "cols": cc}, device_id_type=MESH,
        )

    def each(count, body):
        if count <= 8:
            for i in range(1, count):
                body(i)
        else:
            lax.fori_loop(1, count, lambda i, u: (body(i), u)[1], 0)

    barrier = pltpu.get_barrier_semaphore()

    def greet(rr, cc):
        pl.semaphore_signal(barrier, inc=1, device_id={"rows": rr, "cols": cc}, device_id_type=MESH)

    each(R, lambda i: greet(lax.rem(r + i, R), c))
    each(Q, lambda i: greet(r, lax.rem(c + i, Q)))
    for i in (-1, 1):
        for j in (-1, 1):
            greet(lax.rem(r + i + R, R), lax.rem(c + j + Q, Q))
    pl.semaphore_wait(barrier, R - 1 + Q - 1 + 4)

    def inside(rr, cc):
        return (rr >= 0) & (rr < R) & (cc >= 0) & (cc < Q)

    def lat_copy(k, rr, cc):
        i, j = SIDES[k]
        return remote(latent, lat.at[k], lat_s.at[k], lat_r.at[k], rr, cc)

    for k, (i, j) in enumerate(SIDES):
        @pl.when(inside(r + i, c + j))
        def _():
            lat_copy(k, r + i, c + j).start()

        @pl.when(jnp.logical_not(inside(r - i, c - j)))
        def _():
            lat[k] = jnp.zeros(lat.shape[1:], lat.dtype)

    parity = lax.rem(c, 2)
    mate = c + 1 - 2 * parity
    over = lax.rem(c + 2, Q)
    half_c = lax.rem(r, 2)
    twin = r + 1 - 2 * half_c
    mk, sk = middle.shape[0], skip.shape[0]

    def mid_copies(owner, s, slot_from, target):
        rows_m = pl.ds(pl.multiple_of(owner * mk, TILE), mk)
        rows_s = pl.ds(pl.multiple_of(owner * sk, TILE), sk)
        src_m, src_s = (middle, skip) if slot_from else (mw.at[rows_m], sw.at[rows_s])
        return (
            remote(src_m, mw.at[rows_m], mid_s.at[0, s], mid_r.at[0, s], r, target),
            remote(src_s, sw.at[rows_s], mid_s.at[1, s], mid_r.at[1, s], r, target),
        )

    fk = fw.shape[0] // R if ring else 0
    cut = fk // 2 // TILE * TILE
    spans = ((0, cut), (cut, fk - cut))

    def f_rows(owner, par):
        return pl.ds(pl.multiple_of(owner * fk, TILE) + spans[par][0], spans[par][1])

    def by_parity(par_of, body):
        for par in (0, 1):
            @pl.when(par_of == par)
            def _():
                body(par)

    def f_own(par, target, ssem):
        src = front.at[pl.ds(spans[par][0], spans[par][1])]
        return remote(src, fw.at[f_rows(r, par)], ssem, fm_r.at[r], target, c)

    def f_pass(owner, par, target):
        return remote(fw.at[f_rows(owner, par)], fw.at[f_rows(owner, par)],
                      fy_s.at[owner], fm_r.at[owner], target, c)

    def f_mate(owner, par):
        return remote(fw.at[f_rows(owner, par)], fw.at[f_rows(owner, par)],
                      fc_s.at[owner], fo_r.at[owner], r, mate)

    def by_distance(distances, body):
        for d in distances:
            for t in (r + 2 * d, r - 2 * d):
                @pl.when((t >= 0) & (t < R))
                def _():
                    body(t)

    locals_ = []
    if ring:
        locals_.append(pltpu.make_async_copy(
            front, fw.at[pl.ds(pl.multiple_of(r * fk, TILE), fk)], loc_s.at[0]))
    locals_.append(pltpu.make_async_copy(
        middle, mw.at[pl.ds(pl.multiple_of(c * mk, TILE), mk)], loc_s.at[1]))
    locals_.append(pltpu.make_async_copy(
        skip, sw.at[pl.ds(pl.multiple_of(c * sk, TILE), sk)], loc_s.at[2]))
    for copy in locals_:
        copy.start()

    if ring:
        def first(par):
            f_own(par, twin, fy_s.at[r]).start()
            def one(t):
                f_own(par, t, fz_s.at[t]).start()
            by_distance(range(1, R // 2), one)
        by_parity(parity, first)
    for copy in mid_copies(c, 0, True, over) + mid_copies(c, 1, True, mate):
        copy.start()

    def pass_on(distances):
        def go(par):
            def one(owner):
                f_pass(owner, par, twin).wait_recv()
                f_pass(owner, par, twin).start()
                f_mate(owner, par).start()
            by_distance(distances, one)
        by_parity(parity, go)

    for k, (i, j) in enumerate(SIDES):
        @pl.when(inside(r - i, c - j))
        def _():
            lat_copy(k, r - i, c - j).wait_recv()
    where = {side: k for k, side in enumerate(SIDES)}
    for a in range(3):
        tiles = []
        for b in range(3):
            side = (1 - a, 1 - b)
            block = latent[...] if side == (0, 0) else lat[where[side]]
            tiles.append(block.astype(F32))
        wide = jnp.concatenate(tiles, axis=1)
        for b in range(3):
            start = px + b - 1
            patch[cin * (3 * a + b) : cin * (3 * a + b + 1), :] = wide[:, start : start + px]
    skip_feat = dot(patch[...].T.astype(BF16), in_w[...]).astype(BF16)
    deep_t = deep[...].astype(F32).T.astype(BF16)
    own = pl.ds(TILE, px)
    jext[1, own, :] = jnp.concatenate([deep_t.astype(F32), skip_feat.astype(F32)], axis=1).astype(BF16)

    def halo_copy(stage, ext, k, rr, cc):
        i, j = SIDES[k]
        src = ((TILE, TILE), (TILE, px), (px, TILE))[j + 1]
        dst = ((TILE + px, TILE), (TILE, px), (0, TILE))[j + 1]
        return remote(ext.at[1, pl.ds(*src), :], ext.at[1 - i, pl.ds(*dst), :],
                      halo_s.at[stage, k], halo_r.at[stage, k], rr, cc)

    def halo_send(stage, ext):
        for k, (i, j) in enumerate(SIDES):
            @pl.when(inside(r + i, c + j))
            def _():
                halo_copy(stage, ext, k, r + i, c + j).start()

            @pl.when(jnp.logical_not(inside(r - i, c - j)))
            def _():
                dst = ((TILE + px, TILE), (TILE, px), (0, TILE))[j + 1]
                ext[1 - i, pl.ds(*dst), :] = jnp.zeros((dst[1], ext.shape[2]), ext.dtype)

    def halo_wait(stage, ext):
        for k, (i, j) in enumerate(SIDES):
            @pl.when(inside(r - i, c - j))
            def _():
                halo_copy(stage, ext, k, r - i, c - j).wait_recv()

    def indicator(channels, flip):
        shape = (LANES, channels) if flip else (channels, LANES)
        size = channels // GROUPS
        ch = lax.broadcasted_iota(jnp.int32, shape, 1 if flip else 0)
        g = lax.broadcasted_iota(jnp.int32, shape, 0 if flip else 1)
        return ((ch >= g * size) & (ch < g * size + size)).astype(F32)

    def sum_copy(buf, ssem, rsem, stage, slot, i, rr, cc):
        return remote(buf.at[stage, slot], buf.at[stage, slot],
                      ssem.at[stage, i], rsem.at[stage, i], rr, cc)

    def reduce_start(stage, values):
        top = jnp.sum(values, axis=0, keepdims=True)
        low = jnp.sum(values * values, axis=0, keepdims=True)
        both = jnp.concatenate([top, low, jnp.zeros((6, values.shape[1]), F32)], axis=0)
        sums_a[stage, c] = dot(both, indicator(values.shape[1], False), lax.Precision.HIGHEST)
        for i in range(1, Q):
            sum_copy(sums_a, ca_s, ca_r, stage, c, i, r, lax.rem(c + i, Q)).start()

    def reduce_end(stage, channels):
        for i in range(1, Q):
            s = lax.rem(c + Q - i, Q)
            sum_copy(sums_a, ca_s, ca_r, stage, s, i, r, s).wait_recv()
        sums_b[stage, r] = jnp.sum(sums_a[stage], axis=0)
        each(R, lambda i: sum_copy(sums_b, cb_s, cb_r, stage, r, i, lax.rem(r + i, R), c).start())

        def got(i):
            s = lax.rem(r + R - i, R)
            sum_copy(sums_b, cb_s, cb_r, stage, s, i, s, c).wait_recv()

        each(R, got)
        total = jnp.sum(sums_b[stage], axis=0) / (channels // GROUPS * image)
        center = total[0:1]
        inverse = lax.rsqrt(total[1:2] - center * center + EPS)
        both = jnp.concatenate([center, inverse, jnp.zeros((6, LANES), F32)], axis=0)
        wide = dot(both, indicator(channels, True), lax.Precision.HIGHEST)
        return wide[0:1], wide[1:2]

    def conv(ext, stats, gain, weight, exact=None, shift=None):
        center, inverse = stats
        if shift is not None:
            center = center - shift
        channels = ext.shape[2]
        scale = inverse * gain
        place = lax.broadcasted_iota(jnp.int32, (px + 2 * TILE, 1), 0)
        inner = (place >= TILE) & (place < TILE + px)
        total = None
        for a in (1, 0, 2):
            z = (ext[a].astype(F32) - center) * scale
            here = r + a - 1
            keep = (here >= 0) & (here < R) & (
                inner | ((place < TILE) & (c > 0)) | ((place >= TILE + px) & (c < Q - 1)))
            shifted[:, 0:channels] = jnp.where(keep, silu(z), 0.0)
            if a == 1 and exact is not None:
                shifted[own, 0:channels] = silu((exact - center) * scale)
            for b in range(3):
                act = shifted[TILE + b - 1 : TILE + b - 1 + px, 0:channels].astype(BF16)
                k = (3 * a + b) * channels
                term = dot(act, weight[k : k + channels, :])
                total = term if total is None else total + term
        return total

    joined = jext[1, own, :]
    reduce_start(0, joined.astype(F32))
    halo_send(0, jext)

    hidden = silu(split_dot(rows_in[:, 0:FQ], time_w[...]))
    tk = time_s.shape[0]
    for q in range(Q):
        @pl.when(c == q)
        def _():
            part[...] = hidden[:, q * tk : (q + 1) * tk]
    emb_own = split_dot(part[...], time_s[...])
    emb[c] = emb_own

    def emb_copy(i, src_c, tgt):
        return remote(emb.at[src_c], emb.at[src_c], emb_s.at[i], emb_r.at[i], r, tgt)

    for i in range(1, Q):
        emb_copy(i, c, lax.rem(c + i, Q)).start()

    if ring:
        pass_on((1,))
    stats = reduce_end(0, 2 * C)
    if ring:
        pass_on(range(2, R // 2))

        def from_twin(par):
            def one(t):
                owner = t + twin - r
                f_pass(owner, par, twin).wait_recv()
                f_mate(owner, par).start()
            one(r)
            by_distance(range(1, R // 2), one)
        by_parity(parity, from_twin)

    for copy in mid_copies(over, 0, False, over):
        copy.wait_recv()
    for copy in mid_copies(over, 2, False, mate):
        copy.start()

    for i in range(1, Q):
        s = lax.rem(c + Q - i, Q)
        emb_copy(i, s, s).wait_recv()
    embedded = jnp.sum(emb[...], axis=0)
    time_shift = split_dot(silu(embedded), time_p[...])

    for copy in locals_:
        copy.wait()
    halo_wait(0, jext)
    if ring:
        def from_mate(i):
            owner = lax.rem(r + i, R)
            def go(par):
                f_mate(owner, 1 - par).wait_recv()
            by_parity(parity, go)
        for i in range(1, R):
            from_mate(i)
    front_out = conv(jext, stats, gain_one, fw if ring else front)

    hext[1, own, :] = front_out.astype(BF16)
    reduce_start(1, front_out + time_shift)
    halo_send(1, hext)
    for copy in mid_copies(mate, 1, False, mate):
        copy.wait_recv()
    far = lax.rem(mate + 2, Q)
    for copy in mid_copies(far, 2, False, mate):
        copy.wait_recv()
    shortcut = dot(joined, sw[...])
    stats = reduce_end(1, C)
    halo_wait(1, hext)
    block_out = conv(hext, stats, gain_two, mw, front_out, time_shift) + shortcut

    oext[1, own, :] = block_out.astype(BF16)
    reduce_start(2, block_out)
    halo_send(2, oext)
    stats = reduce_end(2, C)
    halo_wait(2, oext)
    result = conv(oext, stats, gain_three, out_w, block_out)
    noise[...] = result.T[0 : noise.shape[0], :]

    for k, (i, j) in enumerate(SIDES):
        @pl.when(inside(r + i, c + j))
        def _():
            lat_copy(k, r + i, c + j).wait_send()
            for stage, ext in enumerate((jext, hext, oext)):
                halo_copy(stage, ext, k, r + i, c + j).wait_send()
    for i in range(1, Q):
        emb_copy(i, c, lax.rem(c + i, Q)).wait_send()
        for stage in range(3):
            sum_copy(sums_a, ca_s, ca_r, stage, c, i, r, lax.rem(c + i, Q)).wait_send()

    def sent(i):
        for stage in range(3):
            sum_copy(sums_b, cb_s, cb_r, stage, r, i, lax.rem(r + i, R), c).wait_send()

    each(R, sent)
    for copy in (mid_copies(c, 0, True, over) + mid_copies(c, 1, True, mate)
                 + mid_copies(over, 2, False, mate)):
        copy.wait_send()
    if ring:
        def last(par):
            f_own(par, twin, fy_s.at[r]).wait_send()
            def one(t):
                f_own(par, t, fz_s.at[t]).wait_send()
                f_pass(t, par, twin).wait_send()
            by_distance(range(1, R // 2), one)
            for i in range(1, R):
                f_mate(lax.rem(r + i, R), par).wait_send()
        by_parity(parity, last)


def shards(
    R, Q,
    latent, deep, timestep, in_weight, front_weight, middle_weight, skip_weight, out_weight,
    time_weight, time_second, time_proj, input_gain, middle_gain, output_gain,
):
    C = deep.shape[0]
    cin = latent.shape[0]
    px = deep.shape[1] * deep.shape[2]
    assert deep.shape[1] == 1 and Q == 4 and R % 2 == 0 and R > 2
    ring = R <= 8 and front_weight.shape[0] % TILE == 0
    half = time_weight.shape[0] // 2
    ratios = jnp.exp(-math.log(10000.0) * jnp.arange(half, dtype=F32) / half)
    angles = timestep[0].astype(F32) * ratios
    rows_in = jnp.concatenate(
        [jnp.cos(angles), jnp.sin(angles), input_gain, middle_gain, output_gain])[None, :]
    front = front_weight if ring else lax.all_gather(front_weight, "rows", axis=0, tiled=True)
    couts = out_weight.shape[1]
    out_w = jnp.pad(out_weight, ((0, 0), (0, LANES - couts)))
    vmem = pl.BlockSpec(memory_space=pltpu.VMEM)
    dma = pltpu.SemaphoreType.DMA
    wide = time_second.shape[1]
    tall = px + 2 * TILE
    args = (
        latent.reshape(cin, px), deep.reshape(C, px), rows_in, in_weight, front,
        middle_weight, skip_weight, out_w, time_weight, time_second, time_proj,
    )
    out = pl.pallas_call(
        functools.partial(kernel, R, Q, ring),
        out_shape=jax.ShapeDtypeStruct((couts, px), F32),
        in_specs=[vmem] * len(args),
        out_specs=vmem,
        scratch_shapes=[
            pltpu.VMEM((8, cin, px), BF16),
            pltpu.VMEM((3, tall, 2 * C), BF16),
            pltpu.VMEM((3, tall, C), BF16),
            pltpu.VMEM((3, tall, C), BF16),
            pltpu.VMEM((tall, 2 * C), F32),
            pltpu.VMEM((9 * cin, px), F32),
            pltpu.VMEM((18 * C if ring else TILE, C), BF16),
            pltpu.VMEM((9 * C, C), BF16),
            pltpu.VMEM((2 * C, C), BF16),
            pltpu.VMEM((1, time_second.shape[0]), F32),
            pltpu.VMEM((Q, 1, wide), F32),
            pltpu.VMEM((3, Q, 8, LANES), F32),
            pltpu.VMEM((3, R, 8, LANES), F32),
            dma((8,)), dma((8,)), dma((3, 8)), dma((3, 8)),
            dma((R,)), dma((R,)), dma((R,)), dma((R,)), dma((R,)),
            dma((2, 3)), dma((2, 3)), dma((Q,)), dma((Q,)),
            dma((3, Q)), dma((3, Q)), dma((3, R)), dma((3, R)), dma((3,)),
        ],
        compiler_params=pltpu.CompilerParams(
            collective_id=0, has_side_effects=True, vmem_limit_bytes=56 * 1024 * 1024
        ),
    )(*args)
    return out.reshape(couts, 1, px)


UNIT = 16
PACK = 24
ALONE = 3


class Box:
    pass


def snake(pos, c, R):
    q = pos + lax.rem(c, 2) * (R - 1 - 2 * pos)
    late = q // (R // 2)
    return (1 - late) * (2 * q) + late * (2 * (R - 1 - q) + 1)


def place_of(r, c, R):
    odd, h = lax.rem(r, 2), r // 2
    q = (1 - odd) * h + odd * (R - 1 - h)
    return q + lax.rem(c, 2) * (R - 1 - 2 * q)


def dot_nt(a, b, precision=None):
    return lax.dot_general(
        a, b, (((1,), (1,)), ((), ())), preferred_element_type=F32, precision=precision
    )


def pieces_of(row):
    high = row.astype(BF16)
    rest = row - high.astype(F32)
    middle = rest.astype(BF16)
    low = (rest - middle.astype(F32)).astype(BF16)
    return jnp.concatenate(
        [high.astype(F32), middle.astype(F32), low.astype(F32)], axis=0).astype(BF16)


def fast_kernel(
    R, Q, names,
    latent, deep, timestep, in_w, front, middle, skip, out_w, time_w, time_s, time_p,
    input_gain, middle_gain, output_gain, noise, *scratch,
):
    v = Box()
    for name, ref in zip(names, scratch):
        setattr(v, name, ref)
    r = lax.axis_index("rows")
    c = lax.axis_index("cols")
    C, px = deep.shape
    cin = latent.shape[0]
    couts = out_w.shape[0]
    image = float(px * R * Q)
    FQ = time_w.shape[0]
    W = px // R
    N = W * 8
    s = place_of(r, c, R)
    me = c * R + r
    CP = (C + LANES - 1) // LANES * LANES
    GAP = CP - C

    def remote(src, dst, ssem, rsem, rr, cc):
        return pltpu.make_async_remote_copy(
            src_ref=src, dst_ref=dst, send_sem=ssem, recv_sem=rsem,
            device_id={"rows": rr, "cols": cc}, device_id_type=MESH,
        )

    def flipped(value, mask, bits):
        for b in range(bits):
            if mask >> b & 1:
                value = value + (1 - 2 * lax.rem(value // (1 << b), 2)) * (1 << b)
        return value

    others = [(flipped(r, i, 3), flipped(c, j, 2))
              for i in reversed(range(R)) for j in reversed(range(Q)) if (i, j) != (0, 0)]
    barrier = pltpu.get_barrier_semaphore()
    for i, j in others:
        pl.semaphore_signal(
            barrier, inc=1, device_id={"rows": i, "cols": j},
            device_id_type=MESH)

    mk, skr, fk = middle.shape[1], skip.shape[0], front.shape[1]
    loads = {}
    for k, (name, src, dst) in enumerate((
        ("front", front, v.front_v), ("latent", latent, v.lat_v), ("deep", deep, v.deep_v),
        ("in", in_w, v.inw), ("tw", time_w, v.tw), ("ts", time_s, v.ts),
        ("middle", middle, v.mid_v),
        ("skip", skip, v.sw.at[pl.ds(pl.multiple_of(c * skr, TILE), skr)]),
        ("tp", time_p, v.tp), ("out", out_w, v.outw_v),
        ("gain_one", input_gain, v.gain_one), ("gain_two", middle_gain, v.gain_two),
        ("gain_three", output_gain, v.gain_three),
    )):
        loads[name] = pltpu.make_async_copy(src, dst, v.ld_s.at[k])
        loads[name].start()

    tall = PACK * UNIT
    main = C // LANES * LANES
    tail = C - main

    def packed(ref, k):
        turned = ref[...].astype(F32).T
        first, second = turned[0:tall], turned[k - tall : k]
        mixed = jnp.concatenate([first[:, main:C], second[:, main:C]], axis=1)
        return jnp.concatenate([first[:, 0:main], mixed, second[:, 0:main]], axis=1).astype(BF16)

    def unpack(block, ref, start):
        def at(first):
            return pl.ds(first if isinstance(first, int) else pl.multiple_of(first, UNIT), tall)

        mixed = block[:, main : main + LANES]
        ref[at(start), 0:main] = block[:, 0:main]
        ref[at(start), main : main + LANES] = mixed
        swapped = pltpu.roll(mixed.astype(F32), LANES - tail, 1).astype(BF16)
        start = start + fk - tall
        ref[at(start), 0:main] = block[:, main + LANES : 2 * C]
        ref[at(start), main : main + LANES] = swapped

    loads["latent"].wait()
    v.lat[0, r] = v.lat_v[...]
    loads["front"].wait()
    v.fp[r] = packed(v.front_v, fk)

    pl.semaphore_wait(barrier, len(others))

    def lat_row(i, rr):
        return remote(v.lat_v, v.lat.at[0, r], v.one_s.at[0], v.one_r.at[0], rr, c)

    for i in range(1, R):
        lat_row(i, lax.rem(r + i, R)).start()

    def lat_left():
        return remote(v.lat_v, v.lat.at[2, r], v.one_s.at[1], v.one_r.at[2],
                      snake(R - 1, c - 1, R), c - 1)

    def lat_right():
        return remote(v.lat_v, v.lat.at[1, r], v.one_s.at[2], v.one_r.at[1],
                      snake(0, c + 1, R), c + 1)

    @pl.when(c > 0)
    def _():
        lat_left().start()

    @pl.when(c < Q - 1)
    def _():
        lat_right().start()

    core, xx = lax.rem(c, 2), c // 2
    mate = c + 1 - 2 * core
    over = lax.rem(c + 2, Q)
    y = lax.rem(r, 2)
    twin = r + 1 - 2 * y
    share = PACK // 2
    sizes = (ALONE, share - 2 * ALONE)

    def f_part(owner, part, x_of, core_of):
        first = (x_of * (share - ALONE), ALONE)[part]
        return v.fp.at[owner, pl.ds(
            pl.multiple_of((core_of * share + first) * UNIT, UNIT), sizes[part] * UNIT)]

    def f_move(owner, part, ssem, rr, cc):
        ref = f_part(owner, part, xx, core)
        return remote(ref, ref, ssem, v.fm_r.at[part, owner], rr, cc)

    def f_up(owner, part):
        return f_move(owner, part, v.one_s.at[6], r + 2, c)

    def f_down(owner, part):
        return f_move(owner, part, v.one_s.at[7], r - 2, c)

    def f_twin(owner, part):
        return f_move(owner, part, v.one_s.at[8], twin, c)

    def f_over(owner, x_of):
        ref = f_part(owner, 0, x_of, core)
        return remote(ref, ref, v.one_s.at[9], v.fx_r.at[owner], r, over)

    def f_mate(owner, part):
        ref = f_part(owner, part, xx, core)
        return remote(ref, ref, v.one_s.at[10], v.fo_r.at[owner], r, mate)

    def f_mate_extra(owner):
        ref = f_part(owner, 0, 1 - xx, core)
        return remote(ref, ref, v.one_s.at[10], v.fo_r.at[owner], r, mate)

    def when_row(t, body):
        @pl.when((t >= 0) & (t < R))
        def _():
            body()

    for part in (0, 1):
        when_row(r + 2, lambda: f_up(r, part).start())
        when_row(r - 2, lambda: f_down(r, part).start())
        f_twin(r, part).start()

    def from_z(d, sign, part):
        t = r + sign * 2 * d

        def body():
            f_twin(t, part).wait_recv()
            if sign < 0:
                when_row(r + 2, lambda: f_up(t, part).start())
            else:
                when_row(r - 2, lambda: f_down(t, part).start())
            f_twin(t, part).start()
            if part == 0:
                f_over(t, xx).start()
            f_mate(t, part).start()
        when_row(t, body)

    def from_y(owner, part):
        f_twin(owner, part).wait_recv()
        if part == 0:
            f_over(owner, xx).start()
        f_mate(owner, part).start()

    def from_x(owner):
        f_over(owner, 1 - xx).wait_recv()
        f_mate_extra(owner).start()

    def x_steps(d, twins):
        for sign in (-1, 1):
            t = r + sign * 2 * d
            when_row(t, lambda: from_x(t + twins * (twin - r)))

    def z_steps(d):
        for part in (0, 1):
            for sign in (-1, 1):
                from_z(d, sign, part)

    def y_steps(d):
        for part in (0, 1):
            for sign in (-1, 1):
                t = r + sign * 2 * d
                when_row(t, lambda: from_y(t + twin - r, part))

    loads["middle"].wait()
    v.mp[c] = packed(v.mid_v, mk)
    loads["skip"].wait()
    quarter = tall // 4

    def mid_copy(ref, n, rr, cc):
        kind = 1 if n in (2, 9, 11) else 0
        return remote(ref, ref, v.mid_s.at[kind], v.mid_r.at[n], rr, cc)

    def mid_rows(owner, n, of):
        return v.mp.at[owner, pl.ds(pl.multiple_of((2 * of + n) * quarter, UNIT), quarter)]

    def skip_rows(owner):
        return v.sw.at[pl.ds(pl.multiple_of(owner * skr, TILE), skr)]

    far = lax.rem(mate + 2, Q)

    def mid_over(n, owner):
        ref = skip_rows(owner) if n == 2 else mid_rows(owner, n, y)
        return mid_copy(ref, n, r, over)

    def mid_twin(n, of):
        return mid_copy(mid_rows(over, n, of), 3 + n, twin, c)

    def mid_on(n, owner, of):
        ref = skip_rows(owner) if n == 4 else mid_rows(owner, n % 2, of)
        return mid_copy(ref, 5 + n, r, mate)

    def mid_mate(owner):
        return (mid_copy(v.mp.at[owner], 10, r, mate), mid_copy(skip_rows(owner), 11, r, mate))

    mid_over(0, c).start()
    for copy in mid_mate(c):
        copy.start()

    loads["deep"].wait()
    deep_t = v.deep_v[...].astype(F32).T
    v.dr[:, C:CP] = jnp.zeros((px, GAP), BF16)
    v.dr[:, 0:C] = deep_t.astype(BF16)
    pad = jnp.zeros((1, GAP), F32)
    deep_top = jnp.concatenate([jnp.sum(deep_t, axis=0, keepdims=True), pad], axis=1)
    deep_low = jnp.concatenate([jnp.sum(deep_t * deep_t, axis=0, keepdims=True), pad], axis=1)
    def a2a_copy(q):
        return remote(v.dr.at[pl.ds(W * q, W)], v.a2a.at[r], v.one_s.at[3], v.one_r.at[3],
                      snake(q, c, R), c)

    def a2a_send():
        for q in range(R):
            @pl.when(s != q)
            def _():
                a2a_copy(q).start()

            @pl.when(s == q)
            def _():
                v.a2a[r] = v.dr[pl.ds(W * q, W), :]

    unpack(v.fp[r], v.fw, r * fk)

    loads["in"].wait()
    inw = v.inw[...].astype(F32)
    v.wb[...] = jnp.zeros(v.wb.shape, F32)
    for b in range(3):
        rows = [inw[cin * (3 * a + b) : cin * (3 * a + b + 1), :] for a in range(3)]
        band = jnp.concatenate(rows, axis=0)
        band = jnp.concatenate([jnp.zeros((3 * cin, GAP), F32), band], axis=1)
        for yy in range(R):
            lo, hi = max(0, yy - 1), min(R, yy + 2)
            v.wb[b, lo * cin : hi * cin, yy * CP : (yy + 1) * CP] = (
                band[(lo - yy + 1) * cin : (hi - yy + 1) * cin, :])

    loads["tw"].wait()
    loads["ts"].wait()
    half = FQ // 2
    index = lax.broadcasted_iota(jnp.int32, (1, half), 1).astype(F32)
    angles = timestep[0].astype(F32) * jnp.exp(-math.log(10000.0) * index / half)
    v.part[:, 0:half] = jnp.cos(angles)
    v.part[:, half:FQ] = jnp.sin(angles)
    hidden = silu(jnp.sum(dot(pieces_of(v.part[...]), v.tw[...]), axis=0, keepdims=True))
    tk = time_s.shape[0]
    for q in range(Q):
        @pl.when(c == q)
        def _():
            v.part[...] = hidden[:, q * tk : (q + 1) * tk]
    v.emb[c] = jnp.sum(dot(pieces_of(v.part[...]), v.ts[...]), axis=0, keepdims=True)

    def emb_copy(i, src_c, target):
        return remote(v.emb.at[src_c], v.emb.at[src_c], v.one_s.at[5], v.one_r.at[5], r, target)

    for i in range(1, Q):
        emb_copy(i, c, lax.rem(c + i, Q)).start()

    @pl.when((s != 0) | (c == 0))
    def _():
        v.lat[1] = jnp.zeros(v.lat.shape[1:], BF16)

    @pl.when((s != R - 1) | (c == Q - 1))
    def _():
        v.lat[2] = jnp.zeros(v.lat.shape[1:], BF16)

    def all_of(ref, n):
        return remote(ref, ref, v.one_s.at[n], v.one_r.at[n], twin, c)

    all_of(v.lat.at[0, pl.ds(0, R - 1)], 0).wait_recv()

    @pl.when((s == 0) & (c > 0))
    def _():
        all_of(v.lat.at[1], 1).wait_recv()

    @pl.when((s == R - 1) & (c < Q - 1))
    def _():
        all_of(v.lat.at[2], 2).wait_recv()

    for k in range(3):
        for q in range(R):
            v.latrows[k, cin * q : cin * (q + 1), :] = v.lat[k, q].astype(F32)
    lane = lax.broadcasted_iota(jnp.int32, (R * cin, px), 1)
    base = jnp.where((lane == px - 1) & (s == 0), v.latrows[1], v.latrows[0])
    base = jnp.where((lane == 0) & (s == R - 1), v.latrows[2], base)
    rolled = pltpu.roll(base, lax.rem(px + 1 - W * s, px), 1)
    v.tap[0:LANES, 0 : R * cin] = rolled[:, 0:LANES].T
    total = None
    for b in range(3):
        term = dot(v.tap[b : b + W, 0 : R * cin].astype(BF16), v.wb[b].astype(BF16))
        total = term if total is None else total + term
    v.sk[...] = total.astype(BF16).astype(F32)
    top = low = None
    for q in range(R):
        slab = v.sk[:, q * CP : (q + 1) * CP]
        top = slab if top is None else top + slab
        low = slab * slab if low is None else low + slab * slab
    skip_top = jnp.sum(top, axis=0, keepdims=True)
    skip_low = jnp.sum(low, axis=0, keepdims=True)

    def join(d, k):
        cut = C // LANES * LANES
        return jnp.concatenate(
            [d[:, 0:cut], d[:, cut:CP] + k[:, 0 : CP - cut], k[:, CP - cut : CP]], axis=1)

    def indicator(channels, flip):
        shape = (LANES, channels) if flip else (channels, LANES)
        size = channels // GROUPS
        ch = lax.broadcasted_iota(jnp.int32, shape, 1 if flip else 0)
        g = lax.broadcasted_iota(jnp.int32, shape, 0 if flip else 1)
        return ((ch >= g * size) & (ch < g * size + size)).astype(F32).astype(BF16)

    def sum_copy(stage, slot, i, rr, cc):
        return remote(v.sums.at[stage, slot], v.sums.at[stage, slot],
                      v.sum_s.at[stage], v.sum_r.at[stage], rr, cc)

    def reduce_start(stage, top, low):
        channels = top.shape[1]
        res = dot(jnp.concatenate([pieces_of(top), pieces_of(low)], axis=0),
                  indicator(channels, False))
        v.sums[stage, me] = jnp.sum(res[0:3], axis=0, keepdims=True) + pltpu.roll(
            jnp.sum(res[3:6], axis=0, keepdims=True), GROUPS, 1)
        for n, (i, j) in enumerate(others):
            sum_copy(stage, me, n, i, j).start()

    def sum_all(stage):
        ref = v.sums.at[stage, pl.ds(0, R * Q - 1)]
        return remote(ref, ref, v.sum_s.at[stage], v.sum_r.at[stage], twin, c)

    def reduce_end(stage, channels):
        sum_all(stage).wait_recv()
        total = jnp.sum(v.sums[stage], axis=0) / (channels // GROUPS * image)
        spread = pltpu.roll(total, LANES - GROUPS, 1) - total * total
        inverse = lax.rsqrt(jnp.maximum(spread, 0.0) + EPS)
        group = lax.broadcasted_iota(jnp.int32, (1, LANES), 1) < GROUPS
        wide = dot(jnp.concatenate([pieces_of(jnp.where(group, row, 0.0))
                                    for row in (total, inverse)], axis=0),
                   indicator(channels, True))
        return (jnp.sum(wide[0:3], axis=0, keepdims=True),
                jnp.sum(wide[3:6], axis=0, keepdims=True))

    reduce_start(0, join(deep_top, skip_top), join(deep_low, skip_low))

    inner = (s + R - 1) // R
    last = (s + 1) // R
    left = (inner * snake(s - 1, c, R) + (1 - inner) * r, c - (1 - inner))
    right = ((1 - last) * snake(s + 1, c, R) + last * r, c + last)
    has_left, has_right = left[1] >= 0, right[1] < Q

    def halo_left(stage, ext):
        return remote(ext.at[:, pl.ds(8, 8)], ext.at[:, pl.ds(N + 8, 8)],
                      v.halo_s.at[stage, 0], v.halo_r.at[stage, 1], left[0], left[1])

    def halo_right(stage, ext):
        return remote(ext.at[:, pl.ds(N, 8)], ext.at[:, pl.ds(0, 8)],
                      v.halo_s.at[stage, 1], v.halo_r.at[stage, 0], right[0], right[1])

    def halo_send(stage, ext):
        zeros = jnp.zeros((ext.shape[0], 8, LANES), F32)

        @pl.when(has_left)
        def _():
            halo_left(stage, ext).start()

        @pl.when(has_right)
        def _():
            halo_right(stage, ext).start()

        @pl.when(jnp.logical_not(has_left))
        def _():
            ext[:, 0:8, :] = zeros

        @pl.when(jnp.logical_not(has_right))
        def _():
            ext[:, N + 8 : N + 16, :] = zeros

    def halo_wait(stage, ext):
        @pl.when(has_left)
        def _():
            halo_right(stage, ext).wait_recv()

        @pl.when(has_right)
        def _():
            halo_left(stage, ext).wait_recv()

    z_steps(1)
    for part in (0, 1):
        from_y(twin, part)
    z_steps(2)
    a2a_send()
    mid_over(1, c).start()
    y_steps(1)
    for d in range(3, R // 2):
        z_steps(d)
        y_steps(d - 1)
    all_of(v.a2a.at[pl.ds(0, R - 1)], 3).wait_recv()
    for q in range(R):
        joined = join(v.a2a[q].astype(F32), v.sk[:, q * CP : (q + 1) * CP])
        for n in range(2 * C // LANES):
            v.jx[n, pl.ds(8 + q, W, 8), :] = joined[:, n * LANES : (n + 1) * LANES]
    halo_send(0, v.jx)
    from_x(twin)
    x_steps(1, 0)
    x_steps(2, 0)
    x_steps(1, 1)
    y_steps(R // 2 - 1)
    mid_over(2, c).start()
    for n in (0, 1):
        mid_over(n, over).wait_recv()
        mid_twin(n, y).start()
        mid_on(n, over, y).start()

    loads["out"].wait()
    loads["tp"].wait()
    for name in ("gain_one", "gain_two", "gain_three"):
        loads[name].wait()
    v.wr32[...] = jnp.zeros(v.wr32.shape, F32)
    for t in range(9):
        v.wr32[couts * t : couts * (t + 1), :] = v.outw_v[:, C * t : C * (t + 1)].astype(F32)
    out_taps = v.wr32[...].T.astype(BF16)

    all_of(v.emb.at[pl.ds(0, Q - 1)], 5).wait_recv()
    embedded = jnp.sum(v.emb[...], axis=0)
    time_shift = jnp.sum(dot_nt(pieces_of(silu(embedded)), v.tp[...]), axis=0, keepdims=True)

    place = lax.broadcasted_iota(jnp.int32, (W + 2, 8, 1), 0)
    inside = (
        ((place > 0) | has_left) & ((place < W + 1) | has_right))
    row = lax.broadcasted_iota(jnp.int32, (W + 2, 8, 1), 1)

    def keep_own(ext, values):
        for n in range(ext.shape[0]):
            lo, hi = n * LANES, min((n + 1) * LANES, values.shape[1])
            ext[n, 8 : N + 8, 0 : hi - lo] = values[:, lo:hi]

    def rows_of(ext, channels, first, count):
        return jnp.concatenate(
            [ext[n, first : first + count, 0 : min(LANES, channels - n * LANES)]
             for n in range(ext.shape[0])], axis=1)

    def activate(ext, stats, gain):
        center, inverse = stats
        scale = inverse * gain
        channels = gain.shape[1]
        for lo in range(0, channels, LANES):
            hi = min(channels, lo + LANES)
            z = silu((ext[lo // LANES, :, 0 : hi - lo] - center[:, lo:hi]) * scale[:, lo:hi])
            z = jnp.where(inside, z.reshape(W + 2, 8, hi - lo), 0.0)
            for a in range(3):
                if a == 1:
                    moved = z
                elif a == 0:
                    moved = jnp.where(row > 0, pltpu.roll(z, 1, 1), 0.0)
                else:
                    moved = jnp.where(row < 7, pltpu.roll(z, 7, 1), 0.0)
                flat = moved.reshape(N + 16, hi - lo)
                v.act_a[a, :, lo:hi] = flat.astype(BF16)
                v.act_b[a, :, lo:hi] = flat[8 : N + 8].astype(BF16)

    def conv_whole(channels, weight):
        acts = [v.act_b[a] if b == 1 else v.act_a[a, 8 * b : 8 * b + N]
                for a in range(3) for b in range(3)]
        return dot(jnp.concatenate(acts, axis=1), weight[:, 0:C])

    def activate_wide(ext, stats, gain):
        center, inverse = stats
        z = silu((rows_of(ext, C, 0, N + 16) - center) * (inverse * gain))
        z = jnp.where(inside, z.reshape(W + 2, 8, C), 0.0)
        moved = (jnp.where(row > 0, pltpu.roll(z, 1, 1), 0.0), z,
                 jnp.where(row < 7, pltpu.roll(z, 7, 1), 0.0))
        wide = jnp.concatenate([m.reshape(N + 16, C) for m in moved], axis=1)
        v.act_c[...] = wide.astype(BF16)
        v.act_d[...] = wide[8 : N + 8].astype(BF16)

    def conv_columns(weight):
        total = None
        for b, act in enumerate((v.act_c[0:N], v.act_d[...], v.act_c[16 : N + 16])):
            term = dot(act, weight[3 * C * b : 3 * C * (b + 1), 0:C])
            total = term if total is None else total + term
        return total

    def unpack_columns(owner):
        for side in (0, 1):
            first = owner * mk + side * tall
            stop = owner * mk + (tall if side == 0 else mk)
            while first < stop:
                tap, inside_tap = divmod(first, C)
                count = min(C - inside_tap, stop - first)
                at = first - owner * mk - side * (mk - tall)
                to = (tap % 3 * 3 + tap // 3) * C + inside_tap
                block = v.mp[owner, at : at + count]
                mixed = block[:, main : main + LANES]
                if side == 0:
                    v.mw[to : to + count, 0:main] = block[:, 0:main]
                else:
                    v.mw[to : to + count, 0:main] = block[:, main + LANES : 2 * C]
                    mixed = pltpu.roll(mixed.astype(F32), LANES - tail, 1).astype(BF16)
                v.mw[to : to + count, main : main + LANES] = mixed
                first += count

    for d in range(3, R // 2):
        x_steps(d, 0)
        x_steps(d - 1, 1)
    x_steps(R // 2 - 1, 1)

    def ready(owner):
        ref = v.fp.at[owner, pl.ds(0, share * UNIT)]
        remote(ref, ref, v.one_s.at[10], v.fo_r.at[owner], r, mate).wait_recv()
        unpack(v.fp[owner], v.fw, owner * fk)

    def when_pair(d, twins, body):
        for sign in (-1, 1):
            t = r + sign * 2 * d
            when_row(t, lambda: body(t + twins * (twin - r)))

    ready(twin)
    when_pair(1, 0, ready)
    when_pair(1, 1, ready)
    for d in range(2, R // 2 - 1):
        when_pair(d, 0, ready)
    stats = reduce_end(0, 2 * C)
    halo_wait(0, v.jx)
    activate(v.jx, stats, v.gain_one[...].reshape(1, 2 * C))

    for d in range(2, R // 2):
        when_pair(d, 1, ready)
    when_pair(R // 2 - 1, 0, ready)

    hidden_one = conv_whole(2 * C, v.fw) + time_shift
    keep_own(v.hx, hidden_one)
    reduce_start(1, jnp.sum(hidden_one, axis=0, keepdims=True),
                 jnp.sum(hidden_one * hidden_one, axis=0, keepdims=True))
    halo_send(1, v.hx)

    mid_over(2, over).wait_recv()
    mid_on(4, over, y).start()
    for n in (0, 1):
        mid_twin(n, 1 - y).wait_recv()
        mid_on(2 + n, over, 1 - y).start()
    for copy in mid_mate(mate):
        copy.wait_recv()
    for n in range(5):
        mid_on(n, far, y if n < 2 else 1 - y).wait_recv()
    for owner in range(Q):
        unpack_columns(owner)
    shortcut = dot(rows_of(v.jx, 2 * C, 8, N).astype(BF16), v.sw[...])
    stats = reduce_end(1, C)
    halo_wait(1, v.hx)
    activate_wide(v.hx, stats, v.gain_two[...].reshape(1, C))
    block_out = conv_columns(v.mw) + shortcut

    keep_own(v.ox, block_out)
    reduce_start(2, jnp.sum(block_out, axis=0, keepdims=True),
                 jnp.sum(block_out * block_out, axis=0, keepdims=True))
    halo_send(2, v.ox)
    stats = reduce_end(2, C)
    halo_wait(2, v.ox)

    center, inverse = stats
    z = silu((rows_of(v.ox, C, 0, N + 16) - center) * (inverse * v.gain_three[...].reshape(1, C)))
    z = jnp.where(inside, z.reshape(W + 2, 8, C), 0.0).reshape(N + 16, C)
    spread = dot(z.astype(BF16), out_taps)
    lane = lax.broadcasted_iota(jnp.int32, (N, LANES), 1)
    row = lax.broadcasted_iota(jnp.int32, (W, 8, 1), 1)
    total = None
    for a in range(3):
        got = None
        for b in range(3):
            t = couts * (3 * a + b)
            here = jnp.where(
                (lane >= t) & (lane < t + couts), spread[8 * b : 8 * b + N, :], 0.0)
            got = here if got is None else got + here
        got = got.reshape(W, 8, LANES)
        if a == 0:
            got = jnp.where(row > 0, pltpu.roll(got, 1, 1), 0.0)
        elif a == 2:
            got = jnp.where(row < 7, pltpu.roll(got, 7, 1), 0.0)
        total = got if total is None else total + got
    v.tap[...] = total.reshape(N, LANES)
    ordered = jnp.concatenate([v.tap[pl.ds(q, W, 8), :] for q in range(R)], axis=0)
    fold = (lax.rem(lax.broadcasted_iota(jnp.int32, (8, LANES), 1), couts)
            == lax.broadcasted_iota(jnp.int32, (8, LANES), 0)).astype(F32)
    rows = dot_nt(fold, ordered, lax.Precision.HIGHEST)[0:couts]
    for q in range(R):
        v.outs[q, :, 0:W] = rows[:, W * q : W * (q + 1)]

    def out_copy(q, rr):
        return remote(v.outs.at[q], v.outr.at[s], v.one_s.at[4], v.one_r.at[4], rr, c)

    for q in range(R):
        @pl.when(r != q)
        def _():
            out_copy(q, q).start()

        @pl.when(r == q)
        def _():
            v.outr[s] = v.outs[q]

    all_of(v.outr.at[pl.ds(0, R - 1)], 4).wait_recv()
    for q in range(R):
        noise[:, W * q : W * (q + 1)] = v.outr[q, :, 0:W]

    all_of(v.lat.at[0, pl.ds(0, R - 1)], 0).wait_send()

    @pl.when(c > 0)
    def _():
        lat_left().wait_send()

    @pl.when(c < Q - 1)
    def _():
        lat_right().wait_send()

    all_of(v.a2a.at[pl.ds(0, R - 1)], 3).wait_send()
    all_of(v.outr.at[pl.ds(0, R - 1)], 4).wait_send()
    all_of(v.emb.at[pl.ds(0, Q - 1)], 5).wait_send()
    for stage, ext in enumerate((v.jx, v.hx, v.ox)):
        sum_all(stage).wait_send()

        @pl.when(has_left)
        def _():
            halo_left(stage, ext).wait_send()

        @pl.when(has_right)
        def _():
            halo_right(stage, ext).wait_send()
    for kind, ref in enumerate((v.mp.at[pl.ds(0, 3)], v.sw.at[pl.ds(0, 3 * skr)])):
        remote(ref, ref, v.mid_s.at[kind], v.mid_r.at[0], r, mate).wait_send()
    moved = (share - ALONE) * UNIT
    level = r // 2
    for count in range(1, R // 2):
        @pl.when(level == count - 1)
        def _():
            all_of(v.fp.at[pl.ds(0, count), pl.ds(0, moved)], 6).wait_send()

        @pl.when(level == R // 2 - count)
        def _():
            all_of(v.fp.at[pl.ds(0, count), pl.ds(0, moved)], 7).wait_send()

    all_of(v.fp.at[pl.ds(0, R // 2), pl.ds(0, moved)], 8).wait_send()
    all_of(v.fp.at[pl.ds(0, R - 1), pl.ds(0, ALONE * UNIT)], 9).wait_send()
    all_of(v.fp.at[pl.ds(0, R - 1), pl.ds(0, share * UNIT)], 10).wait_send()


def fast_shards(
    R, Q,
    latent, deep, timestep, in_weight, front_weight, middle_weight, skip_weight, out_weight,
    time_weight, time_second, time_proj, input_gain, middle_gain, output_gain,
):
    C = deep.shape[0]
    cin = latent.shape[0]
    px = deep.shape[1] * deep.shape[2]
    couts = out_weight.shape[1]
    W = px // R
    N = W * 8
    CP = (C + LANES - 1) // LANES * LANES
    fk, mk, skr = front_weight.shape[0], middle_weight.shape[0], skip_weight.shape[0]
    hbm = pl.BlockSpec(memory_space=pl.ANY)
    vmem = pl.BlockSpec(memory_space=pltpu.VMEM)
    smem = pl.BlockSpec(memory_space=pltpu.SMEM)
    dma = pltpu.SemaphoreType.DMA
    args = (
        latent.reshape(cin, px), deep.reshape(C, px), timestep, in_weight, front_weight.T,
        middle_weight.T, skip_weight, out_weight.T, time_weight, time_second, time_proj.T,
        input_gain, middle_gain, output_gain,
    )
    fq, wide = time_weight.shape
    shapes = dict(
        lat_v=pltpu.VMEM((cin, px), BF16), lat=pltpu.VMEM((3, R, cin, px), BF16),
        latrows=pltpu.VMEM((3, R * cin, px), F32), deep_v=pltpu.VMEM((C, px), BF16),
        dr=pltpu.VMEM((px, CP), BF16), a2a=pltpu.VMEM((R, W, CP), BF16),
        inw=pltpu.VMEM((9 * cin, C), BF16), wb=pltpu.VMEM((3, R * cin, R * CP), F32),
        sk=pltpu.VMEM((W, R * CP), F32), jx=pltpu.VMEM((2 * C // LANES, N + 16, LANES), F32),
        hx=pltpu.VMEM((CP // LANES, N + 16, LANES), F32),
        ox=pltpu.VMEM((CP // LANES, N + 16, LANES), F32),
        act_a=pltpu.VMEM((3, N + 16, 2 * C), BF16), act_b=pltpu.VMEM((3, N, 2 * C), BF16),
        act_c=pltpu.VMEM((N + 16, 3 * C), BF16), act_d=pltpu.VMEM((N, 3 * C), BF16),
        front_v=pltpu.VMEM((C, fk), BF16), fw=pltpu.VMEM((18 * C, CP), BF16),
        fp=pltpu.VMEM((R, PACK * UNIT, 2 * C), BF16), mp=pltpu.VMEM((Q, PACK * UNIT, 2 * C), BF16),
        mid_v=pltpu.VMEM((C, mk), BF16), mw=pltpu.VMEM((9 * C, CP), BF16),
        sw=pltpu.VMEM((2 * C, C), BF16), outw_v=pltpu.VMEM((couts, 9 * C), BF16),
        wr32=pltpu.VMEM((LANES, C), F32), tw=pltpu.VMEM((fq, wide), BF16),
        ts=pltpu.VMEM(time_second.shape, BF16), tp=pltpu.VMEM((C, wide), BF16),
        part=pltpu.VMEM((1, fq), F32), emb=pltpu.VMEM((Q, 1, wide), F32),
        sums=pltpu.VMEM((3, R * Q, 1, LANES), F32), tap=pltpu.VMEM((N, LANES), F32),
        outs=pltpu.VMEM((R, couts, LANES), F32), outr=pltpu.VMEM((R, couts, LANES), F32),
        gain_one=pltpu.VMEM((2 * C,), F32), gain_two=pltpu.VMEM((C,), F32),
        gain_three=pltpu.VMEM((C,), F32),
        ld_s=dma((13,)), one_s=dma((11,)), one_r=dma((11,)), halo_s=dma((3, 2)), halo_r=dma((3, 2)),
        fm_r=dma((2, R)), fx_r=dma((R,)), fo_r=dma((R,)), mid_s=dma((2,)), mid_r=dma((12,)),
        sum_s=dma((3,)), sum_r=dma((3,)),
    )
    specs = [hbm] * len(args)
    specs[2] = smem
    out = pl.pallas_call(
        functools.partial(fast_kernel, R, Q, tuple(shapes)),
        out_shape=jax.ShapeDtypeStruct((couts, px), F32),
        in_specs=specs,
        out_specs=vmem,
        scratch_shapes=list(shapes.values()),
        compiler_params=pltpu.CompilerParams(
            collective_id=0, has_side_effects=True, vmem_limit_bytes=56 * 1024 * 1024
        ),
    )(*args)
    return out.reshape(couts, 1, px)


def solution(mesh):
    R, Q = mesh.shape["rows"], mesh.shape["cols"]

    def body(*args):
        deep, front = args[1], args[4]
        fits = (
            R == 8 and Q == 4 and deep.shape[1] == 1 and deep.shape[2] % (R * LANES // 4) == 0
            and front.shape[0] % UNIT == 0
            and PACK * UNIT < front.shape[0] <= 2 * PACK * UNIT
            and args[5].shape[0] == front.shape[0] and deep.shape[0] % LANES * 2 == LANES)
        return (fast_shards if fits else shards)(R, Q, *args)

    return jax.shard_map(
        body,
        mesh=mesh,
        in_specs=(
            P(None, "rows", "cols"), P(None, "rows", "cols"), P(), P(),
            P("rows", None), P("cols", None), P("cols", None), P(),
            P(), P("cols", None), P(), P(), P(), P(),
        ),
        out_specs=P(None, "rows", "cols"),
        check_vma=False,
    )
```

```python
import functools
import math

import jax
import jax.numpy as jnp
from jax import lax
from jax.experimental import pallas as pl
from jax.experimental.pallas import tpu as pltpu
from jax.sharding import PartitionSpec as P

GROUPS = 32
EPS = 1e-05
TILE = 16
LANES = 128
MESH = pl.DeviceIdType.MESH
F32 = jnp.float32
BF16 = jnp.bfloat16
SIDES = tuple((i, j) for i in (-1, 0, 1) for j in (-1, 0, 1) if (i, j) != (0, 0))


def dot(a, b, precision=None):
    return lax.dot_general(
        a, b, (((1,), (0,)), ((), ())), preferred_element_type=F32, precision=precision
    )


def split_dot(row, weight):
    high = row.astype(BF16)
    rest = row - high.astype(F32)
    middle = rest.astype(BF16)
    low = (rest - middle.astype(F32)).astype(BF16)
    pieces = jnp.concatenate([high.astype(F32), middle.astype(F32), low.astype(F32)], axis=0)
    return jnp.sum(dot(pieces.astype(BF16), weight), axis=0, keepdims=True)


def silu(z):
    return z / (1.0 + jnp.exp(-z))


def kernel(
    R, Q, ring,
    latent, deep, rows_in, in_w, front, middle, skip, out_w, time_w, time_s, time_p,
    noise,
    lat, jext, hext, oext, shifted, patch, fw, mw, sw, part, emb, sums_a, sums_b,
    lat_s, lat_r, halo_s, halo_r, fz_s, fy_s, fc_s, fm_r, fo_r, mid_s, mid_r, emb_s, emb_r,
    ca_s, ca_r, cb_s, cb_r, loc_s,
):
    r = lax.axis_index("rows")
    c = lax.axis_index("cols")
    C, px = deep.shape
    cin = latent.shape[0]
    image = float(px * R * Q)
    FQ = time_w.shape[0]
    gain_one = rows_in[:, FQ : FQ + 2 * C]
    gain_two = rows_in[:, FQ + 2 * C : FQ + 3 * C]
    gain_three = rows_in[:, FQ + 3 * C : FQ + 4 * C]

    def remote(src, dst, ssem, rsem, rr, cc):
        return pltpu.make_async_remote_copy(
            src_ref=src, dst_ref=dst, send_sem=ssem, recv_sem=rsem,
            device_id={"rows": rr, "cols": cc}, device_id_type=MESH,
        )

    def each(count, body):
        if count <= 8:
            for i in range(1, count):
                body(i)
        else:
            lax.fori_loop(1, count, lambda i, u: (body(i), u)[1], 0)

    barrier = pltpu.get_barrier_semaphore()

    def greet(rr, cc):
        pl.semaphore_signal(barrier, inc=1, device_id={"rows": rr, "cols": cc}, device_id_type=MESH)

    each(R, lambda i: greet(lax.rem(r + i, R), c))
    each(Q, lambda i: greet(r, lax.rem(c + i, Q)))
    for i in (-1, 1):
        for j in (-1, 1):
            greet(lax.rem(r + i + R, R), lax.rem(c + j + Q, Q))
    pl.semaphore_wait(barrier, R - 1 + Q - 1 + 4)

    def inside(rr, cc):
        return (rr >= 0) & (rr < R) & (cc >= 0) & (cc < Q)

    def lat_copy(k, rr, cc):
        i, j = SIDES[k]
        return remote(latent, lat.at[k], lat_s.at[k], lat_r.at[k], rr, cc)

    for k, (i, j) in enumerate(SIDES):
        @pl.when(inside(r + i, c + j))
        def _():
            lat_copy(k, r + i, c + j).start()

        @pl.when(jnp.logical_not(inside(r - i, c - j)))
        def _():
            lat[k] = jnp.zeros(lat.shape[1:], lat.dtype)

    parity = lax.rem(c, 2)
    mate = c + 1 - 2 * parity
    over = lax.rem(c + 2, Q)
    half_c = lax.rem(r, 2)
    twin = r + 1 - 2 * half_c
    mk, sk = middle.shape[0], skip.shape[0]

    def mid_copies(owner, s, slot_from, target):
        rows_m = pl.ds(pl.multiple_of(owner * mk, TILE), mk)
        rows_s = pl.ds(pl.multiple_of(owner * sk, TILE), sk)
        src_m, src_s = (middle, skip) if slot_from else (mw.at[rows_m], sw.at[rows_s])
        return (
            remote(src_m, mw.at[rows_m], mid_s.at[0, s], mid_r.at[0, s], r, target),
            remote(src_s, sw.at[rows_s], mid_s.at[1, s], mid_r.at[1, s], r, target),
        )

    fk = fw.shape[0] // R if ring else 0
    cut = fk // 2 // TILE * TILE
    spans = ((0, cut), (cut, fk - cut))

    def f_rows(owner, par):
        return pl.ds(pl.multiple_of(owner * fk, TILE) + spans[par][0], spans[par][1])

    def by_parity(par_of, body):
        for par in (0, 1):
            @pl.when(par_of == par)
            def _():
                body(par)

    def f_own(par, target, ssem):
        src = front.at[pl.ds(spans[par][0], spans[par][1])]
        return remote(src, fw.at[f_rows(r, par)], ssem, fm_r.at[r], target, c)

    def f_pass(owner, par, target):
        return remote(fw.at[f_rows(owner, par)], fw.at[f_rows(owner, par)],
                      fy_s.at[owner], fm_r.at[owner], target, c)

    def f_mate(owner, par):
        return remote(fw.at[f_rows(owner, par)], fw.at[f_rows(owner, par)],
                      fc_s.at[owner], fo_r.at[owner], r, mate)

    def by_distance(distances, body):
        for d in distances:
            for t in (r + 2 * d, r - 2 * d):
                @pl.when((t >= 0) & (t < R))
                def _():
                    body(t)

    locals_ = []
    if ring:
        locals_.append(pltpu.make_async_copy(
            front, fw.at[pl.ds(pl.multiple_of(r * fk, TILE), fk)], loc_s.at[0]))
    locals_.append(pltpu.make_async_copy(
        middle, mw.at[pl.ds(pl.multiple_of(c * mk, TILE), mk)], loc_s.at[1]))
    locals_.append(pltpu.make_async_copy(
        skip, sw.at[pl.ds(pl.multiple_of(c * sk, TILE), sk)], loc_s.at[2]))
    for copy in locals_:
        copy.start()

    if ring:
        def first(par):
            f_own(par, twin, fy_s.at[r]).start()
            def one(t):
                f_own(par, t, fz_s.at[t]).start()
            by_distance(range(1, R // 2), one)
        by_parity(parity, first)
    for copy in mid_copies(c, 0, True, over) + mid_copies(c, 1, True, mate):
        copy.start()

    def pass_on(distances):
        def go(par):
            def one(owner):
                f_pass(owner, par, twin).wait_recv()
                f_pass(owner, par, twin).start()
                f_mate(owner, par).start()
            by_distance(distances, one)
        by_parity(parity, go)

    for k, (i, j) in enumerate(SIDES):
        @pl.when(inside(r - i, c - j))
        def _():
            lat_copy(k, r - i, c - j).wait_recv()
    where = {side: k for k, side in enumerate(SIDES)}
    for a in range(3):
        tiles = []
        for b in range(3):
            side = (1 - a, 1 - b)
            block = latent[...] if side == (0, 0) else lat[where[side]]
            tiles.append(block.astype(F32))
        wide = jnp.concatenate(tiles, axis=1)
        for b in range(3):
            start = px + b - 1
            patch[cin * (3 * a + b) : cin * (3 * a + b + 1), :] = wide[:, start : start + px]
    skip_feat = dot(patch[...].T.astype(BF16), in_w[...]).astype(BF16)
    deep_t = deep[...].astype(F32).T.astype(BF16)
    own = pl.ds(TILE, px)
    jext[1, own, :] = jnp.concatenate([deep_t.astype(F32), skip_feat.astype(F32)], axis=1).astype(BF16)

    def halo_copy(stage, ext, k, rr, cc):
        i, j = SIDES[k]
        src = ((TILE, TILE), (TILE, px), (px, TILE))[j + 1]
        dst = ((TILE + px, TILE), (TILE, px), (0, TILE))[j + 1]
        return remote(ext.at[1, pl.ds(*src), :], ext.at[1 - i, pl.ds(*dst), :],
                      halo_s.at[stage, k], halo_r.at[stage, k], rr, cc)

    def halo_send(stage, ext):
        for k, (i, j) in enumerate(SIDES):
            @pl.when(inside(r + i, c + j))
            def _():
                halo_copy(stage, ext, k, r + i, c + j).start()

            @pl.when(jnp.logical_not(inside(r - i, c - j)))
            def _():
                dst = ((TILE + px, TILE), (TILE, px), (0, TILE))[j + 1]
                ext[1 - i, pl.ds(*dst), :] = jnp.zeros((dst[1], ext.shape[2]), ext.dtype)

    def halo_wait(stage, ext):
        for k, (i, j) in enumerate(SIDES):
            @pl.when(inside(r - i, c - j))
            def _():
                halo_copy(stage, ext, k, r - i, c - j).wait_recv()

    def indicator(channels, flip):
        shape = (LANES, channels) if flip else (channels, LANES)
        size = channels // GROUPS
        ch = lax.broadcasted_iota(jnp.int32, shape, 1 if flip else 0)
        g = lax.broadcasted_iota(jnp.int32, shape, 0 if flip else 1)
        return ((ch >= g * size) & (ch < g * size + size)).astype(F32)

    def sum_copy(buf, ssem, rsem, stage, slot, i, rr, cc):
        return remote(buf.at[stage, slot], buf.at[stage, slot],
                      ssem.at[stage, i], rsem.at[stage, i], rr, cc)

    def reduce_start(stage, values):
        top = jnp.sum(values, axis=0, keepdims=True)
        low = jnp.sum(values * values, axis=0, keepdims=True)
        both = jnp.concatenate([top, low, jnp.zeros((6, values.shape[1]), F32)], axis=0)
        sums_a[stage, c] = dot(both, indicator(values.shape[1], False), lax.Precision.HIGHEST)
        for i in range(1, Q):
            sum_copy(sums_a, ca_s, ca_r, stage, c, i, r, lax.rem(c + i, Q)).start()

    def reduce_end(stage, channels):
        for i in range(1, Q):
            s = lax.rem(c + Q - i, Q)
            sum_copy(sums_a, ca_s, ca_r, stage, s, i, r, s).wait_recv()
        sums_b[stage, r] = jnp.sum(sums_a[stage], axis=0)
        each(R, lambda i: sum_copy(sums_b, cb_s, cb_r, stage, r, i, lax.rem(r + i, R), c).start())

        def got(i):
            s = lax.rem(r + R - i, R)
            sum_copy(sums_b, cb_s, cb_r, stage, s, i, s, c).wait_recv()

        each(R, got)
        total = jnp.sum(sums_b[stage], axis=0) / (channels // GROUPS * image)
        center = total[0:1]
        inverse = lax.rsqrt(total[1:2] - center * center + EPS)
        both = jnp.concatenate([center, inverse, jnp.zeros((6, LANES), F32)], axis=0)
        wide = dot(both, indicator(channels, True), lax.Precision.HIGHEST)
        return wide[0:1], wide[1:2]

    def conv(ext, stats, gain, weight, exact=None, shift=None):
        center, inverse = stats
        if shift is not None:
            center = center - shift
        channels = ext.shape[2]
        scale = inverse * gain
        place = lax.broadcasted_iota(jnp.int32, (px + 2 * TILE, 1), 0)
        inner = (place >= TILE) & (place < TILE + px)
        total = None
        for a in (1, 0, 2):
            z = (ext[a].astype(F32) - center) * scale
            here = r + a - 1
            keep = (here >= 0) & (here < R) & (
                inner | ((place < TILE) & (c > 0)) | ((place >= TILE + px) & (c < Q - 1)))
            shifted[:, 0:channels] = jnp.where(keep, silu(z), 0.0)
            if a == 1 and exact is not None:
                shifted[own, 0:channels] = silu((exact - center) * scale)
            for b in range(3):
                act = shifted[TILE + b - 1 : TILE + b - 1 + px, 0:channels].astype(BF16)
                k = (3 * a + b) * channels
                term = dot(act, weight[k : k + channels, :])
                total = term if total is None else total + term
        return total

    joined = jext[1, own, :]
    reduce_start(0, joined.astype(F32))
    halo_send(0, jext)

    hidden = silu(split_dot(rows_in[:, 0:FQ], time_w[...]))
    tk = time_s.shape[0]
    for q in range(Q):
        @pl.when(c == q)
        def _():
            part[...] = hidden[:, q * tk : (q + 1) * tk]
    emb_own = split_dot(part[...], time_s[...])
    emb[c] = emb_own

    def emb_copy(i, src_c, tgt):
        return remote(emb.at[src_c], emb.at[src_c], emb_s.at[i], emb_r.at[i], r, tgt)

    for i in range(1, Q):
        emb_copy(i, c, lax.rem(c + i, Q)).start()

    if ring:
        pass_on((1,))
    stats = reduce_end(0, 2 * C)
    if ring:
        pass_on(range(2, R // 2))

        def from_twin(par):
            def one(t):
                owner = t + twin - r
                f_pass(owner, par, twin).wait_recv()
                f_mate(owner, par).start()
            one(r)
            by_distance(range(1, R // 2), one)
        by_parity(parity, from_twin)

    for copy in mid_copies(over, 0, False, over):
        copy.wait_recv()
    for copy in mid_copies(over, 2, False, mate):
        copy.start()

    for i in range(1, Q):
        s = lax.rem(c + Q - i, Q)
        emb_copy(i, s, s).wait_recv()
    embedded = jnp.sum(emb[...], axis=0)
    time_shift = split_dot(silu(embedded), time_p[...])

    for copy in locals_:
        copy.wait()
    halo_wait(0, jext)
    if ring:
        def from_mate(i):
            owner = lax.rem(r + i, R)
            def go(par):
                f_mate(owner, 1 - par).wait_recv()
            by_parity(parity, go)
        for i in range(1, R):
            from_mate(i)
    front_out = conv(jext, stats, gain_one, fw if ring else front)

    hext[1, own, :] = front_out.astype(BF16)
    reduce_start(1, front_out + time_shift)
    halo_send(1, hext)
    for copy in mid_copies(mate, 1, False, mate):
        copy.wait_recv()
    far = lax.rem(mate + 2, Q)
    for copy in mid_copies(far, 2, False, mate):
        copy.wait_recv()
    shortcut = dot(joined, sw[...])
    stats = reduce_end(1, C)
    halo_wait(1, hext)
    block_out = conv(hext, stats, gain_two, mw, front_out, time_shift) + shortcut

    oext[1, own, :] = block_out.astype(BF16)
    reduce_start(2, block_out)
    halo_send(2, oext)
    stats = reduce_end(2, C)
    halo_wait(2, oext)
    result = conv(oext, stats, gain_three, out_w, block_out)
    noise[...] = result.T[0 : noise.shape[0], :]

    for k, (i, j) in enumerate(SIDES):
        @pl.when(inside(r + i, c + j))
        def _():
            lat_copy(k, r + i, c + j).wait_send()
            for stage, ext in enumerate((jext, hext, oext)):
                halo_copy(stage, ext, k, r + i, c + j).wait_send()
    for i in range(1, Q):
        emb_copy(i, c, lax.rem(c + i, Q)).wait_send()
        for stage in range(3):
            sum_copy(sums_a, ca_s, ca_r, stage, c, i, r, lax.rem(c + i, Q)).wait_send()

    def sent(i):
        for stage in range(3):
            sum_copy(sums_b, cb_s, cb_r, stage, r, i, lax.rem(r + i, R), c).wait_send()

    each(R, sent)
    for copy in (mid_copies(c, 0, True, over) + mid_copies(c, 1, True, mate)
                 + mid_copies(over, 2, False, mate)):
        copy.wait_send()
    if ring:
        def last(par):
            f_own(par, twin, fy_s.at[r]).wait_send()
            def one(t):
                f_own(par, t, fz_s.at[t]).wait_send()
                f_pass(t, par, twin).wait_send()
            by_distance(range(1, R // 2), one)
            for i in range(1, R):
                f_mate(lax.rem(r + i, R), par).wait_send()
        by_parity(parity, last)


def shards(
    R, Q,
    latent, deep, timestep, in_weight, front_weight, middle_weight, skip_weight, out_weight,
    time_weight, time_second, time_proj, input_gain, middle_gain, output_gain,
):
    C = deep.shape[0]
    cin = latent.shape[0]
    px = deep.shape[1] * deep.shape[2]
    assert deep.shape[1] == 1 and Q == 4 and R % 2 == 0 and R > 2
    ring = R <= 8 and front_weight.shape[0] % TILE == 0
    half = time_weight.shape[0] // 2
    ratios = jnp.exp(-math.log(10000.0) * jnp.arange(half, dtype=F32) / half)
    angles = timestep[0].astype(F32) * ratios
    rows_in = jnp.concatenate(
        [jnp.cos(angles), jnp.sin(angles), input_gain, middle_gain, output_gain])[None, :]
    front = front_weight if ring else lax.all_gather(front_weight, "rows", axis=0, tiled=True)
    couts = out_weight.shape[1]
    out_w = jnp.pad(out_weight, ((0, 0), (0, LANES - couts)))
    vmem = pl.BlockSpec(memory_space=pltpu.VMEM)
    dma = pltpu.SemaphoreType.DMA
    wide = time_second.shape[1]
    tall = px + 2 * TILE
    args = (
        latent.reshape(cin, px), deep.reshape(C, px), rows_in, in_weight, front,
        middle_weight, skip_weight, out_w, time_weight, time_second, time_proj,
    )
    out = pl.pallas_call(
        functools.partial(kernel, R, Q, ring),
        out_shape=jax.ShapeDtypeStruct((couts, px), F32),
        in_specs=[vmem] * len(args),
        out_specs=vmem,
        scratch_shapes=[
            pltpu.VMEM((8, cin, px), BF16),
            pltpu.VMEM((3, tall, 2 * C), BF16),
            pltpu.VMEM((3, tall, C), BF16),
            pltpu.VMEM((3, tall, C), BF16),
            pltpu.VMEM((tall, 2 * C), F32),
            pltpu.VMEM((9 * cin, px), F32),
            pltpu.VMEM((18 * C if ring else TILE, C), BF16),
            pltpu.VMEM((9 * C, C), BF16),
            pltpu.VMEM((2 * C, C), BF16),
            pltpu.VMEM((1, time_second.shape[0]), F32),
            pltpu.VMEM((Q, 1, wide), F32),
            pltpu.VMEM((3, Q, 8, LANES), F32),
            pltpu.VMEM((3, R, 8, LANES), F32),
            dma((8,)), dma((8,)), dma((3, 8)), dma((3, 8)),
            dma((R,)), dma((R,)), dma((R,)), dma((R,)), dma((R,)),
            dma((2, 3)), dma((2, 3)), dma((Q,)), dma((Q,)),
            dma((3, Q)), dma((3, Q)), dma((3, R)), dma((3, R)), dma((3,)),
        ],
        compiler_params=pltpu.CompilerParams(
            collective_id=0, has_side_effects=True, vmem_limit_bytes=56 * 1024 * 1024
        ),
    )(*args)
    return out.reshape(couts, 1, px)


UNIT = 16
PACK = 24
ALONE = 3


class Box:
    pass


def snake(pos, c, R):
    q = pos + lax.rem(c, 2) * (R - 1 - 2 * pos)
    late = q // (R // 2)
    return (1 - late) * (2 * q) + late * (2 * (R - 1 - q) + 1)


def place_of(r, c, R):
    odd, h = lax.rem(r, 2), r // 2
    q = (1 - odd) * h + odd * (R - 1 - h)
    return q + lax.rem(c, 2) * (R - 1 - 2 * q)


def dot_nt(a, b, precision=None):
    return lax.dot_general(
        a, b, (((1,), (1,)), ((), ())), preferred_element_type=F32, precision=precision
    )


def pieces_of(row):
    high = row.astype(BF16)
    rest = row - high.astype(F32)
    middle = rest.astype(BF16)
    low = (rest - middle.astype(F32)).astype(BF16)
    return jnp.concatenate(
        [high.astype(F32), middle.astype(F32), low.astype(F32)], axis=0).astype(BF16)


def fast_kernel(
    R, Q, names,
    latent, deep, timestep, in_w, front, middle, skip, out_w, time_w, time_s, time_p,
    input_gain, middle_gain, output_gain, noise, *scratch,
):
    v = Box()
    for name, ref in zip(names, scratch):
        setattr(v, name, ref)
    r = lax.axis_index("rows")
    c = lax.axis_index("cols")
    C, px = deep.shape
    cin = latent.shape[0]
    couts = out_w.shape[0]
    image = float(px * R * Q)
    FQ = time_w.shape[0]
    W = px // R
    N = W * 8
    s = place_of(r, c, R)
    me = c * R + r
    CP = (C + LANES - 1) // LANES * LANES
    GAP = CP - C

    def remote(src, dst, ssem, rsem, rr, cc):
        return pltpu.make_async_remote_copy(
            src_ref=src, dst_ref=dst, send_sem=ssem, recv_sem=rsem,
            device_id={"rows": rr, "cols": cc}, device_id_type=MESH,
        )

    def flipped(value, mask, bits):
        for b in range(bits):
            if mask >> b & 1:
                value = value + (1 - 2 * lax.rem(value // (1 << b), 2)) * (1 << b)
        return value

    others = [(flipped(r, i, 3), flipped(c, j, 2))
              for i in reversed(range(R)) for j in reversed(range(Q)) if (i, j) != (0, 0)]
    barrier = pltpu.get_barrier_semaphore()
    for i, j in others:
        pl.semaphore_signal(
            barrier, inc=1, device_id={"rows": i, "cols": j},
            device_id_type=MESH)

    mk, skr, fk = middle.shape[1], skip.shape[0], front.shape[1]
    loads = {}
    for k, (name, src, dst) in enumerate((
        ("front", front, v.front_v), ("latent", latent, v.lat_v), ("deep", deep, v.deep_v),
        ("in", in_w, v.inw), ("tw", time_w, v.tw), ("ts", time_s, v.ts),
        ("middle", middle, v.mid_v),
        ("skip", skip, v.sw.at[pl.ds(pl.multiple_of(c * skr, TILE), skr)]),
        ("tp", time_p, v.tp), ("out", out_w, v.outw_v),
        ("gain_one", input_gain, v.gain_one), ("gain_two", middle_gain, v.gain_two),
        ("gain_three", output_gain, v.gain_three),
    )):
        loads[name] = pltpu.make_async_copy(src, dst, v.ld_s.at[k])
        loads[name].start()

    tall = PACK * UNIT
    main = C // LANES * LANES
    tail = C - main

    def side_by_side(first, second):
        mixed = jnp.concatenate([first[:, main:C], second[:, main:C]], axis=1)
        return jnp.concatenate([first[:, 0:main], mixed, second[:, 0:main]], axis=1).astype(BF16)

    def packed(ref, k):
        turned = ref[...].astype(F32).T
        first, second = turned[0:tall], turned[k - tall : k]
        return side_by_side(first, second)

    def unpack(block, ref, start):
        def at(first):
            return pl.ds(first if isinstance(first, int) else pl.multiple_of(first, UNIT), tall)

        mixed = block[:, main : main + LANES]
        ref[at(start), 0:main] = block[:, 0:main]
        ref[at(start), main : main + LANES] = mixed
        swapped = pltpu.roll(mixed.astype(F32), LANES - tail, 1).astype(BF16)
        start = start + fk - tall
        ref[at(start), 0:main] = block[:, main + LANES : 2 * C]
        ref[at(start), main : main + LANES] = swapped

    loads["latent"].wait()
    v.lat[0, r] = v.lat_v[...]
    loads["front"].wait()
    v.fp[r] = packed(v.front_v, fk)

    pl.semaphore_wait(barrier, len(others))

    def lat_row(i, rr):
        return remote(v.lat_v, v.lat.at[0, r], v.one_s.at[0], v.one_r.at[0], rr, c)

    for i in range(1, R):
        lat_row(i, lax.rem(r + i, R)).start()

    def lat_left():
        return remote(v.lat_v, v.lat.at[2, r], v.one_s.at[1], v.one_r.at[2],
                      snake(R - 1, c - 1, R), c - 1)

    def lat_right():
        return remote(v.lat_v, v.lat.at[1, r], v.one_s.at[2], v.one_r.at[1],
                      snake(0, c + 1, R), c + 1)

    @pl.when(c > 0)
    def _():
        lat_left().start()

    @pl.when(c < Q - 1)
    def _():
        lat_right().start()

    core, xx = lax.rem(c, 2), c // 2
    mate = c + 1 - 2 * core
    over = lax.rem(c + 2, Q)
    y = lax.rem(r, 2)
    twin = r + 1 - 2 * y
    share = PACK // 2
    sizes = (ALONE, share - 2 * ALONE)

    def f_part(owner, part, x_of, core_of):
        first = (x_of * (share - ALONE), ALONE, share // 2)[part]
        return v.fp.at[owner, pl.ds(
            pl.multiple_of((core_of * share + first) * UNIT, UNIT), sizes[part] * UNIT)]

    def f_move(owner, part, ssem, rr, cc):
        ref = f_part(owner, part, xx, core)
        return remote(ref, ref, ssem, v.fm_r.at[part, owner], rr, cc)

    def f_up(owner, part):
        return f_move(owner, part, v.one_s.at[6], r + 2, c)

    def f_down(owner, part):
        return f_move(owner, part, v.one_s.at[7], r - 2, c)

    def f_twin(owner, part):
        return f_move(owner, part, v.one_s.at[8], twin, c)

    def f_over(owner, x_of):
        ref = f_part(owner, 0, x_of, core)
        return remote(ref, ref, v.one_s.at[9], v.fx_r.at[owner], r, over)

    def f_mate(owner, part):
        ref = f_part(owner, part, xx, core)
        return remote(ref, ref, v.one_s.at[10], v.fo_r.at[owner], r, mate)

    def f_mate_extra(owner):
        ref = f_part(owner, 0, 1 - xx, core)
        return remote(ref, ref, v.one_s.at[10], v.fo_r.at[owner], r, mate)

    def when_row(t, body):
        @pl.when((t >= 0) & (t < R))
        def _():
            body()

    for part in range(2):
        when_row(r + 2, lambda: f_up(r, part).start())
        when_row(r - 2, lambda: f_down(r, part).start())
        f_twin(r, part).start()

    def from_z(d, sign, part):
        t = r + sign * 2 * d

        def body():
            f_twin(t, part).wait_recv()
            if sign < 0:
                when_row(r + 2, lambda: f_up(t, part).start())
            else:
                when_row(r - 2, lambda: f_down(t, part).start())
            f_twin(t, part).start()
            if part == 0:
                f_over(t, xx).start()
            f_mate(t, part).start()
        when_row(t, body)

    def from_y(owner, part):
        f_twin(owner, part).wait_recv()
        if part == 0:
            f_over(owner, xx).start()
        f_mate(owner, part).start()

    def from_x(owner):
        f_over(owner, 1 - xx).wait_recv()
        f_mate_extra(owner).start()

    def x_steps(d, twins):
        for sign in (-1, 1):
            t = r + sign * 2 * d
            when_row(t, lambda: from_x(t + twins * (twin - r)))

    def z_steps(d):
        for part in range(2):
            for sign in (-1, 1):
                from_z(d, sign, part)

    def y_steps(d):
        for part in range(2):
            for sign in (-1, 1):
                t = r + sign * 2 * d
                when_row(t, lambda: from_y(t + twin - r, part))

    loads["middle"].wait()
    v.mp[c] = packed(v.mid_v, mk)
    loads["skip"].wait()
    quarter = tall // 4

    def mid_copy(ref, n, rr, cc):
        kind = 1 if n in (2, 9, 11) else 0
        return remote(ref, ref, v.mid_s.at[kind], v.mid_r.at[n], rr, cc)

    def mid_rows(owner, n, of):
        return v.mp.at[owner, pl.ds(pl.multiple_of((2 * of + n) * quarter, UNIT), quarter)]

    def skip_rows(owner):
        return v.sw.at[pl.ds(pl.multiple_of(owner * skr, TILE), skr)]

    far = lax.rem(mate + 2, Q)

    def mid_over(n, owner):
        ref = skip_rows(owner) if n == 2 else mid_rows(owner, n, y)
        return mid_copy(ref, n, r, over)

    def mid_twin(n, of):
        return mid_copy(mid_rows(over, n, of), 3 + n, twin, c)

    def mid_on(n, owner, of):
        ref = skip_rows(owner) if n == 4 else mid_rows(owner, n % 2, of)
        return mid_copy(ref, 5 + n, r, mate)

    def mid_mate(owner):
        return (mid_copy(v.mp.at[owner], 10, r, mate), mid_copy(skip_rows(owner), 11, r, mate))

    mid_over(0, c).start()
    for copy in mid_mate(c):
        copy.start()

    loads["deep"].wait()
    deep_t = v.deep_v[...].astype(F32).T
    halves = deep_t.reshape(R, 2, W // 2, C)
    doubled = side_by_side(halves[:, 0].reshape(px // 2, C), halves[:, 1].reshape(px // 2, C))
    for q in range(R):
        v.dr[q] = doubled[W // 2 * q : W // 2 * (q + 1)]
    pad = jnp.zeros((1, GAP), F32)
    deep_top = jnp.concatenate([jnp.sum(deep_t, axis=0, keepdims=True), pad], axis=1)
    deep_low = jnp.concatenate([jnp.sum(deep_t * deep_t, axis=0, keepdims=True), pad], axis=1)
    def a2a_copy(q):
        return remote(v.dr.at[q], v.a2a.at[r], v.one_s.at[3], v.one_r.at[3],
                      snake(q, c, R), c)

    def a2a_send():
        for q in range(R):
            @pl.when(s != q)
            def _():
                a2a_copy(q).start()

            @pl.when(s == q)
            def _():
                v.a2a[r] = v.dr[q]

    unpack(v.fp[r], v.fw, r * fk)

    loads["in"].wait()
    inw = v.inw[...].astype(F32)
    v.wb[...] = jnp.zeros(v.wb.shape, F32)
    for b in range(3):
        rows = [inw[cin * (3 * a + b) : cin * (3 * a + b + 1), :] for a in range(3)]
        band = jnp.concatenate(rows, axis=0)
        band = jnp.concatenate([jnp.zeros((3 * cin, GAP), F32), band], axis=1)
        for yy in range(R):
            lo, hi = max(0, yy - 1), min(R, yy + 2)
            v.wb[b, lo * cin : hi * cin, yy * CP : (yy + 1) * CP] = (
                band[(lo - yy + 1) * cin : (hi - yy + 1) * cin, :])

    loads["tw"].wait()
    loads["ts"].wait()
    half = FQ // 2
    index = lax.broadcasted_iota(jnp.int32, (1, half), 1).astype(F32)
    angles = timestep[0].astype(F32) * jnp.exp(-math.log(10000.0) * index / half)
    v.part[:, 0:half] = jnp.cos(angles)
    v.part[:, half:FQ] = jnp.sin(angles)
    hidden = silu(jnp.sum(dot(pieces_of(v.part[...]), v.tw[...]), axis=0, keepdims=True))
    tk = time_s.shape[0]
    for q in range(Q):
        @pl.when(c == q)
        def _():
            v.part[...] = hidden[:, q * tk : (q + 1) * tk]
    v.emb[c] = jnp.sum(dot(pieces_of(v.part[...]), v.ts[...]), axis=0, keepdims=True)

    def emb_copy(i, src_c, target):
        return remote(v.emb.at[src_c], v.emb.at[src_c], v.one_s.at[5], v.one_r.at[5], r, target)

    for i in range(1, Q):
        emb_copy(i, c, lax.rem(c + i, Q)).start()

    @pl.when((s != 0) | (c == 0))
    def _():
        v.lat[1] = jnp.zeros(v.lat.shape[1:], BF16)

    @pl.when((s != R - 1) | (c == Q - 1))
    def _():
        v.lat[2] = jnp.zeros(v.lat.shape[1:], BF16)

    def all_of(ref, n):
        return remote(ref, ref, v.one_s.at[n], v.one_r.at[n], twin, c)

    all_of(v.lat.at[0, pl.ds(0, R - 1)], 0).wait_recv()

    @pl.when((s == 0) & (c > 0))
    def _():
        all_of(v.lat.at[1], 1).wait_recv()

    @pl.when((s == R - 1) & (c < Q - 1))
    def _():
        all_of(v.lat.at[2], 2).wait_recv()

    for k in range(3):
        for q in range(R):
            v.latrows[k, cin * q : cin * (q + 1), :] = v.lat[k, q].astype(F32)
    lane = lax.broadcasted_iota(jnp.int32, (R * cin, px), 1)
    base = jnp.where((lane == px - 1) & (s == 0), v.latrows[1], v.latrows[0])
    base = jnp.where((lane == 0) & (s == R - 1), v.latrows[2], base)
    rolled = pltpu.roll(base, lax.rem(px + 1 - W * s, px), 1)
    v.tap[0:LANES, 0 : R * cin] = rolled[:, 0:LANES].T
    total = None
    for b in range(3):
        term = dot(v.tap[b : b + W, 0 : R * cin].astype(BF16), v.wb[b].astype(BF16))
        total = term if total is None else total + term
    v.sk[...] = total.astype(BF16).astype(F32)
    top = low = None
    for q in range(R):
        slab = v.sk[:, q * CP : (q + 1) * CP]
        top = slab if top is None else top + slab
        low = slab * slab if low is None else low + slab * slab
    skip_top = jnp.sum(top, axis=0, keepdims=True)
    skip_low = jnp.sum(low, axis=0, keepdims=True)

    def join(d, k):
        cut = C // LANES * LANES
        return jnp.concatenate(
            [d[:, 0:cut], d[:, cut:CP] + k[:, 0 : CP - cut], k[:, CP - cut : CP]], axis=1)

    def indicator(channels, flip):
        shape = (LANES, channels) if flip else (channels, LANES)
        size = channels // GROUPS
        ch = lax.broadcasted_iota(jnp.int32, shape, 1 if flip else 0)
        g = lax.broadcasted_iota(jnp.int32, shape, 0 if flip else 1)
        return ((ch >= g * size) & (ch < g * size + size)).astype(F32).astype(BF16)

    def sum_copy(stage, slot, i, rr, cc):
        return remote(v.sums.at[stage, slot], v.sums.at[stage, slot],
                      v.sum_s.at[stage], v.sum_r.at[stage], rr, cc)

    def reduce_start(stage, top, low):
        channels = top.shape[1]
        res = dot(jnp.concatenate([pieces_of(top), pieces_of(low)], axis=0),
                  indicator(channels, False))
        v.sums[stage, me] = jnp.sum(res[0:3], axis=0, keepdims=True) + pltpu.roll(
            jnp.sum(res[3:6], axis=0, keepdims=True), GROUPS, 1)
        for n, (i, j) in enumerate(others):
            sum_copy(stage, me, n, i, j).start()

    def sum_all(stage):
        ref = v.sums.at[stage, pl.ds(0, R * Q - 1)]
        return remote(ref, ref, v.sum_s.at[stage], v.sum_r.at[stage], twin, c)

    def reduce_end(stage, channels):
        sum_all(stage).wait_recv()
        total = jnp.sum(v.sums[stage], axis=0) / (channels // GROUPS * image)
        spread = pltpu.roll(total, LANES - GROUPS, 1) - total * total
        inverse = lax.rsqrt(jnp.maximum(spread, 0.0) + EPS)
        group = lax.broadcasted_iota(jnp.int32, (1, LANES), 1) < GROUPS
        wide = dot(jnp.concatenate([pieces_of(jnp.where(group, row, 0.0))
                                    for row in (total, inverse)], axis=0),
                   indicator(channels, True))
        return (jnp.sum(wide[0:3], axis=0, keepdims=True),
                jnp.sum(wide[3:6], axis=0, keepdims=True))

    reduce_start(0, join(deep_top, skip_top), join(deep_low, skip_low))

    inner = (s + R - 1) // R
    last = (s + 1) // R
    left = (inner * snake(s - 1, c, R) + (1 - inner) * r, c - (1 - inner))
    right = ((1 - last) * snake(s + 1, c, R) + last * r, c + last)
    has_left, has_right = left[1] >= 0, right[1] < Q

    def halo_left(stage, ext):
        return remote(ext.at[:, pl.ds(8, 8)], ext.at[:, pl.ds(N + 8, 8)],
                      v.halo_s.at[stage, 0], v.halo_r.at[stage, 1], left[0], left[1])

    def halo_right(stage, ext):
        return remote(ext.at[:, pl.ds(N, 8)], ext.at[:, pl.ds(0, 8)],
                      v.halo_s.at[stage, 1], v.halo_r.at[stage, 0], right[0], right[1])

    def halo_send(stage, ext):
        zeros = jnp.zeros((ext.shape[0], 8, LANES), F32)

        @pl.when(has_left)
        def _():
            halo_left(stage, ext).start()

        @pl.when(has_right)
        def _():
            halo_right(stage, ext).start()

        @pl.when(jnp.logical_not(has_left))
        def _():
            ext[:, 0:8, :] = zeros

        @pl.when(jnp.logical_not(has_right))
        def _():
            ext[:, N + 8 : N + 16, :] = zeros

    def halo_wait(stage, ext):
        @pl.when(has_left)
        def _():
            halo_right(stage, ext).wait_recv()

        @pl.when(has_right)
        def _():
            halo_left(stage, ext).wait_recv()

    z_steps(1)
    for part in range(2):
        from_y(twin, part)
    z_steps(2)
    a2a_send()
    mid_over(1, c).start()
    y_steps(1)
    for d in range(3, R // 2):
        z_steps(d)
        y_steps(d - 1)
    all_of(v.a2a.at[pl.ds(0, R - 1)], 3).wait_recv()
    for q in range(R):
        block = v.a2a[q].astype(F32)
        mixed = block[:, main : main + LANES]
        used = lax.broadcasted_iota(jnp.int32, mixed.shape, 1) < tail
        upper = jnp.concatenate([block[:, 0:main], jnp.where(used, mixed, 0.0)], axis=1)
        lower = jnp.concatenate(
            [block[:, main + LANES : 2 * C],
             jnp.where(used, pltpu.roll(mixed, LANES - tail, 1), 0.0)], axis=1)
        joined = join(jnp.concatenate([upper, lower], axis=0), v.sk[:, q * CP : (q + 1) * CP])
        for n in range(2 * C // LANES):
            v.jx[n, pl.ds(8 + q, W, 8), :] = joined[:, n * LANES : (n + 1) * LANES]
    halo_send(0, v.jx)
    from_x(twin)
    x_steps(1, 0)
    x_steps(2, 0)
    x_steps(1, 1)
    y_steps(R // 2 - 1)
    mid_over(2, c).start()
    for n in (0, 1):
        mid_over(n, over).wait_recv()
        mid_twin(n, y).start()
        mid_on(n, over, y).start()

    loads["out"].wait()
    loads["tp"].wait()
    for name in ("gain_one", "gain_two", "gain_three"):
        loads[name].wait()
    v.wr32[...] = jnp.zeros(v.wr32.shape, F32)
    for t in range(9):
        v.wr32[couts * t : couts * (t + 1), :] = v.outw_v[:, C * t : C * (t + 1)].astype(F32)
    out_taps = v.wr32[...].T.astype(BF16)

    all_of(v.emb.at[pl.ds(0, Q - 1)], 5).wait_recv()
    embedded = jnp.sum(v.emb[...], axis=0)
    time_shift = jnp.sum(dot_nt(pieces_of(silu(embedded)), v.tp[...]), axis=0, keepdims=True)

    place = lax.broadcasted_iota(jnp.int32, (W + 2, 8, 1), 0)
    inside = (
        ((place > 0) | has_left) & ((place < W + 1) | has_right))
    row = lax.broadcasted_iota(jnp.int32, (W + 2, 8, 1), 1)

    def keep_own(ext, values):
        for n in range(ext.shape[0]):
            lo, hi = n * LANES, min((n + 1) * LANES, values.shape[1])
            ext[n, 8 : N + 8, 0 : hi - lo] = values[:, lo:hi]

    def rows_of(ext, channels, first, count):
        return jnp.concatenate(
            [ext[n, first : first + count, 0 : min(LANES, channels - n * LANES)]
             for n in range(ext.shape[0])], axis=1)

    def activate(ext, stats, gain):
        center, inverse = stats
        scale = inverse * gain
        channels = gain.shape[1]
        for lo in range(0, channels, LANES):
            hi = min(channels, lo + LANES)
            z = silu((ext[lo // LANES, :, 0 : hi - lo] - center[:, lo:hi]) * scale[:, lo:hi])
            z = jnp.where(inside, z.reshape(W + 2, 8, hi - lo), 0.0)
            for a in range(3):
                if a == 1:
                    moved = z
                elif a == 0:
                    moved = jnp.where(row > 0, pltpu.roll(z, 1, 1), 0.0)
                else:
                    moved = jnp.where(row < 7, pltpu.roll(z, 7, 1), 0.0)
                flat = moved.reshape(N + 16, hi - lo)
                v.act_a[a, :, lo:hi] = flat.astype(BF16)
                v.act_b[a, :, lo:hi] = flat[8 : N + 8].astype(BF16)

    def conv_whole(channels, weight):
        acts = [v.act_b[a] if b == 1 else v.act_a[a, 8 * b : 8 * b + N]
                for a in range(3) for b in range(3)]
        return dot(jnp.concatenate(acts, axis=1), weight[:, 0:C])

    def activate_wide(ext, stats, gain):
        center, inverse = stats
        z = silu((rows_of(ext, C, 0, N + 16) - center) * (inverse * gain))
        z = jnp.where(inside, z.reshape(W + 2, 8, C), 0.0)
        moved = (jnp.where(row > 0, pltpu.roll(z, 1, 1), 0.0), z,
                 jnp.where(row < 7, pltpu.roll(z, 7, 1), 0.0))
        wide = jnp.concatenate([m.reshape(N + 16, C) for m in moved], axis=1)
        v.act_c[...] = wide.astype(BF16)
        v.act_d[...] = wide[8 : N + 8].astype(BF16)

    def conv_columns(weight):
        total = None
        for b, act in enumerate((v.act_c[0:N], v.act_d[...], v.act_c[16 : N + 16])):
            term = dot(act, weight[3 * C * b : 3 * C * (b + 1), 0:C])
            total = term if total is None else total + term
        return total

    def unpack_columns(owner):
        for side in (0, 1):
            first = owner * mk + side * tall
            stop = owner * mk + (tall if side == 0 else mk)
            while first < stop:
                tap, inside_tap = divmod(first, C)
                count = min(C - inside_tap, stop - first)
                at = first - owner * mk - side * (mk - tall)
                to = (tap % 3 * 3 + tap // 3) * C + inside_tap
                block = v.mp[owner, at : at + count]
                mixed = block[:, main : main + LANES]
                if side == 0:
                    v.mw[to : to + count, 0:main] = block[:, 0:main]
                else:
                    v.mw[to : to + count, 0:main] = block[:, main + LANES : 2 * C]
                    mixed = pltpu.roll(mixed.astype(F32), LANES - tail, 1).astype(BF16)
                v.mw[to : to + count, main : main + LANES] = mixed
                first += count

    for d in range(3, R // 2):
        x_steps(d, 0)
        x_steps(d - 1, 1)
    x_steps(R // 2 - 1, 1)

    def ready(owner):
        ref = v.fp.at[owner, pl.ds(0, share * UNIT)]
        remote(ref, ref, v.one_s.at[10], v.fo_r.at[owner], r, mate).wait_recv()
        unpack(v.fp[owner], v.fw, owner * fk)

    def when_pair(d, twins, body):
        for sign in (-1, 1):
            t = r + sign * 2 * d
            when_row(t, lambda: body(t + twins * (twin - r)))

    ready(twin)
    when_pair(1, 0, ready)
    when_pair(1, 1, ready)
    for d in range(2, R // 2 - 1):
        when_pair(d, 0, ready)
    stats = reduce_end(0, 2 * C)
    halo_wait(0, v.jx)
    activate(v.jx, stats, v.gain_one[...].reshape(1, 2 * C))

    for d in range(2, R // 2):
        when_pair(d, 1, ready)
    when_pair(R // 2 - 1, 0, ready)

    hidden_one = conv_whole(2 * C, v.fw) + time_shift
    keep_own(v.hx, hidden_one)
    reduce_start(1, jnp.sum(hidden_one, axis=0, keepdims=True),
                 jnp.sum(hidden_one * hidden_one, axis=0, keepdims=True))
    halo_send(1, v.hx)

    mid_over(2, over).wait_recv()
    mid_on(4, over, y).start()
    for n in (0, 1):
        mid_twin(n, 1 - y).wait_recv()
        mid_on(2 + n, over, 1 - y).start()
    for copy in mid_mate(mate):
        copy.wait_recv()
    for n in range(5):
        mid_on(n, far, y if n < 2 else 1 - y).wait_recv()
    for owner in range(Q):
        unpack_columns(owner)
    shortcut = dot(rows_of(v.jx, 2 * C, 8, N).astype(BF16), v.sw[...])
    stats = reduce_end(1, C)
    halo_wait(1, v.hx)
    activate_wide(v.hx, stats, v.gain_two[...].reshape(1, C))
    block_out = conv_columns(v.mw) + shortcut

    keep_own(v.ox, block_out)
    reduce_start(2, jnp.sum(block_out, axis=0, keepdims=True),
                 jnp.sum(block_out * block_out, axis=0, keepdims=True))
    halo_send(2, v.ox)
    stats = reduce_end(2, C)
    halo_wait(2, v.ox)

    center, inverse = stats
    z = silu((rows_of(v.ox, C, 0, N + 16) - center) * (inverse * v.gain_three[...].reshape(1, C)))
    z = jnp.where(inside, z.reshape(W + 2, 8, C), 0.0).reshape(N + 16, C)
    spread = dot(z.astype(BF16), out_taps)
    lane = lax.broadcasted_iota(jnp.int32, (N, LANES), 1)
    row = lax.broadcasted_iota(jnp.int32, (W, 8, 1), 1)
    total = None
    for a in range(3):
        got = None
        for b in range(3):
            t = couts * (3 * a + b)
            here = jnp.where(
                (lane >= t) & (lane < t + couts), spread[8 * b : 8 * b + N, :], 0.0)
            got = here if got is None else got + here
        got = got.reshape(W, 8, LANES)
        if a == 0:
            got = jnp.where(row > 0, pltpu.roll(got, 1, 1), 0.0)
        elif a == 2:
            got = jnp.where(row < 7, pltpu.roll(got, 7, 1), 0.0)
        total = got if total is None else total + got
    v.tap[...] = total.reshape(N, LANES)
    ordered = jnp.concatenate([v.tap[pl.ds(q, W, 8), :] for q in range(R)], axis=0)
    fold = (lax.rem(lax.broadcasted_iota(jnp.int32, (8, LANES), 1), couts)
            == lax.broadcasted_iota(jnp.int32, (8, LANES), 0)).astype(F32)
    rows = dot_nt(fold, ordered, lax.Precision.HIGHEST)[0:couts]
    for q in range(R):
        v.outs[q, :, 0:W] = rows[:, W * q : W * (q + 1)]

    def out_copy(q, rr):
        return remote(v.outs.at[q], v.outr.at[s], v.one_s.at[4], v.one_r.at[4], rr, c)

    for q in range(R):
        @pl.when(r != q)
        def _():
            out_copy(q, q).start()

        @pl.when(r == q)
        def _():
            v.outr[s] = v.outs[q]

    all_of(v.outr.at[pl.ds(0, R - 1)], 4).wait_recv()
    for q in range(R):
        noise[:, W * q : W * (q + 1)] = v.outr[q, :, 0:W]

    all_of(v.lat.at[0, pl.ds(0, R - 1)], 0).wait_send()

    @pl.when(c > 0)
    def _():
        lat_left().wait_send()

    @pl.when(c < Q - 1)
    def _():
        lat_right().wait_send()

    all_of(v.a2a.at[pl.ds(0, R - 1)], 3).wait_send()
    all_of(v.outr.at[pl.ds(0, R - 1)], 4).wait_send()
    all_of(v.emb.at[pl.ds(0, Q - 1)], 5).wait_send()
    for stage, ext in enumerate((v.jx, v.hx, v.ox)):
        sum_all(stage).wait_send()

        @pl.when(has_left)
        def _():
            halo_left(stage, ext).wait_send()

        @pl.when(has_right)
        def _():
            halo_right(stage, ext).wait_send()
    for kind, ref in enumerate((v.mp.at[pl.ds(0, 3)], v.sw.at[pl.ds(0, 3 * skr)])):
        remote(ref, ref, v.mid_s.at[kind], v.mid_r.at[0], r, mate).wait_send()
    moved = (share - ALONE) * UNIT
    level = r // 2
    for count in range(1, R // 2):
        @pl.when(level == count - 1)
        def _():
            all_of(v.fp.at[pl.ds(0, count), pl.ds(0, moved)], 6).wait_send()

        @pl.when(level == R // 2 - count)
        def _():
            all_of(v.fp.at[pl.ds(0, count), pl.ds(0, moved)], 7).wait_send()

    all_of(v.fp.at[pl.ds(0, R // 2), pl.ds(0, moved)], 8).wait_send()
    all_of(v.fp.at[pl.ds(0, R - 1), pl.ds(0, ALONE * UNIT)], 9).wait_send()
    all_of(v.fp.at[pl.ds(0, R - 1), pl.ds(0, share * UNIT)], 10).wait_send()


def fast_shards(
    R, Q,
    latent, deep, timestep, in_weight, front_weight, middle_weight, skip_weight, out_weight,
    time_weight, time_second, time_proj, input_gain, middle_gain, output_gain,
):
    C = deep.shape[0]
    cin = latent.shape[0]
    px = deep.shape[1] * deep.shape[2]
    couts = out_weight.shape[1]
    W = px // R
    N = W * 8
    CP = (C + LANES - 1) // LANES * LANES
    fk, mk, skr = front_weight.shape[0], middle_weight.shape[0], skip_weight.shape[0]
    hbm = pl.BlockSpec(memory_space=pl.ANY)
    vmem = pl.BlockSpec(memory_space=pltpu.VMEM)
    smem = pl.BlockSpec(memory_space=pltpu.SMEM)
    dma = pltpu.SemaphoreType.DMA
    args = (
        latent.reshape(cin, px), deep.reshape(C, px), timestep, in_weight, front_weight.T,
        middle_weight.T, skip_weight, out_weight.T, time_weight, time_second, time_proj.T,
        input_gain, middle_gain, output_gain,
    )
    fq, wide = time_weight.shape
    shapes = dict(
        lat_v=pltpu.VMEM((cin, px), BF16), lat=pltpu.VMEM((3, R, cin, px), BF16),
        latrows=pltpu.VMEM((3, R * cin, px), F32), deep_v=pltpu.VMEM((C, px), BF16),
        dr=pltpu.VMEM((R, W // 2, 2 * C), BF16), a2a=pltpu.VMEM((R, W // 2, 2 * C), BF16),
        inw=pltpu.VMEM((9 * cin, C), BF16), wb=pltpu.VMEM((3, R * cin, R * CP), F32),
        sk=pltpu.VMEM((W, R * CP), F32), jx=pltpu.VMEM((2 * C // LANES, N + 16, LANES), F32),
        hx=pltpu.VMEM((CP // LANES, N + 16, LANES), F32),
        ox=pltpu.VMEM((CP // LANES, N + 16, LANES), F32),
        act_a=pltpu.VMEM((3, N + 16, 2 * C), BF16), act_b=pltpu.VMEM((3, N, 2 * C), BF16),
        act_c=pltpu.VMEM((N + 16, 3 * C), BF16), act_d=pltpu.VMEM((N, 3 * C), BF16),
        front_v=pltpu.VMEM((C, fk), BF16), fw=pltpu.VMEM((18 * C, CP), BF16),
        fp=pltpu.VMEM((R, PACK * UNIT, 2 * C), BF16), mp=pltpu.VMEM((Q, PACK * UNIT, 2 * C), BF16),
        mid_v=pltpu.VMEM((C, mk), BF16), mw=pltpu.VMEM((9 * C, CP), BF16),
        sw=pltpu.VMEM((2 * C, C), BF16), outw_v=pltpu.VMEM((couts, 9 * C), BF16),
        wr32=pltpu.VMEM((LANES, C), F32), tw=pltpu.VMEM((fq, wide), BF16),
        ts=pltpu.VMEM(time_second.shape, BF16), tp=pltpu.VMEM((C, wide), BF16),
        part=pltpu.VMEM((1, fq), F32), emb=pltpu.VMEM((Q, 1, wide), F32),
        sums=pltpu.VMEM((3, R * Q, 1, LANES), F32), tap=pltpu.VMEM((N, LANES), F32),
        outs=pltpu.VMEM((R, couts, LANES), F32), outr=pltpu.VMEM((R, couts, LANES), F32),
        gain_one=pltpu.VMEM((2 * C,), F32), gain_two=pltpu.VMEM((C,), F32),
        gain_three=pltpu.VMEM((C,), F32),
        ld_s=dma((13,)), one_s=dma((11,)), one_r=dma((11,)), halo_s=dma((3, 2)), halo_r=dma((3, 2)),
        fm_r=dma((3, R)), fx_r=dma((R,)), fo_r=dma((R,)), mid_s=dma((2,)), mid_r=dma((12,)),
        sum_s=dma((3,)), sum_r=dma((3,)),
    )
    specs = [hbm] * len(args)
    specs[2] = smem
    out = pl.pallas_call(
        functools.partial(fast_kernel, R, Q, tuple(shapes)),
        out_shape=jax.ShapeDtypeStruct((couts, px), F32),
        in_specs=specs,
        out_specs=vmem,
        scratch_shapes=list(shapes.values()),
        compiler_params=pltpu.CompilerParams(
            collective_id=0, has_side_effects=True, vmem_limit_bytes=56 * 1024 * 1024
        ),
    )(*args)
    return out.reshape(couts, 1, px)


def solution(mesh):
    R, Q = mesh.shape["rows"], mesh.shape["cols"]

    def body(*args):
        deep, front = args[1], args[4]
        fits = (
            R == 8 and Q == 4 and deep.shape[1] == 1 and deep.shape[2] % (R * LANES // 4) == 0
            and front.shape[0] % UNIT == 0
            and PACK * UNIT < front.shape[0] <= 2 * PACK * UNIT
            and args[5].shape[0] == front.shape[0] and deep.shape[0] % LANES * 2 == LANES)
        return (fast_shards if fits else shards)(R, Q, *args)

    return jax.shard_map(
        body,
        mesh=mesh,
        in_specs=(
            P(None, "rows", "cols"), P(None, "rows", "cols"), P(), P(),
            P("rows", None), P("cols", None), P("cols", None), P(),
            P(), P("cols", None), P(), P(), P(), P(),
        ),
        out_specs=P(None, "rows", "cols"),
        check_vma=False,
    )
```

```python
import functools
import math

import jax
import jax.numpy as jnp
from jax import lax
from jax.experimental import pallas as pl
from jax.experimental.pallas import tpu as pltpu
from jax.sharding import PartitionSpec as P

GROUPS = 32
EPS = 1e-05
TILE = 16
LANES = 128
MESH = pl.DeviceIdType.MESH
F32 = jnp.float32
BF16 = jnp.bfloat16
SIDES = tuple((i, j) for i in (-1, 0, 1) for j in (-1, 0, 1) if (i, j) != (0, 0))


def dot(a, b, precision=None):
    return lax.dot_general(
        a, b, (((1,), (0,)), ((), ())), preferred_element_type=F32, precision=precision
    )


def split_dot(row, weight):
    high = row.astype(BF16)
    rest = row - high.astype(F32)
    middle = rest.astype(BF16)
    low = (rest - middle.astype(F32)).astype(BF16)
    pieces = jnp.concatenate([high.astype(F32), middle.astype(F32), low.astype(F32)], axis=0)
    return jnp.sum(dot(pieces.astype(BF16), weight), axis=0, keepdims=True)


def silu(z):
    return z / (1.0 + jnp.exp(-z))


def kernel(
    R, Q, ring,
    latent, deep, rows_in, in_w, front, middle, skip, out_w, time_w, time_s, time_p,
    noise,
    lat, jext, hext, oext, shifted, patch, fw, mw, sw, part, emb, sums_a, sums_b,
    lat_s, lat_r, halo_s, halo_r, fz_s, fy_s, fc_s, fm_r, fo_r, mid_s, mid_r, emb_s, emb_r,
    ca_s, ca_r, cb_s, cb_r, loc_s,
):
    r = lax.axis_index("rows")
    c = lax.axis_index("cols")
    C, px = deep.shape
    cin = latent.shape[0]
    image = float(px * R * Q)
    FQ = time_w.shape[0]
    gain_one = rows_in[:, FQ : FQ + 2 * C]
    gain_two = rows_in[:, FQ + 2 * C : FQ + 3 * C]
    gain_three = rows_in[:, FQ + 3 * C : FQ + 4 * C]

    def remote(src, dst, ssem, rsem, rr, cc):
        return pltpu.make_async_remote_copy(
            src_ref=src, dst_ref=dst, send_sem=ssem, recv_sem=rsem,
            device_id={"rows": rr, "cols": cc}, device_id_type=MESH,
        )

    def each(count, body):
        if count <= 8:
            for i in range(1, count):
                body(i)
        else:
            lax.fori_loop(1, count, lambda i, u: (body(i), u)[1], 0)

    barrier = pltpu.get_barrier_semaphore()

    def greet(rr, cc):
        pl.semaphore_signal(barrier, inc=1, device_id={"rows": rr, "cols": cc}, device_id_type=MESH)

    each(R, lambda i: greet(lax.rem(r + i, R), c))
    each(Q, lambda i: greet(r, lax.rem(c + i, Q)))
    for i in (-1, 1):
        for j in (-1, 1):
            greet(lax.rem(r + i + R, R), lax.rem(c + j + Q, Q))
    pl.semaphore_wait(barrier, R - 1 + Q - 1 + 4)

    def inside(rr, cc):
        return (rr >= 0) & (rr < R) & (cc >= 0) & (cc < Q)

    def lat_copy(k, rr, cc):
        i, j = SIDES[k]
        return remote(latent, lat.at[k], lat_s.at[k], lat_r.at[k], rr, cc)

    for k, (i, j) in enumerate(SIDES):
        @pl.when(inside(r + i, c + j))
        def _():
            lat_copy(k, r + i, c + j).start()

        @pl.when(jnp.logical_not(inside(r - i, c - j)))
        def _():
            lat[k] = jnp.zeros(lat.shape[1:], lat.dtype)

    parity = lax.rem(c, 2)
    mate = c + 1 - 2 * parity
    over = lax.rem(c + 2, Q)
    half_c = lax.rem(r, 2)
    twin = r + 1 - 2 * half_c
    mk, sk = middle.shape[0], skip.shape[0]

    def mid_copies(owner, s, slot_from, target):
        rows_m = pl.ds(pl.multiple_of(owner * mk, TILE), mk)
        rows_s = pl.ds(pl.multiple_of(owner * sk, TILE), sk)
        src_m, src_s = (middle, skip) if slot_from else (mw.at[rows_m], sw.at[rows_s])
        return (
            remote(src_m, mw.at[rows_m], mid_s.at[0, s], mid_r.at[0, s], r, target),
            remote(src_s, sw.at[rows_s], mid_s.at[1, s], mid_r.at[1, s], r, target),
        )

    fk = fw.shape[0] // R if ring else 0
    cut = fk // 2 // TILE * TILE
    spans = ((0, cut), (cut, fk - cut))

    def f_rows(owner, par):
        return pl.ds(pl.multiple_of(owner * fk, TILE) + spans[par][0], spans[par][1])

    def by_parity(par_of, body):
        for par in (0, 1):
            @pl.when(par_of == par)
            def _():
                body(par)

    def f_own(par, target, ssem):
        src = front.at[pl.ds(spans[par][0], spans[par][1])]
        return remote(src, fw.at[f_rows(r, par)], ssem, fm_r.at[r], target, c)

    def f_pass(owner, par, target):
        return remote(fw.at[f_rows(owner, par)], fw.at[f_rows(owner, par)],
                      fy_s.at[owner], fm_r.at[owner], target, c)

    def f_mate(owner, par):
        return remote(fw.at[f_rows(owner, par)], fw.at[f_rows(owner, par)],
                      fc_s.at[owner], fo_r.at[owner], r, mate)

    def by_distance(distances, body):
        for d in distances:
            for t in (r + 2 * d, r - 2 * d):
                @pl.when((t >= 0) & (t < R))
                def _():
                    body(t)

    locals_ = []
    if ring:
        locals_.append(pltpu.make_async_copy(
            front, fw.at[pl.ds(pl.multiple_of(r * fk, TILE), fk)], loc_s.at[0]))
    locals_.append(pltpu.make_async_copy(
        middle, mw.at[pl.ds(pl.multiple_of(c * mk, TILE), mk)], loc_s.at[1]))
    locals_.append(pltpu.make_async_copy(
        skip, sw.at[pl.ds(pl.multiple_of(c * sk, TILE), sk)], loc_s.at[2]))
    for copy in locals_:
        copy.start()

    if ring:
        def first(par):
            f_own(par, twin, fy_s.at[r]).start()
            def one(t):
                f_own(par, t, fz_s.at[t]).start()
            by_distance(range(1, R // 2), one)
        by_parity(parity, first)
    for copy in mid_copies(c, 0, True, over) + mid_copies(c, 1, True, mate):
        copy.start()

    def pass_on(distances):
        def go(par):
            def one(owner):
                f_pass(owner, par, twin).wait_recv()
                f_pass(owner, par, twin).start()
                f_mate(owner, par).start()
            by_distance(distances, one)
        by_parity(parity, go)

    for k, (i, j) in enumerate(SIDES):
        @pl.when(inside(r - i, c - j))
        def _():
            lat_copy(k, r - i, c - j).wait_recv()
    where = {side: k for k, side in enumerate(SIDES)}
    for a in range(3):
        tiles = []
        for b in range(3):
            side = (1 - a, 1 - b)
            block = latent[...] if side == (0, 0) else lat[where[side]]
            tiles.append(block.astype(F32))
        wide = jnp.concatenate(tiles, axis=1)
        for b in range(3):
            start = px + b - 1
            patch[cin * (3 * a + b) : cin * (3 * a + b + 1), :] = wide[:, start : start + px]
    skip_feat = dot(patch[...].T.astype(BF16), in_w[...]).astype(BF16)
    deep_t = deep[...].astype(F32).T.astype(BF16)
    own = pl.ds(TILE, px)
    jext[1, own, :] = jnp.concatenate([deep_t.astype(F32), skip_feat.astype(F32)], axis=1).astype(BF16)

    def halo_copy(stage, ext, k, rr, cc):
        i, j = SIDES[k]
        src = ((TILE, TILE), (TILE, px), (px, TILE))[j + 1]
        dst = ((TILE + px, TILE), (TILE, px), (0, TILE))[j + 1]
        return remote(ext.at[1, pl.ds(*src), :], ext.at[1 - i, pl.ds(*dst), :],
                      halo_s.at[stage, k], halo_r.at[stage, k], rr, cc)

    def halo_send(stage, ext):
        for k, (i, j) in enumerate(SIDES):
            @pl.when(inside(r + i, c + j))
            def _():
                halo_copy(stage, ext, k, r + i, c + j).start()

            @pl.when(jnp.logical_not(inside(r - i, c - j)))
            def _():
                dst = ((TILE + px, TILE), (TILE, px), (0, TILE))[j + 1]
                ext[1 - i, pl.ds(*dst), :] = jnp.zeros((dst[1], ext.shape[2]), ext.dtype)

    def halo_wait(stage, ext):
        for k, (i, j) in enumerate(SIDES):
            @pl.when(inside(r - i, c - j))
            def _():
                halo_copy(stage, ext, k, r - i, c - j).wait_recv()

    def indicator(channels, flip):
        shape = (LANES, channels) if flip else (channels, LANES)
        size = channels // GROUPS
        ch = lax.broadcasted_iota(jnp.int32, shape, 1 if flip else 0)
        g = lax.broadcasted_iota(jnp.int32, shape, 0 if flip else 1)
        return ((ch >= g * size) & (ch < g * size + size)).astype(F32)

    def sum_copy(buf, ssem, rsem, stage, slot, i, rr, cc):
        return remote(buf.at[stage, slot], buf.at[stage, slot],
                      ssem.at[stage, i], rsem.at[stage, i], rr, cc)

    def reduce_start(stage, values):
        top = jnp.sum(values, axis=0, keepdims=True)
        low = jnp.sum(values * values, axis=0, keepdims=True)
        both = jnp.concatenate([top, low, jnp.zeros((6, values.shape[1]), F32)], axis=0)
        sums_a[stage, c] = dot(both, indicator(values.shape[1], False), lax.Precision.HIGHEST)
        for i in range(1, Q):
            sum_copy(sums_a, ca_s, ca_r, stage, c, i, r, lax.rem(c + i, Q)).start()

    def reduce_end(stage, channels):
        for i in range(1, Q):
            s = lax.rem(c + Q - i, Q)
            sum_copy(sums_a, ca_s, ca_r, stage, s, i, r, s).wait_recv()
        sums_b[stage, r] = jnp.sum(sums_a[stage], axis=0)
        each(R, lambda i: sum_copy(sums_b, cb_s, cb_r, stage, r, i, lax.rem(r + i, R), c).start())

        def got(i):
            s = lax.rem(r + R - i, R)
            sum_copy(sums_b, cb_s, cb_r, stage, s, i, s, c).wait_recv()

        each(R, got)
        total = jnp.sum(sums_b[stage], axis=0) / (channels // GROUPS * image)
        center = total[0:1]
        inverse = lax.rsqrt(total[1:2] - center * center + EPS)
        both = jnp.concatenate([center, inverse, jnp.zeros((6, LANES), F32)], axis=0)
        wide = dot(both, indicator(channels, True), lax.Precision.HIGHEST)
        return wide[0:1], wide[1:2]

    def conv(ext, stats, gain, weight, exact=None, shift=None):
        center, inverse = stats
        if shift is not None:
            center = center - shift
        channels = ext.shape[2]
        scale = inverse * gain
        place = lax.broadcasted_iota(jnp.int32, (px + 2 * TILE, 1), 0)
        inner = (place >= TILE) & (place < TILE + px)
        total = None
        for a in (1, 0, 2):
            z = (ext[a].astype(F32) - center) * scale
            here = r + a - 1
            keep = (here >= 0) & (here < R) & (
                inner | ((place < TILE) & (c > 0)) | ((place >= TILE + px) & (c < Q - 1)))
            shifted[:, 0:channels] = jnp.where(keep, silu(z), 0.0)
            if a == 1 and exact is not None:
                shifted[own, 0:channels] = silu((exact - center) * scale)
            for b in range(3):
                act = shifted[TILE + b - 1 : TILE + b - 1 + px, 0:channels].astype(BF16)
                k = (3 * a + b) * channels
                term = dot(act, weight[k : k + channels, :])
                total = term if total is None else total + term
        return total

    joined = jext[1, own, :]
    reduce_start(0, joined.astype(F32))
    halo_send(0, jext)

    hidden = silu(split_dot(rows_in[:, 0:FQ], time_w[...]))
    tk = time_s.shape[0]
    for q in range(Q):
        @pl.when(c == q)
        def _():
            part[...] = hidden[:, q * tk : (q + 1) * tk]
    emb_own = split_dot(part[...], time_s[...])
    emb[c] = emb_own

    def emb_copy(i, src_c, tgt):
        return remote(emb.at[src_c], emb.at[src_c], emb_s.at[i], emb_r.at[i], r, tgt)

    for i in range(1, Q):
        emb_copy(i, c, lax.rem(c + i, Q)).start()

    if ring:
        pass_on((1,))
    stats = reduce_end(0, 2 * C)
    if ring:
        pass_on(range(2, R // 2))

        def from_twin(par):
            def one(t):
                owner = t + twin - r
                f_pass(owner, par, twin).wait_recv()
                f_mate(owner, par).start()
            one(r)
            by_distance(range(1, R // 2), one)
        by_parity(parity, from_twin)

    for copy in mid_copies(over, 0, False, over):
        copy.wait_recv()
    for copy in mid_copies(over, 2, False, mate):
        copy.start()

    for i in range(1, Q):
        s = lax.rem(c + Q - i, Q)
        emb_copy(i, s, s).wait_recv()
    embedded = jnp.sum(emb[...], axis=0)
    time_shift = split_dot(silu(embedded), time_p[...])

    for copy in locals_:
        copy.wait()
    halo_wait(0, jext)
    if ring:
        def from_mate(i):
            owner = lax.rem(r + i, R)
            def go(par):
                f_mate(owner, 1 - par).wait_recv()
            by_parity(parity, go)
        for i in range(1, R):
            from_mate(i)
    front_out = conv(jext, stats, gain_one, fw if ring else front)

    hext[1, own, :] = front_out.astype(BF16)
    reduce_start(1, front_out + time_shift)
    halo_send(1, hext)
    for copy in mid_copies(mate, 1, False, mate):
        copy.wait_recv()
    far = lax.rem(mate + 2, Q)
    for copy in mid_copies(far, 2, False, mate):
        copy.wait_recv()
    shortcut = dot(joined, sw[...])
    stats = reduce_end(1, C)
    halo_wait(1, hext)
    block_out = conv(hext, stats, gain_two, mw, front_out, time_shift) + shortcut

    oext[1, own, :] = block_out.astype(BF16)
    reduce_start(2, block_out)
    halo_send(2, oext)
    stats = reduce_end(2, C)
    halo_wait(2, oext)
    result = conv(oext, stats, gain_three, out_w, block_out)
    noise[...] = result.T[0 : noise.shape[0], :]

    for k, (i, j) in enumerate(SIDES):
        @pl.when(inside(r + i, c + j))
        def _():
            lat_copy(k, r + i, c + j).wait_send()
            for stage, ext in enumerate((jext, hext, oext)):
                halo_copy(stage, ext, k, r + i, c + j).wait_send()
    for i in range(1, Q):
        emb_copy(i, c, lax.rem(c + i, Q)).wait_send()
        for stage in range(3):
            sum_copy(sums_a, ca_s, ca_r, stage, c, i, r, lax.rem(c + i, Q)).wait_send()

    def sent(i):
        for stage in range(3):
            sum_copy(sums_b, cb_s, cb_r, stage, r, i, lax.rem(r + i, R), c).wait_send()

    each(R, sent)
    for copy in (mid_copies(c, 0, True, over) + mid_copies(c, 1, True, mate)
                 + mid_copies(over, 2, False, mate)):
        copy.wait_send()
    if ring:
        def last(par):
            f_own(par, twin, fy_s.at[r]).wait_send()
            def one(t):
                f_own(par, t, fz_s.at[t]).wait_send()
                f_pass(t, par, twin).wait_send()
            by_distance(range(1, R // 2), one)
            for i in range(1, R):
                f_mate(lax.rem(r + i, R), par).wait_send()
        by_parity(parity, last)


def shards(
    R, Q,
    latent, deep, timestep, in_weight, front_weight, middle_weight, skip_weight, out_weight,
    time_weight, time_second, time_proj, input_gain, middle_gain, output_gain,
):
    C = deep.shape[0]
    cin = latent.shape[0]
    px = deep.shape[1] * deep.shape[2]
    assert deep.shape[1] == 1 and Q == 4 and R % 2 == 0 and R > 2
    ring = R <= 8 and front_weight.shape[0] % TILE == 0
    half = time_weight.shape[0] // 2
    ratios = jnp.exp(-math.log(10000.0) * jnp.arange(half, dtype=F32) / half)
    angles = timestep[0].astype(F32) * ratios
    rows_in = jnp.concatenate(
        [jnp.cos(angles), jnp.sin(angles), input_gain, middle_gain, output_gain])[None, :]
    front = front_weight if ring else lax.all_gather(front_weight, "rows", axis=0, tiled=True)
    couts = out_weight.shape[1]
    out_w = jnp.pad(out_weight, ((0, 0), (0, LANES - couts)))
    vmem = pl.BlockSpec(memory_space=pltpu.VMEM)
    dma = pltpu.SemaphoreType.DMA
    wide = time_second.shape[1]
    tall = px + 2 * TILE
    args = (
        latent.reshape(cin, px), deep.reshape(C, px), rows_in, in_weight, front,
        middle_weight, skip_weight, out_w, time_weight, time_second, time_proj,
    )
    out = pl.pallas_call(
        functools.partial(kernel, R, Q, ring),
        out_shape=jax.ShapeDtypeStruct((couts, px), F32),
        in_specs=[vmem] * len(args),
        out_specs=vmem,
        scratch_shapes=[
            pltpu.VMEM((8, cin, px), BF16),
            pltpu.VMEM((3, tall, 2 * C), BF16),
            pltpu.VMEM((3, tall, C), BF16),
            pltpu.VMEM((3, tall, C), BF16),
            pltpu.VMEM((tall, 2 * C), F32),
            pltpu.VMEM((9 * cin, px), F32),
            pltpu.VMEM((18 * C if ring else TILE, C), BF16),
            pltpu.VMEM((9 * C, C), BF16),
            pltpu.VMEM((2 * C, C), BF16),
            pltpu.VMEM((1, time_second.shape[0]), F32),
            pltpu.VMEM((Q, 1, wide), F32),
            pltpu.VMEM((3, Q, 8, LANES), F32),
            pltpu.VMEM((3, R, 8, LANES), F32),
            dma((8,)), dma((8,)), dma((3, 8)), dma((3, 8)),
            dma((R,)), dma((R,)), dma((R,)), dma((R,)), dma((R,)),
            dma((2, 3)), dma((2, 3)), dma((Q,)), dma((Q,)),
            dma((3, Q)), dma((3, Q)), dma((3, R)), dma((3, R)), dma((3,)),
        ],
        compiler_params=pltpu.CompilerParams(
            collective_id=0, has_side_effects=True, vmem_limit_bytes=56 * 1024 * 1024
        ),
    )(*args)
    return out.reshape(couts, 1, px)


UNIT = 16
PACK = 24
ALONE = 3


class Box:
    pass


def snake(pos, c, R):
    q = pos + lax.rem(c, 2) * (R - 1 - 2 * pos)
    late = q // (R // 2)
    return (1 - late) * (2 * q) + late * (2 * (R - 1 - q) + 1)


def place_of(r, c, R):
    odd, h = lax.rem(r, 2), r // 2
    q = (1 - odd) * h + odd * (R - 1 - h)
    return q + lax.rem(c, 2) * (R - 1 - 2 * q)


def dot_nt(a, b, precision=None):
    return lax.dot_general(
        a, b, (((1,), (1,)), ((), ())), preferred_element_type=F32, precision=precision
    )


def pieces_of(row):
    high = row.astype(BF16)
    rest = row - high.astype(F32)
    middle = rest.astype(BF16)
    low = (rest - middle.astype(F32)).astype(BF16)
    return jnp.concatenate(
        [high.astype(F32), middle.astype(F32), low.astype(F32)], axis=0).astype(BF16)


def fast_kernel(
    R, Q, names,
    latent, deep, timestep, in_w, front, middle, skip, out_w, time_w, time_s, time_p,
    input_gain, middle_gain, output_gain, noise, *scratch,
):
    v = Box()
    for name, ref in zip(names, scratch):
        setattr(v, name, ref)
    r = lax.axis_index("rows")
    c = lax.axis_index("cols")
    C, px = deep.shape
    cin = latent.shape[0]
    couts = out_w.shape[0]
    image = float(px * R * Q)
    FQ = time_w.shape[0]
    W = px // R
    N = W * 8
    s = place_of(r, c, R)
    me = c * R + r
    CP = (C + LANES - 1) // LANES * LANES
    GAP = CP - C

    def remote(src, dst, ssem, rsem, rr, cc):
        return pltpu.make_async_remote_copy(
            src_ref=src, dst_ref=dst, send_sem=ssem, recv_sem=rsem,
            device_id={"rows": rr, "cols": cc}, device_id_type=MESH,
        )

    def flipped(value, mask, bits):
        for b in range(bits):
            if mask >> b & 1:
                value = value + (1 - 2 * lax.rem(value // (1 << b), 2)) * (1 << b)
        return value

    others = [(flipped(r, i, 3), flipped(c, j, 2))
              for i in reversed(range(R)) for j in reversed(range(Q)) if (i, j) != (0, 0)]
    barrier = pltpu.get_barrier_semaphore()
    for i, j in others:
        pl.semaphore_signal(
            barrier, inc=1, device_id={"rows": i, "cols": j},
            device_id_type=MESH)

    mk, skr, fk = middle.shape[1], skip.shape[0], front.shape[1]
    loads = {}
    for k, (name, src, dst) in enumerate((
        ("front", front, v.front_v), ("latent", latent, v.lat_v), ("deep", deep, v.deep_v),
        ("in", in_w, v.inw), ("tw", time_w, v.tw), ("ts", time_s, v.ts),
        ("middle", middle, v.mid_v),
        ("skip", skip, v.sw.at[pl.ds(pl.multiple_of(c * skr, TILE), skr)]),
        ("tp", time_p, v.tp), ("out", out_w, v.outw_v),
        ("gain_one", input_gain, v.gain_one), ("gain_two", middle_gain, v.gain_two),
        ("gain_three", output_gain, v.gain_three),
    )):
        loads[name] = pltpu.make_async_copy(src, dst, v.ld_s.at[k])
        loads[name].start()

    tall = PACK * UNIT
    main = C // LANES * LANES
    tail = C - main

    def side_by_side(first, second):
        mixed = jnp.concatenate([first[:, main:C], second[:, main:C]], axis=1)
        return jnp.concatenate([first[:, 0:main], mixed, second[:, 0:main]], axis=1).astype(BF16)

    def packed(ref, k):
        turned = ref[...].astype(F32).T
        first, second = turned[0:tall], turned[k - tall : k]
        return side_by_side(first, second)

    def unpack(block, ref, start):
        def at(first):
            return pl.ds(first if isinstance(first, int) else pl.multiple_of(first, UNIT), tall)

        mixed = block[:, main : main + LANES]
        ref[at(start), 0:main] = block[:, 0:main]
        ref[at(start), main : main + LANES] = mixed
        swapped = pltpu.roll(mixed.astype(F32), LANES - tail, 1).astype(BF16)
        start = start + fk - tall
        ref[at(start), 0:main] = block[:, main + LANES : 2 * C]
        ref[at(start), main : main + LANES] = swapped

    loads["latent"].wait()
    v.lat[0, r] = v.lat_v[...]
    loads["front"].wait()
    v.fp[r] = packed(v.front_v, fk)

    pl.semaphore_wait(barrier, len(others))

    def lat_row(i, rr):
        return remote(v.lat_v, v.lat.at[0, r], v.one_s.at[0], v.one_r.at[0], rr, c)

    for i in range(1, R):
        lat_row(i, lax.rem(r + i, R)).start()

    def lat_left():
        return remote(v.lat_v, v.lat.at[2, r], v.one_s.at[1], v.one_r.at[2],
                      snake(R - 1, c - 1, R), c - 1)

    def lat_right():
        return remote(v.lat_v, v.lat.at[1, r], v.one_s.at[2], v.one_r.at[1],
                      snake(0, c + 1, R), c + 1)

    @pl.when(c > 0)
    def _():
        lat_left().start()

    @pl.when(c < Q - 1)
    def _():
        lat_right().start()

    core, xx = lax.rem(c, 2), c // 2
    mate = c + 1 - 2 * core
    over = lax.rem(c + 2, Q)
    y = lax.rem(r, 2)
    twin = r + 1 - 2 * y
    share = PACK // 2
    sizes = (ALONE, share - 2 * ALONE)

    def f_part(owner, part, x_of, core_of):
        first = (x_of * (share - ALONE), ALONE, share // 2)[part]
        return v.fp.at[owner, pl.ds(
            pl.multiple_of((core_of * share + first) * UNIT, UNIT), sizes[part] * UNIT)]

    def f_move(owner, part, ssem, rr, cc):
        ref = f_part(owner, part, xx, core)
        return remote(ref, ref, ssem, v.fm_r.at[part, owner], rr, cc)

    def f_up(owner, part):
        return f_move(owner, part, v.one_s.at[6], r + 2, c)

    def f_down(owner, part):
        return f_move(owner, part, v.one_s.at[7], r - 2, c)

    def f_twin(owner, part):
        return f_move(owner, part, v.one_s.at[8], twin, c)

    def f_over(owner, x_of):
        ref = f_part(owner, 0, x_of, core)
        return remote(ref, ref, v.one_s.at[9], v.fx_r.at[owner], r, over)

    def f_mate(owner, part):
        ref = f_part(owner, part, xx, core)
        return remote(ref, ref, v.one_s.at[10], v.fo_r.at[owner], r, mate)

    def f_mate_extra(owner):
        ref = f_part(owner, 0, 1 - xx, core)
        return remote(ref, ref, v.one_s.at[10], v.fo_r.at[owner], r, mate)

    def when_row(t, body):
        @pl.when((t >= 0) & (t < R))
        def _():
            body()

    for part in range(2):
        when_row(r + 2, lambda: f_up(r, part).start())
        when_row(r - 2, lambda: f_down(r, part).start())
        f_twin(r, part).start()

    def from_z(d, sign, part):
        t = r + sign * 2 * d

        def body():
            f_twin(t, part).wait_recv()
            if sign < 0:
                when_row(r + 2, lambda: f_up(t, part).start())
            else:
                when_row(r - 2, lambda: f_down(t, part).start())
            f_twin(t, part).start()
            if part == 0:
                f_over(t, xx).start()
            f_mate(t, part).start()
        when_row(t, body)

    def from_y(owner, part):
        f_twin(owner, part).wait_recv()
        if part == 0:
            f_over(owner, xx).start()
        f_mate(owner, part).start()

    def from_x(owner):
        f_over(owner, 1 - xx).wait_recv()
        f_mate_extra(owner).start()

    def x_steps(d, twins):
        for sign in (-1, 1):
            t = r + sign * 2 * d
            when_row(t, lambda: from_x(t + twins * (twin - r)))

    def z_steps(d):
        for part in range(2):
            for sign in (-1, 1):
                from_z(d, sign, part)

    def y_steps(d):
        for part in range(2):
            for sign in (-1, 1):
                t = r + sign * 2 * d
                when_row(t, lambda: from_y(t + twin - r, part))

    loads["middle"].wait()
    v.mp[c] = packed(v.mid_v, mk)
    loads["skip"].wait()
    quarter = tall // 4

    def mid_copy(ref, n, rr, cc):
        kind = 1 if n in (2, 9, 11) else 0
        return remote(ref, ref, v.mid_s.at[kind], v.mid_r.at[n], rr, cc)

    def mid_rows(owner, n, of):
        return v.mp.at[owner, pl.ds(pl.multiple_of((2 * of + n) * quarter, UNIT), quarter)]

    def skip_rows(owner):
        return v.sw.at[pl.ds(pl.multiple_of(owner * skr, TILE), skr)]

    far = lax.rem(mate + 2, Q)

    def mid_over(n, owner):
        ref = skip_rows(owner) if n == 2 else mid_rows(owner, n, y)
        return mid_copy(ref, n, r, over)

    def mid_twin(n, of):
        return mid_copy(mid_rows(over, n, of), 3 + n, twin, c)

    def mid_on(n, owner, of):
        ref = skip_rows(owner) if n == 4 else mid_rows(owner, n % 2, of)
        return mid_copy(ref, 5 + n, r, mate)

    def mid_mate(owner):
        return (mid_copy(v.mp.at[owner], 10, r, mate), mid_copy(skip_rows(owner), 11, r, mate))

    mid_over(0, c).start()
    for copy in mid_mate(c):
        copy.start()

    loads["deep"].wait()
    deep_t = v.deep_v[...].astype(F32).T
    halves = deep_t.reshape(R, 2, W // 2, C)
    doubled = side_by_side(halves[:, 0].reshape(px // 2, C), halves[:, 1].reshape(px // 2, C))
    for q in range(R):
        v.dr[q] = doubled[W // 2 * q : W // 2 * (q + 1)]
    pad = jnp.zeros((1, GAP), F32)
    deep_top = jnp.concatenate([jnp.sum(deep_t, axis=0, keepdims=True), pad], axis=1)
    deep_low = jnp.concatenate([jnp.sum(deep_t * deep_t, axis=0, keepdims=True), pad], axis=1)
    def a2a_copy(q):
        return remote(v.dr.at[q], v.a2a.at[r], v.one_s.at[3], v.one_r.at[3],
                      snake(q, c, R), c)

    def a2a_send():
        for q in range(R):
            @pl.when(s != q)
            def _():
                a2a_copy(q).start()

            @pl.when(s == q)
            def _():
                v.a2a[r] = v.dr[q]

    unpack(v.fp[r], v.fw, r * fk)

    loads["in"].wait()
    inw = v.inw[...].astype(F32)
    v.wb[...] = jnp.zeros(v.wb.shape, F32)
    for b in range(3):
        rows = [inw[cin * (3 * a + b) : cin * (3 * a + b + 1), :] for a in range(3)]
        band = jnp.concatenate(rows, axis=0)
        band = jnp.concatenate([jnp.zeros((3 * cin, GAP), F32), band], axis=1)
        for yy in range(R):
            lo, hi = max(0, yy - 1), min(R, yy + 2)
            v.wb[b, lo * cin : hi * cin, yy * CP : (yy + 1) * CP] = (
                band[(lo - yy + 1) * cin : (hi - yy + 1) * cin, :])

    loads["tw"].wait()
    loads["ts"].wait()
    half = FQ // 2
    index = lax.broadcasted_iota(jnp.int32, (1, half), 1).astype(F32)
    angles = timestep[0].astype(F32) * jnp.exp(-math.log(10000.0) * index / half)
    v.part[:, 0:half] = jnp.cos(angles)
    v.part[:, half:FQ] = jnp.sin(angles)
    hidden = silu(jnp.sum(dot(pieces_of(v.part[...]), v.tw[...]), axis=0, keepdims=True))
    tk = time_s.shape[0]
    for q in range(Q):
        @pl.when(c == q)
        def _():
            v.part[...] = hidden[:, q * tk : (q + 1) * tk]
    v.emb[c] = jnp.sum(dot(pieces_of(v.part[...]), v.ts[...]), axis=0, keepdims=True)

    def emb_copy(i, src_c, target):
        return remote(v.emb.at[src_c], v.emb.at[src_c], v.one_s.at[5], v.one_r.at[5], r, target)

    for i in range(1, Q):
        emb_copy(i, c, lax.rem(c + i, Q)).start()

    @pl.when((s != 0) | (c == 0))
    def _():
        v.lat[1] = jnp.zeros(v.lat.shape[1:], BF16)

    @pl.when((s != R - 1) | (c == Q - 1))
    def _():
        v.lat[2] = jnp.zeros(v.lat.shape[1:], BF16)

    def all_of(ref, n):
        return remote(ref, ref, v.one_s.at[n], v.one_r.at[n], twin, c)

    all_of(v.lat.at[0, pl.ds(0, R - 1)], 0).wait_recv()

    @pl.when((s == 0) & (c > 0))
    def _():
        all_of(v.lat.at[1], 1).wait_recv()

    @pl.when((s == R - 1) & (c < Q - 1))
    def _():
        all_of(v.lat.at[2], 2).wait_recv()

    for k in range(3):
        for q in range(R):
            v.latrows[k, cin * q : cin * (q + 1), :] = v.lat[k, q].astype(F32)
    lane = lax.broadcasted_iota(jnp.int32, (R * cin, px), 1)
    base = jnp.where((lane == px - 1) & (s == 0), v.latrows[1], v.latrows[0])
    base = jnp.where((lane == 0) & (s == R - 1), v.latrows[2], base)
    rolled = pltpu.roll(base, lax.rem(px + 1 - W * s, px), 1)
    v.tap[0:LANES, 0 : R * cin] = rolled[:, 0:LANES].T
    total = None
    for b in range(3):
        term = dot(v.tap[b : b + W, 0 : R * cin].astype(BF16), v.wb[b].astype(BF16))
        total = term if total is None else total + term
    v.sk[...] = total.astype(BF16).astype(F32)
    top = low = None
    for q in range(R):
        slab = v.sk[:, q * CP : (q + 1) * CP]
        top = slab if top is None else top + slab
        low = slab * slab if low is None else low + slab * slab
    skip_top = jnp.sum(top, axis=0, keepdims=True)
    skip_low = jnp.sum(low, axis=0, keepdims=True)

    def join(d, k):
        cut = C // LANES * LANES
        return jnp.concatenate(
            [d[:, 0:cut], d[:, cut:CP] + k[:, 0 : CP - cut], k[:, CP - cut : CP]], axis=1)

    def indicator(channels, flip):
        shape = (LANES, channels) if flip else (channels, LANES)
        size = channels // GROUPS
        ch = lax.broadcasted_iota(jnp.int32, shape, 1 if flip else 0)
        g = lax.broadcasted_iota(jnp.int32, shape, 0 if flip else 1)
        return ((ch >= g * size) & (ch < g * size + size)).astype(F32).astype(BF16)

    def sum_copy(stage, slot, i, rr, cc):
        return remote(v.sums.at[stage, slot], v.sums.at[stage, slot],
                      v.sum_s.at[stage], v.sum_r.at[stage], rr, cc)

    def reduce_start(stage, top, low):
        channels = top.shape[1]
        res = dot(jnp.concatenate([pieces_of(top), pieces_of(low)], axis=0),
                  indicator(channels, False))
        v.sums[stage, me] = jnp.sum(res[0:3], axis=0, keepdims=True) + pltpu.roll(
            jnp.sum(res[3:6], axis=0, keepdims=True), GROUPS, 1)
        for n, (i, j) in enumerate(others):
            sum_copy(stage, me, n, i, j).start()

    def sum_all(stage):
        ref = v.sums.at[stage, pl.ds(0, R * Q - 1)]
        return remote(ref, ref, v.sum_s.at[stage], v.sum_r.at[stage], twin, c)

    def reduce_end(stage, channels):
        sum_all(stage).wait_recv()
        total = jnp.sum(v.sums[stage], axis=0) / (channels // GROUPS * image)
        spread = pltpu.roll(total, LANES - GROUPS, 1) - total * total
        inverse = lax.rsqrt(jnp.maximum(spread, 0.0) + EPS)
        group = lax.broadcasted_iota(jnp.int32, (1, LANES), 1) < GROUPS
        wide = dot(jnp.concatenate([pieces_of(jnp.where(group, row, 0.0))
                                    for row in (total, inverse)], axis=0),
                   indicator(channels, True))
        return (jnp.sum(wide[0:3], axis=0, keepdims=True),
                jnp.sum(wide[3:6], axis=0, keepdims=True))

    reduce_start(0, join(deep_top, skip_top), join(deep_low, skip_low))

    inner = (s + R - 1) // R
    last = (s + 1) // R
    left = (inner * snake(s - 1, c, R) + (1 - inner) * r, c - (1 - inner))
    right = ((1 - last) * snake(s + 1, c, R) + last * r, c + last)
    has_left, has_right = left[1] >= 0, right[1] < Q

    def halo_left(stage, ext):
        return remote(ext.at[:, pl.ds(8, 8)], ext.at[:, pl.ds(N + 8, 8)],
                      v.halo_s.at[stage, 0], v.halo_r.at[stage, 1], left[0], left[1])

    def halo_right(stage, ext):
        return remote(ext.at[:, pl.ds(N, 8)], ext.at[:, pl.ds(0, 8)],
                      v.halo_s.at[stage, 1], v.halo_r.at[stage, 0], right[0], right[1])

    def halo_send(stage, ext):
        zeros = jnp.zeros((ext.shape[0], 8, LANES), F32)

        @pl.when(has_left)
        def _():
            halo_left(stage, ext).start()

        @pl.when(has_right)
        def _():
            halo_right(stage, ext).start()

        @pl.when(jnp.logical_not(has_left))
        def _():
            ext[:, 0:8, :] = zeros

        @pl.when(jnp.logical_not(has_right))
        def _():
            ext[:, N + 8 : N + 16, :] = zeros

    def halo_wait(stage, ext):
        @pl.when(has_left)
        def _():
            halo_right(stage, ext).wait_recv()

        @pl.when(has_right)
        def _():
            halo_left(stage, ext).wait_recv()

    z_steps(1)
    for part in range(2):
        from_y(twin, part)
    mid_over(1, c).start()
    z_steps(2)
    a2a_send()
    y_steps(1)
    for d in range(3, R // 2):
        z_steps(d)
        y_steps(d - 1)
    all_of(v.a2a.at[pl.ds(0, R - 1)], 3).wait_recv()
    for q in range(R):
        block = v.a2a[q].astype(F32)
        mixed = block[:, main : main + LANES]
        used = lax.broadcasted_iota(jnp.int32, mixed.shape, 1) < tail
        upper = jnp.concatenate([block[:, 0:main], jnp.where(used, mixed, 0.0)], axis=1)
        lower = jnp.concatenate(
            [block[:, main + LANES : 2 * C],
             jnp.where(used, pltpu.roll(mixed, LANES - tail, 1), 0.0)], axis=1)
        joined = join(jnp.concatenate([upper, lower], axis=0), v.sk[:, q * CP : (q + 1) * CP])
        for n in range(2 * C // LANES):
            v.jx[n, pl.ds(8 + q, W, 8), :] = joined[:, n * LANES : (n + 1) * LANES]
    halo_send(0, v.jx)
    from_x(twin)
    x_steps(1, 0)
    x_steps(2, 0)
    x_steps(1, 1)
    y_steps(R // 2 - 1)
    mid_over(2, c).start()
    for n in (0, 1):
        mid_over(n, over).wait_recv()
        mid_twin(n, y).start()
        mid_on(n, over, y).start()

    loads["out"].wait()
    loads["tp"].wait()
    for name in ("gain_one", "gain_two", "gain_three"):
        loads[name].wait()
    v.wr32[...] = jnp.zeros(v.wr32.shape, F32)
    for t in range(9):
        v.wr32[couts * t : couts * (t + 1), :] = v.outw_v[:, C * t : C * (t + 1)].astype(F32)
    out_taps = v.wr32[...].T.astype(BF16)

    all_of(v.emb.at[pl.ds(0, Q - 1)], 5).wait_recv()
    embedded = jnp.sum(v.emb[...], axis=0)
    time_shift = jnp.sum(dot_nt(pieces_of(silu(embedded)), v.tp[...]), axis=0, keepdims=True)

    place = lax.broadcasted_iota(jnp.int32, (W + 2, 8, 1), 0)
    inside = (
        ((place > 0) | has_left) & ((place < W + 1) | has_right))
    row = lax.broadcasted_iota(jnp.int32, (W + 2, 8, 1), 1)

    def keep_own(ext, values):
        for n in range(ext.shape[0]):
            lo, hi = n * LANES, min((n + 1) * LANES, values.shape[1])
            ext[n, 8 : N + 8, 0 : hi - lo] = values[:, lo:hi]

    def rows_of(ext, channels, first, count):
        return jnp.concatenate(
            [ext[n, first : first + count, 0 : min(LANES, channels - n * LANES)]
             for n in range(ext.shape[0])], axis=1)

    def activate(ext, stats, gain):
        center, inverse = stats
        scale = inverse * gain
        channels = gain.shape[1]
        for lo in range(0, channels, LANES):
            hi = min(channels, lo + LANES)
            z = silu((ext[lo // LANES, :, 0 : hi - lo] - center[:, lo:hi]) * scale[:, lo:hi])
            z = jnp.where(inside, z.reshape(W + 2, 8, hi - lo), 0.0)
            for a in range(3):
                if a == 1:
                    moved = z
                elif a == 0:
                    moved = jnp.where(row > 0, pltpu.roll(z, 1, 1), 0.0)
                else:
                    moved = jnp.where(row < 7, pltpu.roll(z, 7, 1), 0.0)
                flat = moved.reshape(N + 16, hi - lo)
                v.act_a[a, :, lo:hi] = flat.astype(BF16)
                v.act_b[a, :, lo:hi] = flat[8 : N + 8].astype(BF16)

    def conv_whole(channels, weight):
        acts = [v.act_b[a] if b == 1 else v.act_a[a, 8 * b : 8 * b + N]
                for a in range(3) for b in range(3)]
        return dot(jnp.concatenate(acts, axis=1), weight[:, 0:C])

    def activate_wide(ext, stats, gain):
        center, inverse = stats
        z = silu((rows_of(ext, C, 0, N + 16) - center) * (inverse * gain))
        z = jnp.where(inside, z.reshape(W + 2, 8, C), 0.0)
        moved = (jnp.where(row > 0, pltpu.roll(z, 1, 1), 0.0), z,
                 jnp.where(row < 7, pltpu.roll(z, 7, 1), 0.0))
        wide = jnp.concatenate([m.reshape(N + 16, C) for m in moved], axis=1)
        v.act_c[...] = wide.astype(BF16)
        v.act_d[...] = wide[8 : N + 8].astype(BF16)

    def conv_columns(weight):
        total = None
        for b, act in enumerate((v.act_c[0:N], v.act_d[...], v.act_c[16 : N + 16])):
            term = dot(act, weight[3 * C * b : 3 * C * (b + 1), 0:C])
            total = term if total is None else total + term
        return total

    def unpack_columns(owner):
        for side in (0, 1):
            first = owner * mk + side * tall
            stop = owner * mk + (tall if side == 0 else mk)
            while first < stop:
                tap, inside_tap = divmod(first, C)
                count = min(C - inside_tap, stop - first)
                at = first - owner * mk - side * (mk - tall)
                to = (tap % 3 * 3 + tap // 3) * C + inside_tap
                block = v.mp[owner, at : at + count]
                mixed = block[:, main : main + LANES]
                if side == 0:
                    v.mw[to : to + count, 0:main] = block[:, 0:main]
                else:
                    v.mw[to : to + count, 0:main] = block[:, main + LANES : 2 * C]
                    mixed = pltpu.roll(mixed.astype(F32), LANES - tail, 1).astype(BF16)
                v.mw[to : to + count, main : main + LANES] = mixed
                first += count

    for d in range(3, R // 2):
        x_steps(d, 0)
        x_steps(d - 1, 1)
    x_steps(R // 2 - 1, 1)

    def ready(owner):
        ref = v.fp.at[owner, pl.ds(0, share * UNIT)]
        remote(ref, ref, v.one_s.at[10], v.fo_r.at[owner], r, mate).wait_recv()
        unpack(v.fp[owner], v.fw, owner * fk)

    def when_pair(d, twins, body):
        for sign in (-1, 1):
            t = r + sign * 2 * d
            when_row(t, lambda: body(t + twins * (twin - r)))

    ready(twin)
    when_pair(1, 0, ready)
    when_pair(1, 1, ready)
    for d in range(2, R // 2 - 1):
        when_pair(d, 0, ready)
    stats = reduce_end(0, 2 * C)
    halo_wait(0, v.jx)
    activate(v.jx, stats, v.gain_one[...].reshape(1, 2 * C))

    for d in range(2, R // 2):
        when_pair(d, 1, ready)
    when_pair(R // 2 - 1, 0, ready)

    hidden_one = conv_whole(2 * C, v.fw) + time_shift
    keep_own(v.hx, hidden_one)
    reduce_start(1, jnp.sum(hidden_one, axis=0, keepdims=True),
                 jnp.sum(hidden_one * hidden_one, axis=0, keepdims=True))
    halo_send(1, v.hx)

    mid_over(2, over).wait_recv()
    mid_on(4, over, y).start()
    for n in (0, 1):
        mid_twin(n, 1 - y).wait_recv()
        mid_on(2 + n, over, 1 - y).start()
    for copy in mid_mate(mate):
        copy.wait_recv()
    for n in range(5):
        mid_on(n, far, y if n < 2 else 1 - y).wait_recv()
    for owner in range(Q):
        unpack_columns(owner)
    shortcut = dot(rows_of(v.jx, 2 * C, 8, N).astype(BF16), v.sw[...])
    stats = reduce_end(1, C)
    halo_wait(1, v.hx)
    activate_wide(v.hx, stats, v.gain_two[...].reshape(1, C))
    block_out = conv_columns(v.mw) + shortcut

    keep_own(v.ox, block_out)
    reduce_start(2, jnp.sum(block_out, axis=0, keepdims=True),
                 jnp.sum(block_out * block_out, axis=0, keepdims=True))
    halo_send(2, v.ox)
    stats = reduce_end(2, C)
    halo_wait(2, v.ox)

    center, inverse = stats
    z = silu((rows_of(v.ox, C, 0, N + 16) - center) * (inverse * v.gain_three[...].reshape(1, C)))
    z = jnp.where(inside, z.reshape(W + 2, 8, C), 0.0).reshape(N + 16, C)
    spread = dot(z.astype(BF16), out_taps)
    lane = lax.broadcasted_iota(jnp.int32, (N, LANES), 1)
    row = lax.broadcasted_iota(jnp.int32, (W, 8, 1), 1)
    total = None
    for a in range(3):
        got = None
        for b in range(3):
            t = couts * (3 * a + b)
            here = jnp.where(
                (lane >= t) & (lane < t + couts), spread[8 * b : 8 * b + N, :], 0.0)
            got = here if got is None else got + here
        got = got.reshape(W, 8, LANES)
        if a == 0:
            got = jnp.where(row > 0, pltpu.roll(got, 1, 1), 0.0)
        elif a == 2:
            got = jnp.where(row < 7, pltpu.roll(got, 7, 1), 0.0)
        total = got if total is None else total + got
    v.tap[...] = total.reshape(N, LANES)
    ordered = jnp.concatenate([v.tap[pl.ds(q, W, 8), :] for q in range(R)], axis=0)
    fold = (lax.rem(lax.broadcasted_iota(jnp.int32, (8, LANES), 1), couts)
            == lax.broadcasted_iota(jnp.int32, (8, LANES), 0)).astype(F32)
    rows = dot_nt(fold, ordered, lax.Precision.HIGHEST)[0:couts]
    for q in range(R):
        v.outs[q, :, 0:W] = rows[:, W * q : W * (q + 1)]

    def out_copy(q, rr):
        return remote(v.outs.at[q], v.outr.at[s], v.one_s.at[4], v.one_r.at[4], rr, c)

    for q in range(R):
        @pl.when(r != q)
        def _():
            out_copy(q, q).start()

        @pl.when(r == q)
        def _():
            v.outr[s] = v.outs[q]

    all_of(v.outr.at[pl.ds(0, R - 1)], 4).wait_recv()
    for q in range(R):
        noise[:, W * q : W * (q + 1)] = v.outr[q, :, 0:W]

    all_of(v.lat.at[0, pl.ds(0, R - 1)], 0).wait_send()

    @pl.when(c > 0)
    def _():
        lat_left().wait_send()

    @pl.when(c < Q - 1)
    def _():
        lat_right().wait_send()

    all_of(v.a2a.at[pl.ds(0, R - 1)], 3).wait_send()
    all_of(v.outr.at[pl.ds(0, R - 1)], 4).wait_send()
    all_of(v.emb.at[pl.ds(0, Q - 1)], 5).wait_send()
    for stage, ext in enumerate((v.jx, v.hx, v.ox)):
        sum_all(stage).wait_send()

        @pl.when(has_left)
        def _():
            halo_left(stage, ext).wait_send()

        @pl.when(has_right)
        def _():
            halo_right(stage, ext).wait_send()
    for kind, ref in enumerate((v.mp.at[pl.ds(0, 3)], v.sw.at[pl.ds(0, 3 * skr)])):
        remote(ref, ref, v.mid_s.at[kind], v.mid_r.at[0], r, mate).wait_send()
    moved = (share - ALONE) * UNIT
    level = r // 2
    for count in range(1, R // 2):
        @pl.when(level == count - 1)
        def _():
            all_of(v.fp.at[pl.ds(0, count), pl.ds(0, moved)], 6).wait_send()

        @pl.when(level == R // 2 - count)
        def _():
            all_of(v.fp.at[pl.ds(0, count), pl.ds(0, moved)], 7).wait_send()

    all_of(v.fp.at[pl.ds(0, R // 2), pl.ds(0, moved)], 8).wait_send()
    all_of(v.fp.at[pl.ds(0, R - 1), pl.ds(0, ALONE * UNIT)], 9).wait_send()
    all_of(v.fp.at[pl.ds(0, R - 1), pl.ds(0, share * UNIT)], 10).wait_send()


def fast_shards(
    R, Q,
    latent, deep, timestep, in_weight, front_weight, middle_weight, skip_weight, out_weight,
    time_weight, time_second, time_proj, input_gain, middle_gain, output_gain,
):
    C = deep.shape[0]
    cin = latent.shape[0]
    px = deep.shape[1] * deep.shape[2]
    couts = out_weight.shape[1]
    W = px // R
    N = W * 8
    CP = (C + LANES - 1) // LANES * LANES
    fk, mk, skr = front_weight.shape[0], middle_weight.shape[0], skip_weight.shape[0]
    hbm = pl.BlockSpec(memory_space=pl.ANY)
    vmem = pl.BlockSpec(memory_space=pltpu.VMEM)
    smem = pl.BlockSpec(memory_space=pltpu.SMEM)
    dma = pltpu.SemaphoreType.DMA
    args = (
        latent.reshape(cin, px), deep.reshape(C, px), timestep, in_weight, front_weight.T,
        middle_weight.T, skip_weight, out_weight.T, time_weight, time_second, time_proj.T,
        input_gain, middle_gain, output_gain,
    )
    fq, wide = time_weight.shape
    shapes = dict(
        lat_v=pltpu.VMEM((cin, px), BF16), lat=pltpu.VMEM((3, R, cin, px), BF16),
        latrows=pltpu.VMEM((3, R * cin, px), F32), deep_v=pltpu.VMEM((C, px), BF16),
        dr=pltpu.VMEM((R, W // 2, 2 * C), BF16), a2a=pltpu.VMEM((R, W // 2, 2 * C), BF16),
        inw=pltpu.VMEM((9 * cin, C), BF16), wb=pltpu.VMEM((3, R * cin, R * CP), F32),
        sk=pltpu.VMEM((W, R * CP), F32), jx=pltpu.VMEM((2 * C // LANES, N + 16, LANES), F32),
        hx=pltpu.VMEM((CP // LANES, N + 16, LANES), F32),
        ox=pltpu.VMEM((CP // LANES, N + 16, LANES), F32),
        act_a=pltpu.VMEM((3, N + 16, 2 * C), BF16), act_b=pltpu.VMEM((3, N, 2 * C), BF16),
        act_c=pltpu.VMEM((N + 16, 3 * C), BF16), act_d=pltpu.VMEM((N, 3 * C), BF16),
        front_v=pltpu.VMEM((C, fk), BF16), fw=pltpu.VMEM((18 * C, CP), BF16),
        fp=pltpu.VMEM((R, PACK * UNIT, 2 * C), BF16), mp=pltpu.VMEM((Q, PACK * UNIT, 2 * C), BF16),
        mid_v=pltpu.VMEM((C, mk), BF16), mw=pltpu.VMEM((9 * C, CP), BF16),
        sw=pltpu.VMEM((2 * C, C), BF16), outw_v=pltpu.VMEM((couts, 9 * C), BF16),
        wr32=pltpu.VMEM((LANES, C), F32), tw=pltpu.VMEM((fq, wide), BF16),
        ts=pltpu.VMEM(time_second.shape, BF16), tp=pltpu.VMEM((C, wide), BF16),
        part=pltpu.VMEM((1, fq), F32), emb=pltpu.VMEM((Q, 1, wide), F32),
        sums=pltpu.VMEM((3, R * Q, 1, LANES), F32), tap=pltpu.VMEM((N, LANES), F32),
        outs=pltpu.VMEM((R, couts, LANES), F32), outr=pltpu.VMEM((R, couts, LANES), F32),
        gain_one=pltpu.VMEM((2 * C,), F32), gain_two=pltpu.VMEM((C,), F32),
        gain_three=pltpu.VMEM((C,), F32),
        ld_s=dma((13,)), one_s=dma((11,)), one_r=dma((11,)), halo_s=dma((3, 2)), halo_r=dma((3, 2)),
        fm_r=dma((3, R)), fx_r=dma((R,)), fo_r=dma((R,)), mid_s=dma((2,)), mid_r=dma((12,)),
        sum_s=dma((3,)), sum_r=dma((3,)),
    )
    specs = [hbm] * len(args)
    specs[2] = smem
    out = pl.pallas_call(
        functools.partial(fast_kernel, R, Q, tuple(shapes)),
        out_shape=jax.ShapeDtypeStruct((couts, px), F32),
        in_specs=specs,
        out_specs=vmem,
        scratch_shapes=list(shapes.values()),
        compiler_params=pltpu.CompilerParams(
            collective_id=0, has_side_effects=True, vmem_limit_bytes=56 * 1024 * 1024
        ),
    )(*args)
    return out.reshape(couts, 1, px)


def solution(mesh):
    R, Q = mesh.shape["rows"], mesh.shape["cols"]

    def body(*args):
        deep, front = args[1], args[4]
        fits = (
            R == 8 and Q == 4 and deep.shape[1] == 1 and deep.shape[2] % (R * LANES // 4) == 0
            and front.shape[0] % UNIT == 0
            and PACK * UNIT < front.shape[0] <= 2 * PACK * UNIT
            and args[5].shape[0] == front.shape[0] and deep.shape[0] % LANES * 2 == LANES)
        return (fast_shards if fits else shards)(R, Q, *args)

    return jax.shard_map(
        body,
        mesh=mesh,
        in_specs=(
            P(None, "rows", "cols"), P(None, "rows", "cols"), P(), P(),
            P("rows", None), P("cols", None), P("cols", None), P(),
            P(), P("cols", None), P(), P(), P(), P(),
        ),
        out_specs=P(None, "rows", "cols"),
        check_vma=False,
    )
```
